8 devices in a mesh: dp: 2 (over z, y), cp: 4 (over x, core).
Axes of the slice: x: 2, y: 2, z: 1, core: 2. Of those that a mesh axis runs over, the one named last changes fastest.
Arguments:
- x_act: bfloat16 [8192, 1536], P(('dp', 'cp')), parts along dimension 0
- seg_ids: int32 [8192], P(('dp', 'cp')), parts along dimension 0
- w_q: bfloat16 [1536, 12, 128], replicated
- w_k: bfloat16 [1536, 2, 128], replicated
- w_v: bfloat16 [1536, 2, 128], replicated
- w_o: bfloat16 [1536, 12, 128], replicated
- dy_act: bfloat16 [8192, 1536], P(('dp', 'cp')), parts along dimension 0
Outputs:
- output 1: bfloat16 [8192, 1536], P(('dp', 'cp')), parts along dimension 0
- output 2: bfloat16 [8192, 1536], P(('dp', 'cp')), parts along dimension 0
- output 3: float32 [3072, 12, 128], P(('dp', 'cp')), parts along dimension 0
- output 4: float32 [3072, 2, 128], P(('dp', 'cp')), parts along dimension 0
- output 5: float32 [3072, 2, 128], P(('dp', 'cp')), parts along dimension 0
- output 6: float32 [3072, 12, 128], P(('dp', 'cp')), parts along dimension 0
There are 2 independent parts. The reference program is written for one: setup_inputs(seed, part) draws one part's arguments, and reference() takes and returns one part's arrays. A program takes and returns all parts, laid end to end along the dimension named above; an argument that names none is the same for every part.
All inputs are finite; a program needn't handle non-finite values.
Results may differ from the reference program's by a relative error of at most 0.02.
Values are sent between devices in bfloat16 or wider.
A program may use at most 1 GiB of HBM per device.

```python
import jax
import jax.numpy as jnp
from jax import lax

CP_SIZE = 4
TOK_DEV = 1024
MODEL_DIM = 1536
Q_HEADS = 12
KV_HEADS = 2
HEAD_DIM = 128

SEQ_LEN = CP_SIZE * TOK_DEV
GROUP_SIZE = Q_HEADS // KV_HEADS
Q_BLOCK = min(TOK_DEV, 128)
N_BLOCKS = SEQ_LEN // Q_BLOCK


def draw_segments(seg_key):
    key_zone, key_kind, key_short = jax.random.split(seg_key, 3)
    positions = jnp.arange(SEQ_LEN)
    zone_start = (jax.random.randint(key_zone, (SEQ_LEN,), 0, 2 * TOK_DEV) == 0) | (positions == 0)
    zone_index = jnp.cumsum(zone_start.astype(jnp.int32))
    parity = jax.random.randint(key_kind, (), 0, 2)
    short_zone = (zone_index + parity) % 2 == 0
    short_start = jax.random.randint(key_short, (SEQ_LEN,), 0, max(TOK_DEV // 8, 2)) == 0
    starts = zone_start | (short_zone & short_start)
    return (jnp.cumsum(starts.astype(jnp.int32)) - 1).astype(jnp.int32)


def setup_inputs(seed: int = 0, part: int = 0) -> dict:
    base_key = jax.random.key(seed)
    part_key = jax.random.fold_in(base_key, part)
    weight_key = jax.random.fold_in(base_key, 1000003)
    key_seg, key_x, key_dy = jax.random.split(part_key, 3)
    key_q, key_k, key_v, key_o = jax.random.split(weight_key, 4)
    in_scale = MODEL_DIM ** -0.5
    out_scale = (Q_HEADS * HEAD_DIM) ** -0.5
    q_shape = (MODEL_DIM, Q_HEADS, HEAD_DIM)
    kv_shape = (MODEL_DIM, KV_HEADS, HEAD_DIM)
    return {
        'x_act': jax.random.normal(key_x, (SEQ_LEN, MODEL_DIM), jnp.float32).astype(jnp.bfloat16),
        'seg_ids': draw_segments(key_seg),
        'w_q': (1.5 * in_scale * jax.random.normal(key_q, q_shape, jnp.float32)).astype(jnp.bfloat16),
        'w_k': (in_scale * jax.random.normal(key_k, kv_shape, jnp.float32)).astype(jnp.bfloat16),
        'w_v': (in_scale * jax.random.normal(key_v, kv_shape, jnp.float32)).astype(jnp.bfloat16),
        'w_o': (out_scale * jax.random.normal(key_o, q_shape, jnp.float32)).astype(jnp.bfloat16),
        'dy_act': jax.random.normal(key_dy, (SEQ_LEN, MODEL_DIM), jnp.float32).astype(jnp.bfloat16),
    }


def product32(einsum_form, left_arg, right_arg):
    return jnp.einsum(einsum_form, left_arg.astype(jnp.float32), right_arg.astype(jnp.float32))


def reference(x_act, seg_ids, w_q, w_k, w_v, w_o, dy_act):
    score_scale = HEAD_DIM ** -0.5
    w_q4 = w_q.reshape(MODEL_DIM, KV_HEADS, GROUP_SIZE, HEAD_DIM)
    w_o4 = w_o.reshape(MODEL_DIM, KV_HEADS, GROUP_SIZE, HEAD_DIM)
    q_all = product32('sm,mkgd->skgd', x_act, w_q4).astype(jnp.bfloat16)
    k_all = product32('sm,mkd->skd', x_act, w_k).astype(jnp.bfloat16)
    v_all = product32('sm,mkd->skd', x_act, w_v).astype(jnp.bfloat16)
    do_all = product32('qm,mkgd->qkgd', dy_act, w_o4).astype(jnp.bfloat16)
    k_wide = k_all.astype(jnp.float32)
    v_wide = v_all.astype(jnp.float32)
    key_pos = jnp.arange(SEQ_LEN)

    def block_step(carry_in, block_in):
        dk_acc, dv_acc = carry_in
        q_blk, do_blk, seg_blk, first_pos = block_in
        q_wide = q_blk.astype(jnp.float32)
        do_wide = do_blk.astype(jnp.float32)
        query_pos = first_pos + jnp.arange(Q_BLOCK)
        allowed = (seg_blk[:, None] == seg_ids[None, :]) & (key_pos[None, :] <= query_pos[:, None])
        scores = jnp.einsum('qkgd,skd->kqgs', q_wide, k_wide) * score_scale
        scores = jnp.where(allowed[None, :, None, :], scores, -jnp.inf)
        attn_prob = jax.nn.softmax(scores, axis=-1)
        prob_half = attn_prob.astype(jnp.bfloat16).astype(jnp.float32)
        out_blk = jnp.einsum('kqgs,skd->kqgd', prob_half, v_wide).astype(jnp.bfloat16)
        row_delta = jnp.einsum('qkgd,kqgd->kqg', do_wide, out_blk.astype(jnp.float32))
        dprobs = jnp.einsum('qkgd,skd->kqgs', do_wide, v_wide)
        dscores = (attn_prob * (dprobs - row_delta[..., None])).astype(jnp.bfloat16).astype(jnp.float32)
        dq_blk = (jnp.einsum('kqgs,skd->kqgd', dscores, k_wide) * score_scale).astype(jnp.bfloat16)
        dk_acc = dk_acc + jnp.einsum('kqgs,qkgd->skd', dscores, q_wide)
        dv_acc = dv_acc + jnp.einsum('kqgs,qkgd->skd', prob_half, do_wide)
        return (dk_acc, dv_acc), (out_blk, dq_blk)

    zeros_kv = jnp.zeros((SEQ_LEN, KV_HEADS, HEAD_DIM), jnp.float32)
    block_inputs = (
        q_all.reshape(N_BLOCKS, Q_BLOCK, KV_HEADS, GROUP_SIZE, HEAD_DIM),
        do_all.reshape(N_BLOCKS, Q_BLOCK, KV_HEADS, GROUP_SIZE, HEAD_DIM),
        seg_ids.reshape(N_BLOCKS, Q_BLOCK),
        jnp.arange(N_BLOCKS) * Q_BLOCK,
    )
    (dk_acc, dv_acc), (out_blocks, dq_blocks) = lax.scan(block_step, (zeros_kv, zeros_kv), block_inputs)
    grad_k = (dk_acc * score_scale).astype(jnp.bfloat16)
    grad_v = dv_acc.astype(jnp.bfloat16)
    x_blocks = x_act.reshape(N_BLOCKS, Q_BLOCK, MODEL_DIM)
    dy_blocks = dy_act.reshape(N_BLOCKS, Q_BLOCK, MODEL_DIM)
    y_out = product32('nkqgd,mkgd->nqm', out_blocks, w_o4).reshape(SEQ_LEN, MODEL_DIM).astype(jnp.bfloat16)
    dx_wide = (product32('nkqgd,mkgd->nqm', dq_blocks, w_q4).reshape(SEQ_LEN, MODEL_DIM)
               + product32('skd,mkd->sm', grad_k, w_k) + product32('skd,mkd->sm', grad_v, w_v))
    dx_out = dx_wide.astype(jnp.bfloat16)
    dw_q = product32('nqm,nkqgd->mkgd', x_blocks, dq_blocks).reshape(MODEL_DIM, Q_HEADS, HEAD_DIM)
    dw_k = product32('sm,skd->mkd', x_act, grad_k)
    dw_v = product32('sm,skd->mkd', x_act, grad_v)
    dw_o = product32('nqm,nkqgd->mkgd', dy_blocks, out_blocks).reshape(MODEL_DIM, Q_HEADS, HEAD_DIM)
    return (y_out, dx_out, dw_q, dw_k, dw_v, dw_o)
```

```python
import functools
import math

import jax
import jax.numpy as jnp
from jax import lax
from jax.experimental import pallas as pl
from jax.experimental.pallas import tpu as pltpu
from jax.sharding import PartitionSpec as P

BLK = 256
HEADS = 6
HD = 128
WIDE = HEADS * BLK
HALF = 8
VMEM_LIMIT = 60 * 1024 * 1024


def dot(a, b):
    return jnp.dot(a, b, preferred_element_type=jnp.float32)


def dot_tn(a, b):
    return lax.dot_general(a, b, (((0,), (0,)), ((), ())), preferred_element_type=jnp.float32)


def dot_nt(a, b):
    return lax.dot_general(a, b, (((1,), (1,)), ((), ())), preferred_element_type=jnp.float32)


def stack_heads(src, dst):
    for h in range(HEADS):
        dst[h * BLK:(h + 1) * BLK, :] = src[:, h * HD:(h + 1) * HD]


def flip_heads(src, dst):
    for h in range(HEADS):
        dst[:, h * BLK:(h + 1) * BLK] = src[:, h * HD:(h + 1) * HD].T


def pair_mask(segk_ref, segq_ref, key_start, key_block, query_block):
    segk = segk_ref[pl.ds(key_start, BLK), :]
    segk = jnp.concatenate([segk] * (BLK // 128), axis=1)
    same = segk == segq_ref[0]
    rel = (lax.broadcasted_iota(jnp.int32, (BLK, BLK), 0)
           - lax.broadcasted_iota(jnp.int32, (BLK, BLK), 1))
    return same & (rel <= (query_block - key_block) * BLK)


def fwd_kernel(lo_ref, hi_ref, core_ref, q_own, q_oth, kv_ref, segk_ref, segq_ref,
               o_own, o_oth, lse_ref, qt, acc, m_ref, l_ref):
    step = pl.program_id(0)
    scale2 = HD ** -0.5 * math.log2(math.e)

    @pl.when(step < 4)
    def _():
        flip_heads(q_own, qt)

    @pl.when(step >= 4)
    def _():
        flip_heads(q_oth, qt)

    acc[...] = jnp.zeros_like(acc)
    m_ref[...] = jnp.full_like(m_ref, -jnp.inf)
    l_ref[...] = jnp.zeros_like(l_ref)
    hi = hi_ref[step]
    count = hi - lo_ref[step] + 1

    def body(it, carry):
        p = hi - it
        store = (p & 8) + ((p + 4 * core_ref[0]) & 7)
        key_start = pl.multiple_of(store * BLK, BLK)
        k_blk = kv_ref[pl.ds(key_start, BLK), :HD]
        v_t = kv_ref[pl.ds(key_start, BLK), HD:].T
        mask = pair_mask(segk_ref, segq_ref, key_start, p, hi)
        for h in range(HEADS):
            cols = slice(h * BLK, (h + 1) * BLK)
            s = jnp.where(mask, dot(k_blk, qt[:, cols]), -jnp.inf)
            m_old = m_ref[:, cols]
            m_new = jnp.maximum(m_old, jnp.max(s, axis=0, keepdims=True))
            w = jnp.exp2((s - m_new) * scale2)
            fac = jnp.exp2((m_old - m_new) * scale2)
            m_ref[:, cols] = m_new
            l_ref[:, cols] = l_ref[:, cols] * fac + jnp.sum(w, axis=0, keepdims=True)
            acc[:, cols] = acc[:, cols] * fac + dot(v_t, w.astype(jnp.bfloat16))
        return carry

    lax.fori_loop(0, count, body, 0)
    total = l_ref[...]
    lse_ref[0] = m_ref[...] * scale2 + jnp.log2(total)
    inv = 1.0 / total

    def put(dst):
        for h in range(HEADS):
            cols = slice(h * BLK, (h + 1) * BLK)
            dst[:, h * HD:(h + 1) * HD] = (acc[:, cols] * inv[:, cols]).T.astype(jnp.bfloat16)

    @pl.when(step < 4)
    def _():
        put(o_own)

    @pl.when(step >= 4)
    def _():
        put(o_oth)


def bwd_kernel(remote, *refs):
    if remote:
        (lo_ref, hi_ref, pq_ref, core_ref, q_own, q_oth, do_own, do_oth, o_own, o_oth, kv_ref,
         segk_ref, segq_ref, lse_ref, dq_out, dk_ref, dv_ref,
         qs, qt, ds_, dt, delta, pm, sm, dqt) = refs
    else:
        (lo_ref, hi_ref, pq_ref, core_ref, q_own, q_oth, do_own, do_oth, o_own, o_oth, kv_ref,
         segk_ref, segq_ref, lse_ref, dq_in, dq_own, dq_oth, dk_ref, dv_ref,
         qs, qt, ds_, dt, delta, pm, sm, dqt) = refs
    step = pl.program_id(0)
    scale = HD ** -0.5
    scale2 = scale * math.log2(math.e)

    @pl.when(step == 0)
    def _():
        dk_ref[...] = jnp.zeros_like(dk_ref)
        dv_ref[...] = jnp.zeros_like(dv_ref)

    lo = lo_ref[step]
    hi = hi_ref[step]
    count = hi - lo + 1

    def prepare(q, do, o):
        stack_heads(q, qs)
        flip_heads(q, qt)
        stack_heads(do, ds_)
        flip_heads(do, dt)
        for h in range(HEADS):
            hc = slice(h * HD, (h + 1) * HD)
            prod = do[:, hc].astype(jnp.float32) * o[:, hc].astype(jnp.float32)
            delta[:, h * BLK:(h + 1) * BLK] = jnp.sum(prod.T, axis=0, keepdims=True)

    @pl.when((step < 4) & (count > 0))
    def _():
        prepare(q_own, do_own, o_own)

    @pl.when((step >= 4) & (count > 0))
    def _():
        prepare(q_oth, do_oth, o_oth)

    if remote:
        dqt[...] = jnp.zeros_like(dqt)
    else:
        dqt[...] = dq_in[0]

    def body(it, carry):
        p = lo + it
        key_start = pl.multiple_of(((p + 4 * core_ref[0]) & 7) * BLK, BLK)
        k_blk = kv_ref[pl.ds(key_start, BLK), :HD]
        v_blk = kv_ref[pl.ds(key_start, BLK), HD:]
        mask = pair_mask(segk_ref, segq_ref, key_start, p, pq_ref[step])
        for h in range(HEADS):
            cols = slice(h * BLK, (h + 1) * BLK)
            s = dot(k_blk, qt[:, cols])
            w = jnp.where(mask, jnp.exp2(s * scale2 - lse_ref[0, :, cols]), 0.0)
            dp = dot(v_blk, dt[:, cols])
            dsv = w * (dp - delta[:, cols])
            pm[:, cols] = w.astype(jnp.bfloat16)
            sm[:, cols] = dsv.astype(jnp.bfloat16)
        dv_ref[pl.ds(key_start, BLK), :] += dot(pm[...], ds_[...])
        dk_ref[pl.ds(key_start, BLK), :] += dot(sm[...], qs[...])
        dqt[...] += dot(k_blk.T, sm[...])
        return carry

    lax.fori_loop(0, count, body, 0)
    if remote:
        dq_out[0] = dqt[...]
    else:
        def put(dst):
            for h in range(HEADS):
                cols = slice(h * BLK, (h + 1) * BLK)
                dst[:, h * HD:(h + 1) * HD] = (dqt[:, cols] * scale).T.astype(jnp.bfloat16)

        @pl.when(step < 4)
        def _():
            put(dq_own)

        @pl.when(step >= 4)
        def _():
            put(dq_oth)


def own_block(i, *_):
    return (jnp.minimum(i, 3), 0)


def oth_block(i, *_):
    return (jnp.maximum(i - 4, 0), 0)


def whole(i, *_):
    return (0, 0)


def lead(i, *_):
    return (i, 0, 0)


def params():
    return pltpu.CompilerParams(dimension_semantics=('arbitrary',), vmem_limit_bytes=VMEM_LIMIT)


def attend(lo, hi, core, q_own, q_oth, kv, segk, segq):
    keys = kv.shape[0]
    tok = q_own.shape[0]
    grid = 2 * tok // BLK
    qspec = [pl.BlockSpec((BLK, HEADS * HD), own_block), pl.BlockSpec((BLK, HEADS * HD), oth_block)]
    return pl.pallas_call(
        fwd_kernel,
        grid_spec=pltpu.PrefetchScalarGridSpec(
            num_scalar_prefetch=3, grid=(grid,),
            in_specs=qspec + [pl.BlockSpec((keys, 2 * HD), whole), pl.BlockSpec((keys, 128), whole),
                              pl.BlockSpec((1, 1, BLK), lead)],
            out_specs=qspec + [pl.BlockSpec((1, 1, WIDE), lead)],
            scratch_shapes=[pltpu.VMEM((HD, WIDE), jnp.bfloat16), pltpu.VMEM((HD, WIDE), jnp.float32),
                            pltpu.VMEM((1, WIDE), jnp.float32), pltpu.VMEM((1, WIDE), jnp.float32)]),
        out_shape=[jax.ShapeDtypeStruct((tok, HEADS * HD), jnp.bfloat16)] * 2
        + [jax.ShapeDtypeStruct((grid, 1, WIDE), jnp.float32)],
        compiler_params=params(), name='attend',
        cost_estimate=pl.CostEstimate(flops=40 * 4 * WIDE * BLK * HD, bytes_accessed=12 << 20, transcendentals=0),
    )(lo, hi, core, q_own, q_oth, kv, segk, segq)


def attend_grad(remote, lo, hi, pq, core, q, do, o, kv, segk, segq, lse, dq_in=None):
    keys = kv.shape[0]
    tok = q[0].shape[0]
    grid = 2 * tok // BLK
    qspec = [pl.BlockSpec((BLK, HEADS * HD), own_block), pl.BlockSpec((BLK, HEADS * HD), oth_block)]
    in_specs = qspec * 3 + [pl.BlockSpec((keys, 2 * HD), whole), pl.BlockSpec((keys, 128), whole),
                            pl.BlockSpec((1, 1, BLK), lead), pl.BlockSpec((1, 1, WIDE), lead)]
    args = [lo, hi, pq, core, *q, *do, *o, kv, segk, segq, lse]
    dqt_spec = pl.BlockSpec((1, HD, WIDE), lead)
    kv_grads = [jax.ShapeDtypeStruct((keys, HD), jnp.float32)] * 2
    kv_specs = [pl.BlockSpec((keys, HD), whole)] * 2
    if remote:
        out_shape = [jax.ShapeDtypeStruct((grid, HD, WIDE), jnp.float32)] + kv_grads
        out_specs = [dqt_spec] + kv_specs
    else:
        in_specs.append(dqt_spec)
        args.append(dq_in)
        out_shape = [jax.ShapeDtypeStruct((tok, HEADS * HD), jnp.bfloat16)] * 2 + kv_grads
        out_specs = qspec + kv_specs
    stack = pltpu.VMEM((WIDE, HD), jnp.bfloat16)
    flip = pltpu.VMEM((HD, WIDE), jnp.bfloat16)
    tile = pltpu.VMEM((BLK, WIDE), jnp.bfloat16)
    return pl.pallas_call(
        functools.partial(bwd_kernel, remote),
        grid_spec=pltpu.PrefetchScalarGridSpec(
            num_scalar_prefetch=4, grid=(grid,), in_specs=in_specs, out_specs=out_specs,
            scratch_shapes=[stack, flip, stack, flip, pltpu.VMEM((1, WIDE), jnp.float32),
                            tile, tile, pltpu.VMEM((HD, WIDE), jnp.float32)]),
        out_shape=out_shape, compiler_params=params(),
        name='attend_grad_remote' if remote else 'attend_grad_local',
        cost_estimate=pl.CostEstimate(flops=20 * 10 * WIDE * BLK * HD, bytes_accessed=20 << 20, transcendentals=0),
    )(*args)


def solution(mesh):
    row_spec = P(('dp', 'cp'), None)
    tok_spec = P(('dp', 'cp'))
    weight_spec = P(None, None, None)
    grad_spec = P(('dp', 'cp'), None, None)
    core_pairs = [(0, 1), (1, 0), (2, 3), (3, 2)]
    chip_pairs = [(0, 2), (2, 0), (1, 3), (3, 1)]
    up_pairs = [(0, 2), (1, 3)]
    down_pairs = [(2, 0), (3, 1)]

    def local_step(x, seg, w_q, w_k, w_v, w_o, dy):
        tok = x.shape[0]
        dim = x.shape[1]
        width = HEADS * HD
        rows = dim // 4
        index = lax.axis_index('cp')
        core = index % 2
        chip = index // 2

        def swap(a):
            return lax.ppermute(a, 'cp', core_pairs)

        def cross(a):
            return lax.ppermute(a, 'cp', chip_pairs)

        x_o = swap(x)
        dy_o = swap(dy)
        seg_all = lax.all_gather(seg, 'cp')

        def heads_of(w, which):
            per = w.shape[1] // 2
            return lax.dynamic_slice_in_dim(w, which * per, per, 1).reshape(dim, per * HD)

        wq_c, wq_p = heads_of(w_q, core), heads_of(w_q, 1 - core)
        wo_c, wo_p = heads_of(w_o, core), heads_of(w_o, 1 - core)
        wkv_c = jnp.concatenate([heads_of(w_k, core), heads_of(w_v, core)], axis=1)
        wkv_p = jnp.concatenate([heads_of(w_k, 1 - core), heads_of(w_v, 1 - core)], axis=1)

        mine0 = lax.dynamic_index_in_dim(seg_all, 2 * chip, 0, False)
        mine1 = lax.dynamic_index_in_dim(seg_all, 2 * chip + 1, 0, False)
        rem0 = jnp.where(chip == 1, seg_all[0], -1)
        rem1 = jnp.where(chip == 1, seg_all[1], -1)
        flip = core == 1
        seg_pos = jnp.concatenate([rem0, rem1, mine0, mine1])
        seg_keys = jnp.concatenate([jnp.where(flip, rem1, rem0), jnp.where(flip, rem0, rem1),
                                    jnp.where(flip, mine1, mine0), jnp.where(flip, mine0, mine1)])
        seg_qry = seg_keys[2 * tok:].reshape(2 * tok // BLK, 1, BLK)
        blocks = jnp.arange(2 * tok // BLK, dtype=jnp.int32)
        pq = HALF + ((blocks + 4 * core) & 7)
        ends = seg_pos.reshape(-1, BLK)[:, -1]
        firsts = seg_qry[:, 0, 0]
        lo = jnp.sum((ends[None, :] < firsts[:, None]).astype(jnp.int32), axis=1).astype(jnp.int32)
        core1 = core.reshape(1).astype(jnp.int32)
        segk = jnp.broadcast_to(seg_keys[:, None], (4 * tok, 128))

        kv_own = dot(x, wkv_c).astype(jnp.bfloat16)
        kv_oth = dot(x_o, wkv_c).astype(jnp.bfloat16)
        kv_loc = jnp.concatenate([kv_own, kv_oth], axis=0)
        kv_rem = lax.ppermute(kv_loc, 'cp', up_pairs)
        q = (dot(x, wq_c).astype(jnp.bfloat16), dot(x_o, wq_c).astype(jnp.bfloat16))
        do = (dot(dy, wo_c).astype(jnp.bfloat16), dot(dy_o, wo_c).astype(jnp.bfloat16))
        kv_all = jnp.concatenate([kv_rem, kv_loc], axis=0)

        o_own, o_oth, lse = attend(lo, pq, core1, q[0], q[1], kv_all, segk, seg_qry)
        o_swap = swap(o_oth)

        def ship(part):
            cols = part.shape[1]

            def block(row_chip, row_core):
                return lax.dynamic_slice(part, ((2 * row_chip + row_core) * rows, 0), (rows, cols))

            far_swap = swap(block(1 - chip, 1 - core))
            far_mine = cross(block(1 - chip, core))
            near_swap = swap(block(chip, 1 - core))
            far_other = cross(far_swap)
            return block(chip, core), far_mine, near_swap, far_other

        def assemble(pieces):
            near, far, near_o, far_o = pieces
            a, b = near + far, near_o + far_o
            return a, b

        def two(a_own, a_oth, b_own, b_oth):
            return dot_tn(a_own, b_own) + dot_tn(a_oth, b_oth)

        wo_pieces = ship(two(dy, dy_o, o_own, o_oth))

        low_hi = jnp.minimum(pq, HALF - 1)
        dq_part, dk_far, dv_far = attend_grad(True, lo, low_hi, pq, core1, q, do, (o_own, o_oth),
                                              kv_rem, segk[:2 * tok], seg_qry, lse)
        dkv_back = lax.ppermute(jnp.concatenate([dk_far, dv_far], axis=1), 'cp', down_pairs)
        y = (dot_nt(o_own, wo_c) + dot_nt(o_swap, wo_p)).astype(jnp.bfloat16)

        dq_own, dq_oth, dk_loc, dv_loc = attend_grad(False, jnp.maximum(lo, HALF), pq, pq, core1, q, do,
                                                     (o_own, o_oth), kv_loc, segk[2 * tok:], seg_qry, lse, dq_part)
        dq_swap = swap(dq_oth)
        wq_pieces = ship(two(x, x_o, dq_own, dq_oth))

        dk = ((dk_loc + dkv_back[:, :HD]) * HD ** -0.5).astype(jnp.bfloat16)
        dv = (dv_loc + dkv_back[:, HD:]).astype(jnp.bfloat16)
        dkv = jnp.concatenate([dk, dv], axis=1)
        dkv_own, dkv_oth = dkv[:tok], dkv[tok:]
        dkv_swap = swap(dkv_oth)
        wkv_pieces = ship(two(x, x_o, dkv_own, dkv_oth))
        dx = (dot_nt(dq_own, wq_c) + dot_nt(dq_swap, wq_p)
              + dot_nt(dkv_own, wkv_c) + dot_nt(dkv_swap, wkv_p)).astype(jnp.bfloat16)

        def join(a, b):
            heads = a.shape[1] // HD
            a3, b3 = a.reshape(rows, heads, HD), b.reshape(rows, heads, HD)
            return jnp.where(flip, jnp.concatenate([b3, a3], axis=1), jnp.concatenate([a3, b3], axis=1))

        dw_q = join(*assemble(wq_pieces))
        dw_o = join(*assemble(wo_pieces))
        kv_a, kv_b = assemble(wkv_pieces)
        dw_k = join(kv_a[:, :HD], kv_b[:, :HD])
        dw_v = join(kv_a[:, HD:], kv_b[:, HD:])
        return y, dx, dw_q, dw_k, dw_v, dw_o

    return jax.shard_map(local_step, mesh=mesh,
                         in_specs=(row_spec, tok_spec, weight_spec, weight_spec, weight_spec, weight_spec, row_spec),
                         out_specs=(row_spec, row_spec, grad_spec, grad_spec, grad_spec, grad_spec),
                         check_vma=False)
```

```python
import functools
import math

import jax
import jax.numpy as jnp
from jax import lax
from jax.experimental import pallas as pl
from jax.experimental.pallas import tpu as pltpu
from jax.sharding import PartitionSpec as P

BLK = 256
HEADS = 6
HD = 128
WIDE = HEADS * BLK
HALF = 8
VMEM_LIMIT = 60 * 1024 * 1024


def dot(a, b):
    return jnp.dot(a, b, preferred_element_type=jnp.float32)


def dot_tn(a, b):
    return lax.dot_general(a, b, (((0,), (0,)), ((), ())), preferred_element_type=jnp.float32)


def dot_nt(a, b):
    return lax.dot_general(a, b, (((1,), (1,)), ((), ())), preferred_element_type=jnp.float32)


def stack_heads(src, dst):
    for h in range(HEADS):
        dst[h * BLK:(h + 1) * BLK, :] = src[:, h * HD:(h + 1) * HD]


def flip_heads(src, dst):
    for h in range(HEADS):
        dst[:, h * BLK:(h + 1) * BLK] = src[:, h * HD:(h + 1) * HD].T


def store_block(p, core):
    return (p & HALF) + ((p + 4 * core) & (HALF - 1))


def first_block(seg_ref, ids_ref, step):
    core, chip = ids_ref[0], ids_ref[1]
    first = seg_ref[(HALF + step) * BLK]
    near = jnp.int32(0)
    far = jnp.int32(0)
    for b in range(HALF):
        far += (seg_ref[b * BLK + BLK - 1] < first).astype(jnp.int32)
        near += (seg_ref[(HALF + b) * BLK + BLK - 1] < first).astype(jnp.int32)
    far = jnp.where(chip == 0, HALF, far)
    return far + near


def spread_segments(rows_ref, dst, first, count):
    for b in range(count):
        row = jnp.broadcast_to(rows_ref[first + b], (128, BLK))
        dst[b * BLK:(b + 1) * BLK, :] = row.T


def pair_mask(segk, segq, key_block, query_block):
    segk = jnp.concatenate([segk] * (BLK // 128), axis=1)
    same = segk == segq
    rel = (lax.broadcasted_iota(jnp.int32, (BLK, BLK), 0)
           - lax.broadcasted_iota(jnp.int32, (BLK, BLK), 1))
    return same & (rel <= (query_block - key_block) * BLK)


def fwd_kernel(seg_ref, ids_ref, q_own, q_oth, kv_far, kv_near, rows_ref,
               o_own, o_oth, lse_ref, segk, kv_ref, qt, acc, m_ref, l_ref, f_ref, pm):
    step = pl.program_id(0)
    core = ids_ref[0]
    scale2 = HD ** -0.5 * math.log2(math.e)

    @pl.when(step == 0)
    def _():
        spread_segments(rows_ref, segk, 0, 2 * HALF)
        kv_ref[:HALF * BLK, :] = kv_far[...]
        kv_ref[HALF * BLK:, :] = kv_near[...]

    @pl.when(step < 4)
    def _():
        flip_heads(q_own, qt)

    @pl.when(step >= 4)
    def _():
        flip_heads(q_oth, qt)

    acc[...] = jnp.zeros_like(acc)
    m_ref[...] = jnp.full_like(m_ref, -jnp.inf)
    l_ref[...] = jnp.zeros_like(l_ref)
    hi = HALF + ((step + 4 * core) & (HALF - 1))
    count = hi - first_block(seg_ref, ids_ref, step) + 1
    segq = rows_ref[HALF + step]

    def body(it, carry):
        p = hi - it
        key_start = pl.multiple_of(store_block(p, core) * BLK, BLK)
        k_blk = kv_ref[pl.ds(key_start, BLK), :HD]
        v_t = kv_ref[pl.ds(key_start, BLK), HD:].T
        mask = pair_mask(segk[pl.ds(key_start, BLK), :], segq, p, hi)
        for h in range(HEADS):
            cols = slice(h * BLK, (h + 1) * BLK)
            s = jnp.where(mask, dot(k_blk, qt[:, cols]) * scale2, -jnp.inf)
            m_old = m_ref[:, cols]
            m_new = jnp.maximum(m_old, jnp.max(s, axis=0, keepdims=True))
            w = jnp.exp2(s - m_new)
            fac = jnp.exp2(m_old - m_new)
            m_ref[:, cols] = m_new
            l_ref[:, cols] = l_ref[:, cols] * fac + jnp.sum(w, axis=0, keepdims=True)
            f_ref[:, cols] = fac
            pm[:, cols] = w.astype(jnp.bfloat16)
        acc[...] = acc[...] * f_ref[...] + dot(v_t, pm[...])
        return carry

    lax.fori_loop(0, count, body, 0)
    total = l_ref[...]
    lse_ref[0] = m_ref[...] + jnp.log2(total)
    inv = 1.0 / total

    def put(dst):
        for h in range(HEADS):
            cols = slice(h * BLK, (h + 1) * BLK)
            dst[:, h * HD:(h + 1) * HD] = (acc[:, cols] * inv[:, cols]).T.astype(jnp.bfloat16)

    @pl.when(step < 4)
    def _():
        put(o_own)

    @pl.when(step >= 4)
    def _():
        put(o_oth)


def bwd_kernel(remote, *refs):
    if remote:
        (seg_ref, ids_ref, q_own, q_oth, do_own, do_oth, o_own, o_oth, kv_ref,
         rows_ref, lse_ref, dq_out, dkv_ref,
         segk, qs, qt, ds_, dt, delta, pm, sm, dqt) = refs
    else:
        (seg_ref, ids_ref, q_own, q_oth, do_own, do_oth, o_own, o_oth, kv_ref,
         rows_ref, lse_ref, dq_in, dq_own, dq_oth, dkv_ref,
         segk, qs, qt, ds_, dt, delta, pm, sm, dqt) = refs
    step = pl.program_id(0)
    core = ids_ref[0]
    scale = HD ** -0.5
    scale2 = scale * math.log2(math.e)

    @pl.when(step == 0)
    def _():
        dkv_ref[...] = jnp.zeros_like(dkv_ref)
        spread_segments(rows_ref, segk, 0 if remote else HALF, HALF)

    query = HALF + ((step + 4 * core) & (HALF - 1))
    first = first_block(seg_ref, ids_ref, step)
    if remote:
        lo, hi = first, jnp.int32(HALF - 1)
    else:
        lo, hi = jnp.maximum(first, HALF), query
    count = hi - lo + 1
    segq = rows_ref[HALF + step]

    def prepare(q, do, o):
        stack_heads(q, qs)
        flip_heads(q, qt)
        stack_heads(do, ds_)
        flip_heads(do, dt)
        for h in range(HEADS):
            hc = slice(h * HD, (h + 1) * HD)
            prod = do[:, hc].astype(jnp.float32) * o[:, hc].astype(jnp.float32)
            delta[:, h * BLK:(h + 1) * BLK] = jnp.sum(prod.T, axis=0, keepdims=True)

    @pl.when((step < 4) & (count > 0))
    def _():
        prepare(q_own, do_own, o_own)

    @pl.when((step >= 4) & (count > 0))
    def _():
        prepare(q_oth, do_oth, o_oth)

    if remote:
        dqt[...] = jnp.zeros_like(dqt)
    else:
        dqt[...] = dq_in[0]

    def body(it, carry):
        p = lo + it
        key_start = pl.multiple_of((store_block(p, core) & (HALF - 1)) * BLK, BLK)
        k_blk = kv_ref[pl.ds(key_start, BLK), :HD]
        v_blk = kv_ref[pl.ds(key_start, BLK), HD:]
        mask = pair_mask(segk[pl.ds(key_start, BLK), :], segq, p, query)
        for h in range(HEADS):
            cols = slice(h * BLK, (h + 1) * BLK)
            s = dot(k_blk, qt[:, cols])
            w = jnp.where(mask, jnp.exp2(s * scale2 - lse_ref[0, :, cols]), 0.0)
            dp = dot(v_blk, dt[:, cols])
            dsv = w * (dp - delta[:, cols])
            pm[:, cols] = w.astype(jnp.bfloat16)
            sm[:, cols] = dsv.astype(jnp.bfloat16)
        dkv_ref[pl.ds(key_start, BLK), HD:] += dot(pm[...], ds_[...])
        dkv_ref[pl.ds(key_start, BLK), :HD] += dot(sm[...], qs[...])
        dqt[...] += dot(k_blk.T, sm[...])
        return carry

    lax.fori_loop(0, count, body, 0)
    if remote:
        dq_out[0] = dqt[...]
    else:
        def put(dst):
            for h in range(HEADS):
                cols = slice(h * BLK, (h + 1) * BLK)
                dst[:, h * HD:(h + 1) * HD] = (dqt[:, cols] * scale).T.astype(jnp.bfloat16)

        @pl.when(step < 4)
        def _():
            put(dq_own)

        @pl.when(step >= 4)
        def _():
            put(dq_oth)


def wgrad_kernel(ids_ref, a_own, a_oth, b_own, b_oth, c_own, c_oth, out_ref, at):
    step = pl.program_id(0)
    half = pl.num_programs(0) // 2
    tok = a_own.shape[0]

    @pl.when(step == 0)
    def _():
        for t in range(0, tok, BLK):
            at[:, t:t + BLK] = a_own[t:t + BLK, :].T
            at[:, tok + t:tok + t + BLK] = a_oth[t:t + BLK, :].T

    @pl.when(step < half)
    def _():
        out_ref[...] = dot(at[:, :tok], b_own[...]) + dot(at[:, tok:], b_oth[...])

    @pl.when(step >= half)
    def _():
        out_ref[...] = dot(at[:, :tok], c_own[...]) + dot(at[:, tok:], c_oth[...])


def own_block(i, *_):
    return (jnp.minimum(i, 3), 0)


def oth_block(i, *_):
    return (jnp.maximum(i - 4, 0), 0)


def whole(i, *_):
    return (0, 0)


def whole3(i, *_):
    return (0, 0, 0)


def lead(i, *_):
    return (i, 0, 0)


def params():
    return pltpu.CompilerParams(dimension_semantics=('arbitrary',), vmem_limit_bytes=VMEM_LIMIT)


def attend(seg, ids, q_own, q_oth, kv_far, kv_near, rows):
    keys = 2 * kv_near.shape[0]
    tok = q_own.shape[0]
    grid = 2 * tok // BLK
    qspec = [pl.BlockSpec((BLK, HEADS * HD), own_block), pl.BlockSpec((BLK, HEADS * HD), oth_block)]
    stat = pltpu.VMEM((1, WIDE), jnp.float32)
    return pl.pallas_call(
        fwd_kernel,
        grid_spec=pltpu.PrefetchScalarGridSpec(
            num_scalar_prefetch=2, grid=(grid,),
            in_specs=qspec + [pl.BlockSpec((keys // 2, 2 * HD), whole)] * 2
            + [pl.BlockSpec((keys // BLK, 1, BLK), whole3)],
            out_specs=qspec + [pl.BlockSpec((1, 1, WIDE), lead)],
            scratch_shapes=[pltpu.VMEM((keys, 128), jnp.int32), pltpu.VMEM((keys, 2 * HD), jnp.bfloat16),
                            pltpu.VMEM((HD, WIDE), jnp.bfloat16), pltpu.VMEM((HD, WIDE), jnp.float32),
                            stat, stat, stat, pltpu.VMEM((BLK, WIDE), jnp.bfloat16)]),
        out_shape=[jax.ShapeDtypeStruct((tok, HEADS * HD), jnp.bfloat16)] * 2
        + [jax.ShapeDtypeStruct((grid, 1, WIDE), jnp.float32)],
        compiler_params=params(), name='attend',
        cost_estimate=pl.CostEstimate(flops=40 * 4 * WIDE * BLK * HD, bytes_accessed=12 << 20, transcendentals=0),
    )(seg, ids, q_own, q_oth, kv_far, kv_near, rows)


def attend_grad(remote, seg, ids, q, do, o, kv, rows, lse, dq_in=None):
    keys = kv.shape[0]
    tok = q[0].shape[0]
    grid = 2 * tok // BLK
    qspec = [pl.BlockSpec((BLK, HEADS * HD), own_block), pl.BlockSpec((BLK, HEADS * HD), oth_block)]
    in_specs = qspec * 3 + [pl.BlockSpec((keys, 2 * HD), whole), pl.BlockSpec(rows.shape, whole3),
                            pl.BlockSpec((1, 1, WIDE), lead)]
    args = [seg, ids, *q, *do, *o, kv, rows, lse]
    dqt_spec = pl.BlockSpec((1, HD, WIDE), lead)
    kv_grad = [jax.ShapeDtypeStruct((keys, 2 * HD), jnp.float32)]
    kv_spec = [pl.BlockSpec((keys, 2 * HD), whole)]
    if remote:
        out_shape = [jax.ShapeDtypeStruct((grid, HD, WIDE), jnp.float32)] + kv_grad
        out_specs = [dqt_spec] + kv_spec
    else:
        in_specs.append(dqt_spec)
        args.append(dq_in)
        out_shape = [jax.ShapeDtypeStruct((tok, HEADS * HD), jnp.bfloat16)] * 2 + kv_grad
        out_specs = qspec + kv_spec
    stack = pltpu.VMEM((WIDE, HD), jnp.bfloat16)
    flip = pltpu.VMEM((HD, WIDE), jnp.bfloat16)
    tile = pltpu.VMEM((BLK, WIDE), jnp.bfloat16)
    return pl.pallas_call(
        functools.partial(bwd_kernel, remote),
        grid_spec=pltpu.PrefetchScalarGridSpec(
            num_scalar_prefetch=2, grid=(grid,), in_specs=in_specs, out_specs=out_specs,
            scratch_shapes=[pltpu.VMEM((keys, 128), jnp.int32), stack, flip, stack, flip,
                            pltpu.VMEM((1, WIDE), jnp.float32),
                            tile, tile, pltpu.VMEM((HD, WIDE), jnp.float32)]),
        out_shape=out_shape, compiler_params=params(),
        name='attend_grad_remote' if remote else 'attend_grad_local',
        cost_estimate=pl.CostEstimate(flops=20 * 10 * WIDE * BLK * HD, bytes_accessed=20 << 20, transcendentals=0),
    )(*args)


def wgrad(where, core, a, b, c):
    tok, dim = a[0].shape
    width = b[0].shape[1]
    rows = dim // 4
    step = min(width, 384)
    half = width // step
    a_spec = pl.BlockSpec((tok, rows), lambda i, ids: (0, ids[0]))
    b_spec = pl.BlockSpec((tok, step), lambda i, ids: (0, jnp.minimum(i, half - 1)))
    c_spec = pl.BlockSpec((tok, step), lambda i, ids: (0, jnp.maximum(i - half, 0)))
    return pl.pallas_call(
        wgrad_kernel,
        grid_spec=pltpu.PrefetchScalarGridSpec(
            num_scalar_prefetch=1, grid=(2 * half,),
            in_specs=[a_spec] * 2 + [b_spec] * 2 + [c_spec] * 2,
            out_specs=pl.BlockSpec((rows, step), lambda i, ids: (0, lax.rem(i + half * ids[1], 2 * half))),
            scratch_shapes=[pltpu.VMEM((rows, 2 * tok), jnp.bfloat16)]),
        out_shape=jax.ShapeDtypeStruct((rows, 2 * width), jnp.float32),
        compiler_params=params(), name='wgrad',
        cost_estimate=pl.CostEstimate(flops=8 * tok * rows * width, bytes_accessed=10 << 20, transcendentals=0),
    )(jnp.stack([where, core]).astype(jnp.int32), *a, *b, *c)


def after(value, *others):
    return lax.optimization_barrier((value, *others))[0]


def solution(mesh):
    row_spec = P(('dp', 'cp'), None)
    tok_spec = P(('dp', 'cp'))
    weight_spec = P(None, None, None)
    grad_spec = P(('dp', 'cp'), None, None)
    core_pairs = [(0, 1), (1, 0), (2, 3), (3, 2)]
    chip_pairs = [(0, 2), (2, 0), (1, 3), (3, 1)]
    up_pairs = [(0, 2), (1, 3)]
    down_pairs = [(2, 0), (3, 1)]

    def local_step(x, seg, w_q, w_k, w_v, w_o, dy):
        tok, dim = x.shape
        rows = dim // 4
        width = HEADS * HD
        index = lax.axis_index('cp')
        core = index % 2
        chip = index // 2
        near_rows = index
        far_rows = 2 * (1 - chip) + core
        ids = jnp.stack([core, chip]).astype(jnp.int32)

        def swap(pair):
            return tuple(lax.ppermute(a, 'cp', core_pairs) for a in pair)

        def mine(w, which, per):
            return lax.dynamic_slice_in_dim(w, which * per, per, 1)

        seg_o = lax.ppermute(seg, 'cp', core_pairs)
        x_o = lax.ppermute(x, 'cp', core_pairs)
        dy_o = lax.ppermute(dy, 'cp', core_pairs)
        seg_near = jnp.concatenate([seg, seg_o])
        seg_far = lax.ppermute(seg_near, 'cp', up_pairs)
        seg_all = jnp.concatenate([seg_far, seg_near])
        seg_rows = seg_all.reshape(-1, 1, BLK)

        w_kv = jnp.stack([w_k, w_v], axis=2).reshape(dim, 4 * HD)
        w_kv = lax.optimization_barrier(w_kv)
        wkv_c = mine(w_kv, core, 2 * HD)
        kv_own = dot(x, wkv_c).astype(jnp.bfloat16)
        w_q = lax.optimization_barrier(after(w_q, kv_own).reshape(dim, 2 * width))
        wq_c = mine(w_q, core, width)
        kv_oth = dot(x_o, wkv_c).astype(jnp.bfloat16)
        kv_near = jnp.concatenate([kv_own, kv_oth], axis=0)
        kv_far = lax.ppermute(kv_near, 'cp', up_pairs)
        w_o = lax.optimization_barrier(after(w_o, kv_near).reshape(dim, 2 * width))
        wo_c = mine(w_o, core, width)
        x_2 = after(x, kv_near)
        dy_2 = after(dy, kv_near)
        q = (dot(x_2, wq_c).astype(jnp.bfloat16), dot(x_o, wq_c).astype(jnp.bfloat16))
        do = (dot(dy_2, wo_c).astype(jnp.bfloat16), dot(dy_o, wo_c).astype(jnp.bfloat16))

        *o, lse = attend(seg_all, ids, q[0], q[1], kv_far, kv_near, seg_rows)
        o_p = swap(o)[::-1]
        dwo_far = wgrad(far_rows, core, (dy, dy_o), o, o_p)
        dwo_in = lax.ppermute(dwo_far, 'cp', chip_pairs)

        lse = after(lse, dwo_far)
        dq_part, dkv_far = attend_grad(True, seg_all, ids, q, do, o, kv_far, seg_rows, lse)
        dkv_in = lax.ppermute(dkv_far, 'cp', down_pairs)
        dq_own, dq_oth, dkv_near = attend_grad(False, seg_all, ids, q, do, o, kv_near, seg_rows, lse, dq_part)
        dq = (dq_own, dq_oth)
        dq_p = swap(dq)[::-1]
        dwq_far = wgrad(far_rows, core, (x, x_o), dq, dq_p)
        dwq_in = lax.ppermute(dwq_far, 'cp', chip_pairs)

        o_2, o_p2 = after(o[0], dwq_far), after(o_p[0], dwq_far)
        dq_2, dq_p2 = after(dq[0], dwq_far), after(dq_p[0], dwq_far)
        y = (dot_nt(o_2, wo_c) + dot_nt(o_p2, mine(w_o, 1 - core, width))).astype(jnp.bfloat16)
        dx = dot_nt(dq_2, wq_c) + dot_nt(dq_p2, mine(w_q, 1 - core, width))
        dwo_near = wgrad(near_rows, core, (dy, after(dy_o, dwq_far)), o, o_p)
        dwq_near = wgrad(near_rows, core, (x, after(x_o, dwq_far)), dq, dq_p)

        dkv = dkv_near + dkv_in
        dkv = jnp.concatenate([dkv[:, :HD] * HD ** -0.5, dkv[:, HD:]], axis=1).astype(jnp.bfloat16)
        dkv = (dkv[:tok], dkv[tok:])
        dkv_p = swap(dkv)[::-1]
        dwkv_far = wgrad(far_rows, core, (x, x_o), dkv, dkv_p)
        dwkv_in = lax.ppermute(dwkv_far, 'cp', chip_pairs)
        dwkv_near = wgrad(near_rows, core, (x, after(x_o, dwkv_far)), dkv, dkv_p)
        dx = (dx + dot_nt(dkv[0], wkv_c) + dot_nt(dkv_p[0], mine(w_kv, 1 - core, 2 * HD))).astype(jnp.bfloat16)

        dw_q = (dwq_near + dwq_in).reshape(rows, 2 * HEADS, HD)
        dw_o = (dwo_near + dwo_in).reshape(rows, 2 * HEADS, HD)
        dw_kv = (dwkv_near + dwkv_in).reshape(rows, 2, 2, HD)
        return y, dx, dw_q, dw_kv[:, :, 0], dw_kv[:, :, 1], dw_o

    return jax.shard_map(local_step, mesh=mesh,
                         in_specs=(row_spec, tok_spec, weight_spec, weight_spec, weight_spec, weight_spec, row_spec),
                         out_specs=(row_spec, row_spec, grad_spec, grad_spec, grad_spec, grad_spec),
                         check_vma=False)
```

```python
import functools
import math

import jax
import jax.numpy as jnp
from jax import lax
from jax.experimental import pallas as pl
from jax.experimental.pallas import tpu as pltpu
from jax.sharding import PartitionSpec as P

BLK = 256
HEADS = 6
HD = 128
WIDE = HEADS * BLK
HALF = 8
VMEM_LIMIT = 60 * 1024 * 1024


def dot(a, b):
    return jnp.dot(a, b, preferred_element_type=jnp.float32)


def dot_nt(a, b):
    return lax.dot_general(a, b, (((1,), (1,)), ((), ())), preferred_element_type=jnp.float32)


def stack_heads(src, dst):
    for h in range(HEADS):
        dst[h * BLK:(h + 1) * BLK, :] = src[:, h * HD:(h + 1) * HD]


def flip_heads(src, dst):
    for h in range(HEADS):
        dst[:, h * BLK:(h + 1) * BLK] = src[:, h * HD:(h + 1) * HD].T


def store_block(p, core):
    return (p & HALF) + ((p + 4 * core) & (HALF - 1))


def first_block(seg_ref, ids_ref, step):
    chip = ids_ref[1]
    first = seg_ref[(HALF + step) * BLK]
    near = jnp.int32(0)
    far = jnp.int32(0)
    for b in range(HALF):
        far += (seg_ref[b * BLK + BLK - 1] < first).astype(jnp.int32)
        near += (seg_ref[(HALF + b) * BLK + BLK - 1] < first).astype(jnp.int32)
    far = jnp.where(chip == 0, HALF, far)
    return far + near


def spread_segments(rows_ref, dst, first, count):
    for b in range(count):
        row = jnp.broadcast_to(rows_ref[first + b], (128, BLK))
        dst[b * BLK:(b + 1) * BLK, :] = row.T


def pair_mask(segk, segq, key_block, query_block):
    segk = jnp.concatenate([segk] * (BLK // 128), axis=1)
    same = segk == segq
    rel = (lax.broadcasted_iota(jnp.int32, (BLK, BLK), 0)
           - lax.broadcasted_iota(jnp.int32, (BLK, BLK), 1))
    return same & (rel <= (query_block - key_block) * BLK)


def fwd_kernel(seg_ref, ids_ref, q_own, q_oth, kv_far, kv_near, rows_ref,
               o_own, o_oth, lse_ref, segk, kv_ref, qt, acc, m_ref, l_ref, f_ref, pm):
    step = pl.program_id(0)
    core = ids_ref[0]
    scale2 = HD ** -0.5 * math.log2(math.e)

    @pl.when(step == 0)
    def _():
        spread_segments(rows_ref, segk, 0, 2 * HALF)
        kv_ref[:HALF * BLK, :] = kv_far[...]
        kv_ref[HALF * BLK:, :] = kv_near[...]

    @pl.when(step < 4)
    def _():
        flip_heads(q_own, qt)

    @pl.when(step >= 4)
    def _():
        flip_heads(q_oth, qt)

    acc[...] = jnp.zeros_like(acc)
    m_ref[...] = jnp.full_like(m_ref, -jnp.inf)
    l_ref[...] = jnp.zeros_like(l_ref)
    hi = HALF + ((step + 4 * core) & (HALF - 1))
    count = hi - first_block(seg_ref, ids_ref, step) + 1
    segq = rows_ref[HALF + step]

    def body(it, carry):
        p = hi - it
        key_start = pl.multiple_of(store_block(p, core) * BLK, BLK)
        k_blk = kv_ref[pl.ds(key_start, BLK), :HD]
        v_t = kv_ref[pl.ds(key_start, BLK), HD:].T
        mask = pair_mask(segk[pl.ds(key_start, BLK), :], segq, p, hi)
        for h in range(HEADS):
            cols = slice(h * BLK, (h + 1) * BLK)
            s = jnp.where(mask, dot(k_blk, qt[:, cols]) * scale2, -jnp.inf)
            m_old = m_ref[:, cols]
            m_new = jnp.maximum(m_old, jnp.max(s, axis=0, keepdims=True))
            w = jnp.exp2(s - m_new)
            fac = jnp.exp2(m_old - m_new)
            m_ref[:, cols] = m_new
            l_ref[:, cols] = l_ref[:, cols] * fac + jnp.sum(w, axis=0, keepdims=True)
            f_ref[:, cols] = fac
            pm[:, cols] = w.astype(jnp.bfloat16)
        acc[...] = acc[...] * f_ref[...] + dot(v_t, pm[...])
        return carry

    lax.fori_loop(0, count, body, 0)
    total = l_ref[...]
    lse_ref[0] = m_ref[...] + jnp.log2(total)
    inv = 1.0 / total

    def put(dst):
        for h in range(HEADS):
            cols = slice(h * BLK, (h + 1) * BLK)
            dst[:, h * HD:(h + 1) * HD] = (acc[:, cols] * inv[:, cols]).T.astype(jnp.bfloat16)

    @pl.when(step < 4)
    def _():
        put(o_own)

    @pl.when(step >= 4)
    def _():
        put(o_oth)


def bwd_kernel(remote, *refs):
    if remote:
        (seg_ref, ids_ref, q_own, q_oth, do_own, do_oth, o_own, o_oth, kv_ref,
         rows_ref, lse_ref, dq_out, dkv_ref,
         segk, qs, qt, ds_, dt, delta, pm, sm, dqt) = refs
    else:
        (seg_ref, ids_ref, q_own, q_oth, do_own, do_oth, o_own, o_oth, kv_ref,
         rows_ref, lse_ref, dq_in, dq_own, dq_oth, dkv_ref,
         segk, qs, qt, ds_, dt, delta, pm, sm, dqt) = refs
    step = pl.program_id(0)
    core = ids_ref[0]
    scale = HD ** -0.5
    scale2 = scale * math.log2(math.e)

    @pl.when(step == 0)
    def _():
        dkv_ref[...] = jnp.zeros_like(dkv_ref)
        spread_segments(rows_ref, segk, 0 if remote else HALF, HALF)

    query = HALF + ((step + 4 * core) & (HALF - 1))
    first = first_block(seg_ref, ids_ref, step)
    if remote:
        lo, hi = first, jnp.int32(HALF - 1)
    else:
        lo, hi = jnp.maximum(first, HALF), query
    count = hi - lo + 1
    segq = rows_ref[HALF + step]

    def prepare(q, do, o):
        stack_heads(q, qs)
        flip_heads(q, qt)
        stack_heads(do, ds_)
        flip_heads(do, dt)
        for h in range(HEADS):
            hc = slice(h * HD, (h + 1) * HD)
            prod = do[:, hc].astype(jnp.float32) * o[:, hc].astype(jnp.float32)
            delta[:, h * BLK:(h + 1) * BLK] = jnp.sum(prod.T, axis=0, keepdims=True)

    @pl.when((step < 4) & (count > 0))
    def _():
        prepare(q_own, do_own, o_own)

    @pl.when((step >= 4) & (count > 0))
    def _():
        prepare(q_oth, do_oth, o_oth)

    if remote:
        dqt[...] = jnp.zeros_like(dqt)
    else:
        dqt[...] = dq_in[0]

    def body(it, carry):
        p = lo + it
        key_start = pl.multiple_of((store_block(p, core) & (HALF - 1)) * BLK, BLK)
        k_blk = kv_ref[pl.ds(key_start, BLK), :HD]
        v_blk = kv_ref[pl.ds(key_start, BLK), HD:]
        mask = pair_mask(segk[pl.ds(key_start, BLK), :], segq, p, query)
        for h in range(HEADS):
            cols = slice(h * BLK, (h + 1) * BLK)
            s = dot(k_blk, qt[:, cols])
            w = jnp.where(mask, jnp.exp2(s * scale2 - lse_ref[0, :, cols]), 0.0)
            dp = dot(v_blk, dt[:, cols])
            dsv = w * (dp - delta[:, cols])
            pm[:, cols] = w.astype(jnp.bfloat16)
            sm[:, cols] = dsv.astype(jnp.bfloat16)
        dkv_ref[pl.ds(key_start, BLK), HD:] += dot(pm[...], ds_[...])
        dkv_ref[pl.ds(key_start, BLK), :HD] += dot(sm[...], qs[...])
        dqt[...] += dot(k_blk.T, sm[...])
        return carry

    lax.fori_loop(0, count, body, 0)
    if remote:
        dq_out[0] = dqt[...]
    else:
        def put(dst):
            for h in range(HEADS):
                cols = slice(h * BLK, (h + 1) * BLK)
                dst[:, h * HD:(h + 1) * HD] = (dqt[:, cols] * scale).T.astype(jnp.bfloat16)

        @pl.when(step < 4)
        def _():
            put(dq_own)

        @pl.when(step >= 4)
        def _():
            put(dq_oth)


def lanes(ref, first, count):
    return jnp.concatenate([ref[first + h] for h in range(count)], axis=1)


def project_kernel(ids_ref, a_ref, w_ref, out_ref, at_ref):
    step = pl.program_id(0)
    out_ref[...] = dot(a_ref[...], lanes(w_ref, 0, 2)).astype(jnp.bfloat16)
    cols = at_ref.shape[0]
    first = pl.multiple_of(step * cols, cols)
    for t in range(0, a_ref.shape[0], BLK):
        at_ref[:, t:t + BLK] = a_ref[t:t + BLK, pl.ds(first, cols)].T


def expand_kernel(ids_ref, a_ref, b_ref, wa_ref, wb_ref, out_ref):
    out_ref[...] = (dot_nt(a_ref[...], lanes(wa_ref, 0, HEADS))
                    + dot_nt(b_ref[...], lanes(wb_ref, 0, HEADS))).astype(jnp.bfloat16)


def expand_kv_kernel(ids_ref, a_ref, b_ref, wa_ref, wb_ref, c_ref, d_ref, wc_ref, wd_ref, out_ref):
    out_ref[...] = (dot_nt(a_ref[...], lanes(wa_ref, 0, HEADS))
                    + dot_nt(b_ref[...], lanes(wb_ref, 0, HEADS))
                    + dot_nt(c_ref[...], wc_ref[...]) + dot_nt(d_ref[...], wd_ref[...])).astype(jnp.bfloat16)


def wgrad_kernel(ids_ref, a_own, a_oth, b_own, b_oth, c_own, c_oth, out_ref):
    step = pl.program_id(0)
    half = pl.num_programs(0) // 2

    def put(own, oth):
        val = dot(a_own[...], own[...]) + dot(a_oth[...], oth[...])
        for h in range(out_ref.shape[0]):
            out_ref[h] = val[:, h * HD:(h + 1) * HD]

    @pl.when(step < half)
    def _():
        put(b_own, b_oth)

    @pl.when(step >= half)
    def _():
        put(c_own, c_oth)


def own_block(i, *_):
    return (jnp.minimum(i, 3), 0)


def oth_block(i, *_):
    return (jnp.maximum(i - 4, 0), 0)


def whole(i, *_):
    return (0, 0)


def whole3(i, *_):
    return (0, 0, 0)


def lead(i, *_):
    return (i, 0, 0)


def params():
    return pltpu.CompilerParams(dimension_semantics=('arbitrary',), vmem_limit_bytes=VMEM_LIMIT)


def attend(seg, ids, q_own, q_oth, kv_far, kv_near, rows):
    keys = 2 * kv_near.shape[0]
    tok = q_own.shape[0]
    grid = 2 * tok // BLK
    qspec = [pl.BlockSpec((BLK, HEADS * HD), own_block), pl.BlockSpec((BLK, HEADS * HD), oth_block)]
    stat = pltpu.VMEM((1, WIDE), jnp.float32)
    return pl.pallas_call(
        fwd_kernel,
        grid_spec=pltpu.PrefetchScalarGridSpec(
            num_scalar_prefetch=2, grid=(grid,),
            in_specs=qspec + [pl.BlockSpec((keys // 2, 2 * HD), whole)] * 2
            + [pl.BlockSpec((keys // BLK, 1, BLK), whole3)],
            out_specs=qspec + [pl.BlockSpec((1, 1, WIDE), lead)],
            scratch_shapes=[pltpu.VMEM((keys, 128), jnp.int32), pltpu.VMEM((keys, 2 * HD), jnp.bfloat16),
                            pltpu.VMEM((HD, WIDE), jnp.bfloat16), pltpu.VMEM((HD, WIDE), jnp.float32),
                            stat, stat, stat, pltpu.VMEM((BLK, WIDE), jnp.bfloat16)]),
        out_shape=[jax.ShapeDtypeStruct((tok, HEADS * HD), jnp.bfloat16)] * 2
        + [jax.ShapeDtypeStruct((grid, 1, WIDE), jnp.float32)],
        compiler_params=params(), name='attend',
        cost_estimate=pl.CostEstimate(flops=40 * 4 * WIDE * BLK * HD, bytes_accessed=12 << 20, transcendentals=0),
    )(seg, ids, q_own, q_oth, kv_far, kv_near, rows)


def attend_grad(remote, seg, ids, q, do, o, kv, rows, lse, dq_in=None):
    keys = kv.shape[0]
    tok = q[0].shape[0]
    grid = 2 * tok // BLK
    qspec = [pl.BlockSpec((BLK, HEADS * HD), own_block), pl.BlockSpec((BLK, HEADS * HD), oth_block)]
    in_specs = qspec * 3 + [pl.BlockSpec((keys, 2 * HD), whole), pl.BlockSpec(rows.shape, whole3),
                            pl.BlockSpec((1, 1, WIDE), lead)]
    args = [seg, ids, *q, *do, *o, kv, rows, lse]
    dqt_spec = pl.BlockSpec((1, HD, WIDE), lead)
    kv_grad = [jax.ShapeDtypeStruct((keys, 2 * HD), jnp.float32)]
    kv_spec = [pl.BlockSpec((keys, 2 * HD), whole)]
    if remote:
        out_shape = [jax.ShapeDtypeStruct((grid, HD, WIDE), jnp.float32)] + kv_grad
        out_specs = [dqt_spec] + kv_spec
    else:
        in_specs.append(dqt_spec)
        args.append(dq_in)
        out_shape = [jax.ShapeDtypeStruct((tok, HEADS * HD), jnp.bfloat16)] * 2 + kv_grad
        out_specs = qspec + kv_spec
    stack = pltpu.VMEM((WIDE, HD), jnp.bfloat16)
    flip = pltpu.VMEM((HD, WIDE), jnp.bfloat16)
    tile = pltpu.VMEM((BLK, WIDE), jnp.bfloat16)
    return pl.pallas_call(
        functools.partial(bwd_kernel, remote),
        grid_spec=pltpu.PrefetchScalarGridSpec(
            num_scalar_prefetch=2, grid=(grid,), in_specs=in_specs, out_specs=out_specs,
            scratch_shapes=[pltpu.VMEM((keys, 128), jnp.int32), stack, flip, stack, flip,
                            pltpu.VMEM((1, WIDE), jnp.float32),
                            tile, tile, pltpu.VMEM((HD, WIDE), jnp.float32)]),
        out_shape=out_shape, compiler_params=params(),
        name='attend_grad_remote' if remote else 'attend_grad_local',
        cost_estimate=pl.CostEstimate(flops=20 * 10 * WIDE * BLK * HD, bytes_accessed=20 << 20, transcendentals=0),
    )(*args)


def project(ids, a, w):
    tok, dim = a.shape
    steps = HEADS // 2
    return pl.pallas_call(
        project_kernel,
        grid_spec=pltpu.PrefetchScalarGridSpec(
            num_scalar_prefetch=1, grid=(steps,),
            in_specs=[pl.BlockSpec((tok, dim), whole),
                      pl.BlockSpec((2, dim, HD), lambda i, ids: (steps * ids[0] + i, 0, 0))],
            out_specs=[pl.BlockSpec((tok, 2 * HD), lambda i, ids: (0, i)),
                       pl.BlockSpec((dim // steps, tok), lambda i, ids: (i, 0))]),
        out_shape=[jax.ShapeDtypeStruct((tok, HEADS * HD), jnp.bfloat16),
                   jax.ShapeDtypeStruct((dim, tok), jnp.bfloat16)],
        compiler_params=params(),
        cost_estimate=pl.CostEstimate(flops=2 * tok * dim * HEADS * HD, bytes_accessed=10 << 20, transcendentals=0),
    )(ids, a, w)


def expand(ids, a, b, w, extra=()):
    tok, width = a.shape
    dim = w.shape[1]
    cols = 512
    act = pl.BlockSpec((tok, width), whole)
    specs = [act, act, pl.BlockSpec((HEADS, cols, HD), lambda i, ids: (ids[0], i, 0)),
             pl.BlockSpec((HEADS, cols, HD), lambda i, ids: (1 - ids[0], i, 0))]
    args = [a, b, w, w]
    if extra:
        c, d, w_kv = extra
        act = pl.BlockSpec((tok, 2 * HD), whole)
        specs += [act, act, pl.BlockSpec((cols, 2 * HD), lambda i, ids: (i, ids[0])),
                  pl.BlockSpec((cols, 2 * HD), lambda i, ids: (i, 1 - ids[0]))]
        args += [c, d, w_kv, w_kv]
    return pl.pallas_call(
        expand_kv_kernel if extra else expand_kernel,
        grid_spec=pltpu.PrefetchScalarGridSpec(
            num_scalar_prefetch=1, grid=(dim // cols,), in_specs=specs,
            out_specs=pl.BlockSpec((tok, cols), lambda i, ids: (0, i))),
        out_shape=jax.ShapeDtypeStruct((tok, dim), jnp.bfloat16),
        compiler_params=params(), name='grad_x' if extra else 'out_y',
        cost_estimate=pl.CostEstimate(flops=4 * tok * dim * width, bytes_accessed=14 << 20, transcendentals=0),
    )(ids, *args)


def wgrad(where, core, a, b, c):
    dim, tok = a[0].shape
    width = b[0].shape[1]
    rows = dim // 4
    step = 256
    half = width // step
    heads = step // HD
    a_spec = pl.BlockSpec((rows, tok), lambda i, ids: (ids[0], 0))
    b_spec = pl.BlockSpec((tok, step), lambda i, ids: (0, jnp.minimum(i, half - 1)))
    c_spec = pl.BlockSpec((tok, step), lambda i, ids: (0, jnp.maximum(i - half, 0)))
    return pl.pallas_call(
        wgrad_kernel,
        grid_spec=pltpu.PrefetchScalarGridSpec(
            num_scalar_prefetch=1, grid=(2 * half,),
            in_specs=[a_spec] * 2 + [b_spec] * 2 + [c_spec] * 2,
            out_specs=pl.BlockSpec((heads, rows, HD), lambda i, ids: (lax.rem(i + half * ids[1], 2 * half), 0, 0))),
        out_shape=jax.ShapeDtypeStruct((2 * width // HD, rows, HD), jnp.float32),
        compiler_params=params(),
        cost_estimate=pl.CostEstimate(flops=8 * tok * rows * width, bytes_accessed=10 << 20, transcendentals=0),
    )(jnp.stack([where, core]).astype(jnp.int32), *a, *b, *c)


def after(value, *others):
    return lax.optimization_barrier((value, *others))[0]


def solution(mesh):
    row_spec = P(('dp', 'cp'), None)
    tok_spec = P(('dp', 'cp'))
    weight_spec = P(None, None, None)
    grad_spec = P(('dp', 'cp'), None, None)
    core_pairs = [(0, 1), (1, 0), (2, 3), (3, 2)]
    chip_pairs = [(0, 2), (2, 0), (1, 3), (3, 1)]
    up_pairs = [(0, 2), (1, 3)]
    down_pairs = [(2, 0), (3, 1)]

    def send(a, pairs):
        return lax.ppermute(a, 'cp', pairs)

    def layer(x, seg, w_q, w_k, w_v, w_o, dy):
        tok, dim = x.shape
        rows = dim // 4
        index = lax.axis_index('cp')
        core = index % 2
        chip = index // 2
        near_rows = index
        far_rows = 2 * (1 - chip) + core
        ids = jnp.stack([core, chip]).astype(jnp.int32)
        w_q = jnp.transpose(w_q, (1, 0, 2))
        w_o = jnp.transpose(w_o, (1, 0, 2))

        def swap(pair):
            return tuple(send(a, core_pairs) for a in pair)[::-1]

        x_o = send(x, core_pairs)
        seg_o = send(seg, core_pairs)
        dy_o = send(dy, core_pairs)
        seg_near = jnp.concatenate([seg, seg_o])
        seg_far = send(seg_near, up_pairs)
        seg_all = jnp.concatenate([seg_far, seg_near])
        seg_rows = seg_all.reshape(-1, 1, BLK)

        w_kv = jnp.stack([w_k, w_v], axis=2).reshape(dim, 4 * HD)
        w_kv = lax.optimization_barrier(w_kv)
        wkv_c = lax.dynamic_slice_in_dim(w_kv, core * 2 * HD, 2 * HD, 1)
        kv_own = dot(x, wkv_c).astype(jnp.bfloat16)
        kv_oth = dot(x_o, wkv_c).astype(jnp.bfloat16)
        kv_near = jnp.concatenate([kv_own, kv_oth], axis=0)
        kv_far = send(kv_near, up_pairs)
        q_own, xt = project(ids, after(x, kv_near), w_q)
        q_oth, xt_o = project(ids, x_o, w_q)
        do_own, dyt = project(ids, dy, w_o)
        do_oth, dyt_o = project(ids, dy_o, w_o)
        q, do, xt, dyt = (q_own, q_oth), (do_own, do_oth), (xt, xt_o), (dyt, dyt_o)

        *o, lse = attend(seg_all, ids, q[0], q[1], kv_far, kv_near, seg_rows)
        o_p = swap(o)
        dwo_far = wgrad(far_rows, core, dyt, o, o_p)
        dwo_in = send(dwo_far, chip_pairs)

        lse = after(lse, dwo_far)
        dq_part, dkv_far = attend_grad(True, seg_all, ids, q, do, o, kv_far, seg_rows, lse)
        dkv_in = send(dkv_far, down_pairs)
        dq_own, dq_oth, dkv_near = attend_grad(False, seg_all, ids, q, do, o, kv_near, seg_rows, lse, dq_part)
        dq = (dq_own, dq_oth)
        dq_p = swap(dq)
        dwq_far = wgrad(far_rows, core, xt, dq, dq_p)
        dwq_in = send(dwq_far, chip_pairs)

        y = expand(ids, after(o[0], dwq_far), o_p[0], w_o)
        dwo_near = wgrad(near_rows, core, (dyt[0], after(dyt[1], dwq_far)), o, o_p)
        dwq_near = wgrad(near_rows, core, (xt[0], after(xt[1], dwq_far)), dq, dq_p)

        dkv = dkv_near + dkv_in
        dkv = jnp.concatenate([dkv[:, :HD] * HD ** -0.5, dkv[:, HD:]], axis=1).astype(jnp.bfloat16)
        dkv = (dkv[:tok], dkv[tok:])
        dkv_p = swap(dkv)
        dwkv_far = wgrad(far_rows, core, xt, dkv, dkv_p)
        dwkv_in = send(dwkv_far, chip_pairs)
        dwkv_near = wgrad(near_rows, core, (xt[0], after(xt[1], dwkv_far)), dkv, dkv_p)
        dx = expand(ids, after(dq[0], dwkv_far), dq_p[0], w_q, (dkv[0], dkv_p[0], w_kv))

        dw_q = jnp.transpose(dwq_near + dwq_in, (1, 0, 2))
        dw_o = jnp.transpose(dwo_near + dwo_in, (1, 0, 2))
        dw_kv = jnp.transpose(dwkv_near + dwkv_in, (1, 0, 2)).reshape(rows, 2, 2, HD)
        return y, dx, dw_q, dw_kv[:, :, 0], dw_kv[:, :, 1], dw_o

    return jax.shard_map(layer, mesh=mesh,
                         in_specs=(row_spec, tok_spec, weight_spec, weight_spec, weight_spec, weight_spec, row_spec),
                         out_specs=(row_spec, row_spec, grad_spec, grad_spec, grad_spec, grad_spec),
                         check_vma=False)
```

```python
import functools
import math

import jax
import jax.numpy as jnp
from jax import lax
from jax.experimental import pallas as pl
from jax.experimental.pallas import tpu as pltpu
from jax.sharding import PartitionSpec as P

BLK = 256
HEADS = 6
HD = 128
WIDE = HEADS * BLK
HALF = 8


def dot(a, b):
    return jnp.dot(a, b, preferred_element_type=jnp.float32)


def dot_nt(a, b):
    return lax.dot_general(a, b, (((1,), (1,)), ((), ())), preferred_element_type=jnp.float32)


def stack_heads(src, dst):
    for h in range(HEADS):
        dst[h * BLK:(h + 1) * BLK, :] = src[:, h * HD:(h + 1) * HD]


def flip_heads(src, dst):
    for h in range(HEADS):
        dst[:, h * BLK:(h + 1) * BLK] = src[:, h * HD:(h + 1) * HD].T


def store_block(p, core):
    return (p & HALF) + ((p + 4 * core) & (HALF - 1))


def first_block(seg_ref, ids_ref, step):
    chip = ids_ref[1]
    first = seg_ref[(HALF + step) * BLK]
    near = jnp.int32(0)
    far = jnp.int32(0)
    for b in range(HALF):
        far += (seg_ref[b * BLK + BLK - 1] < first).astype(jnp.int32)
        near += (seg_ref[(HALF + b) * BLK + BLK - 1] < first).astype(jnp.int32)
    far = jnp.where(chip == 0, HALF, far)
    return far + near


def spread_segments(rows_ref, dst, first, count):
    for b in range(count):
        row = jnp.broadcast_to(rows_ref[first + b], (128, BLK))
        dst[b * BLK:(b + 1) * BLK, :] = row.T


def pair_mask(segk, segq, key_block, query_block):
    segk = jnp.concatenate([segk] * (BLK // 128), axis=1)
    same = segk == segq
    rel = (lax.broadcasted_iota(jnp.int32, (BLK, BLK), 0)
           - lax.broadcasted_iota(jnp.int32, (BLK, BLK), 1))
    return same & (rel <= (query_block - key_block) * BLK)


def full_blocks(seg_ref, ids_ref, step, hi):
    last = seg_ref[(HALF + step) * BLK + BLK - 1]
    count = jnp.int32(0)
    for p in range(2 * HALF):
        same = seg_ref[store_block(p, ids_ref[0]) * BLK] == last
        count += (same & (p < hi)).astype(jnp.int32)
    return count


def fwd_kernel(seg_ref, ids_ref, q_own, q_oth, kv_far0, kv_far1, kv_own, kv_oth, rows_ref,
               o_own, o_oth, lse_ref, segk, kv_ref, qt, acc, m_ref, l_ref, pm):
    step = pl.program_id(0)
    core = ids_ref[0]
    scale2 = HD ** -0.5 * math.log2(math.e)
    tok = kv_own.shape[0]

    @pl.when(step == 0)
    def _():
        spread_segments(rows_ref, segk, 0, 2 * HALF)
        for i, part in enumerate((kv_far0, kv_far1, kv_own, kv_oth)):
            kv_ref[i * tok:(i + 1) * tok, :] = part[...]

    @pl.when(step < 4)
    def _():
        flip_heads(q_own, qt)

    @pl.when(step >= 4)
    def _():
        flip_heads(q_oth, qt)

    hi = HALF + ((step + 4 * core) & (HALF - 1))
    lo = first_block(seg_ref, ids_ref, step)
    full = jnp.maximum(hi - full_blocks(seg_ref, ids_ref, step, hi), lo)
    segq = rows_ref[HALF + step]

    def start_of(p):
        return pl.multiple_of(store_block(p, core) * BLK, BLK)

    def fold(w):
        return jnp.sum(w.reshape(BLK // 8, 8, BLK), axis=0)

    def keys(start):
        return kv_ref[pl.ds(start, BLK), :HD]

    def values(start):
        return kv_ref[pl.ds(pl.multiple_of(start, BLK), BLK), HD:].T

    def mask_of(start, p):
        return pair_mask(segk[pl.ds(start, BLK), :], segq, p, hi)

    def diagonal():
        start = start_of(hi)
        mask = mask_of(start, hi)
        for h in range(HEADS):
            cols = slice(h * BLK, (h + 1) * BLK)
            s = jnp.where(mask, dot(keys(start), qt[:, cols]) * scale2, -jnp.inf)
            top = jnp.max(s, axis=0, keepdims=True)
            w = jnp.exp2(s - top)
            m_ref[:, cols] = top
            l_ref[:, cols] = fold(w)
            pm[:, cols] = w.astype(jnp.bfloat16)
        acc[...] = jnp.zeros_like(acc)
        return start

    def weigh(p, prev, masked):
        start = start_of(p)
        v_t = values(prev)
        k_blk = keys(start)
        if masked:
            mask = mask_of(start, p)
        for h in range(HEADS):
            cols = slice(h * BLK, (h + 1) * BLK)
            s = dot(k_blk, qt[:, cols]) * scale2 - m_ref[:, cols]
            acc[:, cols] += dot(v_t, pm[:, cols])
            if masked:
                s = jnp.where(mask, s, -jnp.inf)
            w = jnp.exp2(s)
            l_ref[:, cols] += fold(w)
            pm[:, cols] = w.astype(jnp.bfloat16)
        return start

    prev = diagonal()
    prev = lax.fori_loop(0, hi - full, lambda i, c: weigh(hi - 1 - i, c, False), prev)
    prev = lax.fori_loop(0, full - lo, lambda i, c: weigh(full - 1 - i, c, True), prev)
    acc[...] += dot(values(prev), pm[...])

    @pl.when(jnp.logical_not(jnp.max(l_ref[...]) <= 2.0 ** 20))
    def _():
        def safe(i, carry):
            p = hi - 1 - i
            start = start_of(p)
            mask = mask_of(start, p)
            for h in range(HEADS):
                cols = slice(h * BLK, (h + 1) * BLK)
                s = jnp.where(mask, dot(keys(start), qt[:, cols]) * scale2, -jnp.inf)
                top = jnp.maximum(m_ref[:, cols], jnp.max(s, axis=0, keepdims=True))
                fac = jnp.exp2(m_ref[:, cols] - top)
                w = jnp.exp2(s - top)
                m_ref[:, cols] = top
                l_ref[:, cols] = l_ref[:, cols] * fac + fold(w)
                acc[:, cols] = acc[:, cols] * fac + dot(values(start), w.astype(jnp.bfloat16))
            return carry

        first = diagonal()
        acc[...] += dot(values(first), pm[...])
        lax.fori_loop(0, hi - lo, safe, 0)

    total = jnp.sum(l_ref[...], axis=0, keepdims=True)
    lse_ref[0] = m_ref[...] + jnp.log2(total)
    inv = 1.0 / total

    def put(dst):
        for h in range(HEADS):
            cols = slice(h * BLK, (h + 1) * BLK)
            dst[:, h * HD:(h + 1) * HD] = (acc[:, cols] * inv[:, cols]).T.astype(jnp.bfloat16)

    @pl.when(step < 4)
    def _():
        put(o_own)

    @pl.when(step >= 4)
    def _():
        put(o_oth)


def bwd_kernel(remote, *refs):
    if remote:
        (seg_ref, ids_ref, q_own, q_oth, do_own, do_oth, o_own, o_oth, kv_ref,
         rows_ref, lse_ref, dq_out, dkv_ref,
         segk, qs, qt, ds_, dt, delta, pm, sm, dqt) = refs
    else:
        (seg_ref, ids_ref, q_own, q_oth, do_own, do_oth, o_own, o_oth, kv_ref,
         rows_ref, lse_ref, dq_in, dq_own, dq_oth, dkv_ref,
         segk, qs, qt, ds_, dt, delta, pm, sm, dqt) = refs
    step = pl.program_id(0)
    core = ids_ref[0]
    scale = HD ** -0.5
    scale2 = scale * math.log2(math.e)

    @pl.when(step == 0)
    def _():
        dkv_ref[...] = jnp.zeros_like(dkv_ref)
        spread_segments(rows_ref, segk, 0 if remote else HALF, HALF)

    query = HALF + ((step + 4 * core) & (HALF - 1))
    first = first_block(seg_ref, ids_ref, step)
    if remote:
        lo, hi = first, jnp.int32(HALF - 1)
    else:
        lo, hi = jnp.maximum(first, HALF), query
    count = hi - lo + 1
    segq = rows_ref[HALF + step]

    def prepare(q, do, o):
        stack_heads(q, qs)
        flip_heads(q, qt)
        stack_heads(do, ds_)
        flip_heads(do, dt)
        for h in range(HEADS):
            hc = slice(h * HD, (h + 1) * HD)
            prod = do[:, hc].astype(jnp.float32) * o[:, hc].astype(jnp.float32)
            delta[:, h * BLK:(h + 1) * BLK] = jnp.sum(prod.T, axis=0, keepdims=True)

    @pl.when((step < 4) & (count > 0))
    def _():
        prepare(q_own, do_own, o_own)

    @pl.when((step >= 4) & (count > 0))
    def _():
        prepare(q_oth, do_oth, o_oth)

    if remote:
        dqt[...] = jnp.zeros_like(dqt)
    else:
        dqt[...] = dq_in[0]

    def body(it, carry):
        p = lo + it
        key_start = pl.multiple_of((store_block(p, core) & (HALF - 1)) * BLK, BLK)
        k_blk = kv_ref[pl.ds(key_start, BLK), :HD]
        v_blk = kv_ref[pl.ds(key_start, BLK), HD:]
        mask = pair_mask(segk[pl.ds(key_start, BLK), :], segq, p, query)
        for h in range(HEADS):
            cols = slice(h * BLK, (h + 1) * BLK)
            s = dot(k_blk, qt[:, cols])
            w = jnp.where(mask, jnp.exp2(s * scale2 - lse_ref[0, :, cols]), 0.0)
            dp = dot(v_blk, dt[:, cols])
            dsv = w * (dp - delta[:, cols])
            pm[:, cols] = w.astype(jnp.bfloat16)
            sm[:, cols] = dsv.astype(jnp.bfloat16)
        dkv_ref[pl.ds(key_start, BLK), HD:] += dot(pm[...], ds_[...])
        dkv_ref[pl.ds(key_start, BLK), :HD] += dot(sm[...], qs[...])
        dqt[...] += dot(k_blk.T, sm[...])
        return carry

    lax.fori_loop(0, count, body, 0)
    if remote:
        dq_out[0] = dqt[...]
    else:
        def put(dst):
            for h in range(HEADS):
                cols = slice(h * BLK, (h + 1) * BLK)
                dst[:, h * HD:(h + 1) * HD] = (dqt[:, cols] * scale).T.astype(jnp.bfloat16)

        @pl.when(step < 4)
        def _():
            put(dq_own)

        @pl.when(step >= 4)
        def _():
            put(dq_oth)


def lanes(ref, first, count):
    return jnp.concatenate([ref[first + h] for h in range(count)], axis=1)


def project_kernel(ids_ref, a_ref, w_ref, out_ref, at_ref):
    step = pl.program_id(0)
    out_ref[...] = dot(a_ref[...], lanes(w_ref, 0, 2)).astype(jnp.bfloat16)
    cols = at_ref.shape[0]
    first = pl.multiple_of(step * cols, cols)
    for t in range(0, a_ref.shape[0], BLK):
        at_ref[:, t:t + BLK] = a_ref[t:t + BLK, pl.ds(first, cols)].T


def project_kv_kernel(ids_ref, a_ref, wk_ref, wv_ref, out_ref, mine_ref, other_ref, wide):
    @pl.when(pl.program_id(0) == 0)
    def _():
        dim = mine_ref.shape[0]
        for i, ref in enumerate((wk_ref, wv_ref)):
            wide[...] = ref[...].astype(jnp.float32)
            cols = slice(i * HD, (i + 1) * HD)
            mine_ref[:, cols] = wide[pl.ds(ids_ref[0], dim, stride=2), :].astype(jnp.bfloat16)
            other_ref[:, cols] = wide[pl.ds(1 - ids_ref[0], dim, stride=2), :].astype(jnp.bfloat16)

    out_ref[...] = dot(a_ref[...], mine_ref[...]).astype(jnp.bfloat16)


def expand_kernel(ids_ref, a_ref, b_ref, wa_ref, wb_ref, out_ref):
    out_ref[...] = (dot_nt(a_ref[...], lanes(wa_ref, 0, HEADS))
                    + dot_nt(b_ref[...], lanes(wb_ref, 0, HEADS))).astype(jnp.bfloat16)


def expand_kv_kernel(ids_ref, a_ref, b_ref, wa_ref, wb_ref, c_ref, d_ref, wc_ref, wd_ref, out_ref):
    out_ref[...] = (dot_nt(a_ref[...], lanes(wa_ref, 0, HEADS))
                    + dot_nt(b_ref[...], lanes(wb_ref, 0, HEADS))
                    + dot_nt(c_ref[...], wc_ref[...]) + dot_nt(d_ref[...], wd_ref[...])).astype(jnp.bfloat16)


def wgrad_kernel(ids_ref, a_own, a_oth, b_own, b_oth, c_own, c_oth, out_ref):
    step = pl.program_id(0)
    half = pl.num_programs(0) // 2

    def put(own, oth):
        val = dot(a_own[...], own[...]) + dot(a_oth[...], oth[...])
        for h in range(out_ref.shape[0]):
            out_ref[h] = val[:, h * HD:(h + 1) * HD]

    @pl.when(step < half)
    def _():
        put(b_own, b_oth)

    @pl.when(step >= half)
    def _():
        put(c_own, c_oth)


def own_block(i, *_):
    return (jnp.minimum(i, 3), 0)


def oth_block(i, *_):
    return (jnp.maximum(i - 4, 0), 0)


def whole(i, *_):
    return (0, 0)


def whole3(i, *_):
    return (0, 0, 0)


def lead(i, *_):
    return (i, 0, 0)


def params(mib):
    return pltpu.CompilerParams(dimension_semantics=('arbitrary',), vmem_limit_bytes=mib * 1024 * 1024)


def attend(seg, ids, q_own, q_oth, kv_far, kv_near, rows):
    tok = q_own.shape[0]
    keys = 4 * tok
    grid = 2 * tok // BLK
    qspec = [pl.BlockSpec((BLK, HEADS * HD), own_block), pl.BlockSpec((BLK, HEADS * HD), oth_block)]
    stat = pltpu.VMEM((1, WIDE), jnp.float32)
    return pl.pallas_call(
        fwd_kernel,
        grid_spec=pltpu.PrefetchScalarGridSpec(
            num_scalar_prefetch=2, grid=(grid,),
            in_specs=qspec + [pl.BlockSpec((tok, 2 * HD), whole)] * 4
            + [pl.BlockSpec((keys // BLK, 1, BLK), whole3)],
            out_specs=qspec + [pl.BlockSpec((1, 1, WIDE), lead)],
            scratch_shapes=[pltpu.VMEM((keys, 128), jnp.int32), pltpu.VMEM((keys, 2 * HD), jnp.bfloat16),
                            pltpu.VMEM((HD, WIDE), jnp.bfloat16), pltpu.VMEM((HD, WIDE), jnp.float32),
                            stat, pltpu.VMEM((8, WIDE), jnp.float32), pltpu.VMEM((BLK, WIDE), jnp.bfloat16)]),
        out_shape=[jax.ShapeDtypeStruct((tok, HEADS * HD), jnp.bfloat16)] * 2
        + [jax.ShapeDtypeStruct((grid, 1, WIDE), jnp.float32)],
        compiler_params=params(28), name='attend',
        cost_estimate=pl.CostEstimate(flops=40 * 4 * WIDE * BLK * HD, bytes_accessed=12 << 20, transcendentals=0),
    )(seg, ids, q_own, q_oth, *kv_far, *kv_near, rows)


def attend_grad(remote, seg, ids, q, do, o, kv, rows, lse, dq_in=None):
    keys = kv.shape[0]
    tok = q[0].shape[0]
    grid = 2 * tok // BLK
    qspec = [pl.BlockSpec((BLK, HEADS * HD), own_block), pl.BlockSpec((BLK, HEADS * HD), oth_block)]
    in_specs = qspec * 3 + [pl.BlockSpec((keys, 2 * HD), whole), pl.BlockSpec(rows.shape, whole3),
                            pl.BlockSpec((1, 1, WIDE), lead)]
    args = [seg, ids, *q, *do, *o, kv, rows, lse]
    dqt_spec = pl.BlockSpec((1, HD, WIDE), lead)
    kv_grad = [jax.ShapeDtypeStruct((keys, 2 * HD), jnp.float32)]
    kv_spec = [pl.BlockSpec((keys, 2 * HD), whole)]
    if remote:
        out_shape = [jax.ShapeDtypeStruct((grid, HD, WIDE), jnp.float32)] + kv_grad
        out_specs = [dqt_spec] + kv_spec
    else:
        in_specs.append(dqt_spec)
        args.append(dq_in)
        out_shape = [jax.ShapeDtypeStruct((tok, HEADS * HD), jnp.bfloat16)] * 2 + kv_grad
        out_specs = qspec + kv_spec
    stack = pltpu.VMEM((WIDE, HD), jnp.bfloat16)
    flip = pltpu.VMEM((HD, WIDE), jnp.bfloat16)
    tile = pltpu.VMEM((BLK, WIDE), jnp.bfloat16)
    return pl.pallas_call(
        functools.partial(bwd_kernel, remote),
        grid_spec=pltpu.PrefetchScalarGridSpec(
            num_scalar_prefetch=2, grid=(grid,), in_specs=in_specs, out_specs=out_specs,
            scratch_shapes=[pltpu.VMEM((keys, 128), jnp.int32), stack, flip, stack, flip,
                            pltpu.VMEM((1, WIDE), jnp.float32),
                            tile, tile, pltpu.VMEM((HD, WIDE), jnp.float32)]),
        out_shape=out_shape, compiler_params=params(36),
        name='attend_grad_remote' if remote else 'attend_grad_local',
        cost_estimate=pl.CostEstimate(flops=20 * 10 * WIDE * BLK * HD, bytes_accessed=20 << 20, transcendentals=0),
    )(*args)


def project(ids, a, w):
    tok, dim = a.shape
    steps = HEADS // 2
    return pl.pallas_call(
        project_kernel,
        grid_spec=pltpu.PrefetchScalarGridSpec(
            num_scalar_prefetch=1, grid=(steps,),
            in_specs=[pl.BlockSpec((tok, dim), whole),
                      pl.BlockSpec((2, dim, HD), lambda i, ids: (steps * ids[0] + i, 0, 0))],
            out_specs=[pl.BlockSpec((tok, 2 * HD), lambda i, ids: (0, i)),
                       pl.BlockSpec((dim // steps, tok), lambda i, ids: (i, 0))]),
        out_shape=[jax.ShapeDtypeStruct((tok, HEADS * HD), jnp.bfloat16),
                   jax.ShapeDtypeStruct((dim, tok), jnp.bfloat16)],
        compiler_params=params(16),
        cost_estimate=pl.CostEstimate(flops=2 * tok * dim * HEADS * HD, bytes_accessed=10 << 20, transcendentals=0),
    )(ids, a, w)


def project_kv(ids, a, w_k, w_v):
    tok, dim = a.shape
    mine = jax.ShapeDtypeStruct((dim, 2 * HD), jnp.bfloat16)
    pack = pl.BlockSpec((2 * dim, HD), whole)
    return pl.pallas_call(
        project_kv_kernel,
        grid_spec=pltpu.PrefetchScalarGridSpec(
            num_scalar_prefetch=1, grid=(2,),
            in_specs=[pl.BlockSpec((tok // 2, dim), lambda i, ids: (i, 0)), pack, pack],
            out_specs=[pl.BlockSpec((tok // 2, 2 * HD), lambda i, ids: (i, 0))]
            + [pl.BlockSpec((dim, 2 * HD), whole)] * 2,
            scratch_shapes=[pltpu.VMEM((2 * dim, HD), jnp.float32)]),
        out_shape=[jax.ShapeDtypeStruct((tok, 2 * HD), jnp.bfloat16), mine, mine],
        compiler_params=params(20), name='project_kv',
        cost_estimate=pl.CostEstimate(flops=4 * tok * dim * HD, bytes_accessed=6 << 20, transcendentals=0),
    )(ids, a, w_k.reshape(2 * dim, HD), w_v.reshape(2 * dim, HD))


def expand(ids, a, b, w, extra=()):
    tok, width = a.shape
    dim = w.shape[1]
    cols = 512
    act = pl.BlockSpec((tok, width), whole)
    specs = [act, act, pl.BlockSpec((HEADS, cols, HD), lambda i, ids: (ids[0], i, 0)),
             pl.BlockSpec((HEADS, cols, HD), lambda i, ids: (1 - ids[0], i, 0))]
    args = [a, b, w, w]
    if extra:
        act = pl.BlockSpec((tok, 2 * HD), whole)
        specs += [act, act] + [pl.BlockSpec((cols, 2 * HD), lambda i, ids: (i, 0))] * 2
        args += extra
    return pl.pallas_call(
        expand_kv_kernel if extra else expand_kernel,
        grid_spec=pltpu.PrefetchScalarGridSpec(
            num_scalar_prefetch=1, grid=(dim // cols,), in_specs=specs,
            out_specs=pl.BlockSpec((tok, cols), lambda i, ids: (0, i))),
        out_shape=jax.ShapeDtypeStruct((tok, dim), jnp.bfloat16),
        compiler_params=params(20), name='grad_x' if extra else 'out_y',
        cost_estimate=pl.CostEstimate(flops=4 * tok * dim * width, bytes_accessed=14 << 20, transcendentals=0),
    )(ids, *args)


def wgrad(where, core, a, b, c):
    dim, tok = a[0].shape
    width = b[0].shape[1]
    rows = dim // 4
    step = 256
    half = width // step
    heads = step // HD
    a_spec = pl.BlockSpec((rows, tok), lambda i, ids: (ids[0], 0))
    b_spec = pl.BlockSpec((tok, step), lambda i, ids: (0, jnp.minimum(i, half - 1)))
    c_spec = pl.BlockSpec((tok, step), lambda i, ids: (0, jnp.maximum(i - half, 0)))
    return pl.pallas_call(
        wgrad_kernel,
        grid_spec=pltpu.PrefetchScalarGridSpec(
            num_scalar_prefetch=1, grid=(2 * half,),
            in_specs=[a_spec] * 2 + [b_spec] * 2 + [c_spec] * 2,
            out_specs=pl.BlockSpec((heads, rows, HD), lambda i, ids: (lax.rem(i + half * ids[1], 2 * half), 0, 0))),
        out_shape=jax.ShapeDtypeStruct((2 * width // HD, rows, HD), jnp.float32),
        compiler_params=params(16),
        cost_estimate=pl.CostEstimate(flops=8 * tok * rows * width, bytes_accessed=10 << 20, transcendentals=0),
    )(jnp.stack([where, core]).astype(jnp.int32), *a, *b, *c)


def after(value, *others):
    return lax.optimization_barrier((value, *others))[0]


def solution(mesh):
    row_spec = P(('dp', 'cp'), None)
    tok_spec = P(('dp', 'cp'))
    weight_spec = P(None, None, None)
    grad_spec = P(('dp', 'cp'), None, None)
    core_pairs = [(0, 1), (1, 0), (2, 3), (3, 2)]
    chip_pairs = [(0, 2), (2, 0), (1, 3), (3, 1)]
    up_pairs = [(0, 2), (1, 3)]
    down_pairs = [(2, 0), (3, 1)]

    def send(a, pairs):
        return lax.ppermute(a, 'cp', pairs)

    def layer(x, seg, w_q, w_k, w_v, w_o, dy):
        tok, dim = x.shape
        rows = dim // 4
        index = lax.axis_index('cp')
        core = index % 2
        chip = index // 2
        near_rows = index
        far_rows = 2 * (1 - chip) + core
        ids = jnp.stack([core, chip]).astype(jnp.int32)
        w_q = jnp.transpose(w_q, (1, 0, 2))
        w_o = jnp.transpose(w_o, (1, 0, 2))

        def swap(pair):
            return tuple(send(a, core_pairs) for a in pair)[::-1]

        x_o = send(x, core_pairs)
        seg_o = send(seg, core_pairs)
        kv_own, wkv_c, wkv_p = project_kv(ids, x, w_k, w_v)
        kv_far0 = send(kv_own, up_pairs)
        kv_oth = dot(x_o, wkv_c).astype(jnp.bfloat16)
        kv_far1 = send(kv_oth, up_pairs)
        dy_o = send(after(dy, kv_own), core_pairs)
        seg_near = jnp.concatenate([seg, seg_o])
        seg_far = send(seg_near, up_pairs)
        seg_all = jnp.concatenate([seg_far, seg_near])
        seg_rows = seg_all.reshape(-1, 1, BLK)
        kv_far, kv_near = (kv_far0, kv_far1), (kv_own, kv_oth)
        q_own, xt = project(ids, after(x, kv_own), w_q)
        q_oth, xt_o = project(ids, after(x_o, kv_oth), w_q)
        q, xt = (q_own, q_oth), (xt, xt_o)

        *o, lse = attend(seg_all, ids, q[0], q[1], kv_far, kv_near, seg_rows)
        o_p = swap(o)
        do_own, dyt = project(ids, after(dy, o[0]), w_o)
        do_oth, dyt_o = project(ids, after(dy_o, o[0]), w_o)
        do, dyt = (do_own, do_oth), (dyt, dyt_o)
        dwo_far = wgrad(far_rows, core, dyt, o, o_p)
        dwo_in = send(dwo_far, chip_pairs)

        lse = after(lse, dwo_far)
        dq_part, dkv_far = attend_grad(True, seg_all, ids, q, do, o, jnp.concatenate(kv_far), seg_rows, lse)
        dkv_in = send(dkv_far, down_pairs)
        dq_own, dq_oth, dkv_near = attend_grad(False, seg_all, ids, q, do, o, jnp.concatenate(kv_near), seg_rows, lse, dq_part)
        dq = (dq_own, dq_oth)
        dq_p = swap(dq)
        dwq_far = wgrad(far_rows, core, xt, dq, dq_p)
        dwq_in = send(dwq_far, chip_pairs)

        y = expand(ids, after(o[0], dwq_far), o_p[0], w_o)
        dwo_near = wgrad(near_rows, core, (dyt[0], after(dyt[1], dwq_far)), o, o_p)
        dwq_near = wgrad(near_rows, core, (xt[0], after(xt[1], dwq_far)), dq, dq_p)

        dkv = dkv_near + dkv_in
        dkv = jnp.concatenate([dkv[:, :HD] * HD ** -0.5, dkv[:, HD:]], axis=1).astype(jnp.bfloat16)
        dkv = (dkv[:tok], dkv[tok:])
        dkv_p = swap(dkv)
        dwkv_far = wgrad(far_rows, core, xt, dkv, dkv_p)
        dwkv_in = send(dwkv_far, chip_pairs)
        dwkv_near = wgrad(near_rows, core, (xt[0], after(xt[1], dwkv_far)), dkv, dkv_p)
        dx = expand(ids, after(dq[0], dwkv_far), dq_p[0], w_q, (dkv[0], dkv_p[0], wkv_c, wkv_p))

        dw_q = jnp.transpose(dwq_near + dwq_in, (1, 0, 2))
        dw_o = jnp.transpose(dwo_near + dwo_in, (1, 0, 2))
        dw_kv = jnp.transpose(dwkv_near + dwkv_in, (1, 0, 2)).reshape(rows, 2, 2, HD)
        return y, dx, dw_q, dw_kv[:, :, 0], dw_kv[:, :, 1], dw_o

    return jax.shard_map(layer, mesh=mesh,
                         in_specs=(row_spec, tok_spec, weight_spec, weight_spec, weight_spec, weight_spec, row_spec),
                         out_specs=(row_spec, row_spec, grad_spec, grad_spec, grad_spec, grad_spec),
                         check_vma=False)
```

```python
import functools
import math

import jax
import jax.numpy as jnp
from jax import lax
from jax.experimental import pallas as pl
from jax.experimental.pallas import tpu as pltpu
from jax.sharding import PartitionSpec as P

BLK = 256
HEADS = 6
HD = 128
WIDE = HEADS * BLK
HALF = 8


def dot(a, b):
    return jnp.dot(a, b, preferred_element_type=jnp.float32)


def dot_nt(a, b):
    return lax.dot_general(a, b, (((1,), (1,)), ((), ())), preferred_element_type=jnp.float32)


def stack_heads(src, dst):
    for h in range(HEADS):
        dst[h * BLK:(h + 1) * BLK, :] = src[:, h * HD:(h + 1) * HD]


def flip_heads(src, dst):
    for h in range(HEADS):
        dst[:, h * BLK:(h + 1) * BLK] = src[:, h * HD:(h + 1) * HD].T


def store_block(p, core):
    return (p & HALF) + ((p + 4 * core) & (HALF - 1))


def first_block(seg_ref, ids_ref, step):
    chip = ids_ref[1]
    first = seg_ref[(HALF + step) * BLK]
    near = jnp.int32(0)
    far = jnp.int32(0)
    for b in range(HALF):
        far += (seg_ref[b * BLK + BLK - 1] < first).astype(jnp.int32)
        near += (seg_ref[(HALF + b) * BLK + BLK - 1] < first).astype(jnp.int32)
    far = jnp.where(chip == 0, HALF, far)
    return far + near


def spread_segments(rows_ref, dst, first, count):
    for b in range(count):
        row = jnp.broadcast_to(rows_ref[first + b], (128, BLK))
        dst[b * BLK:(b + 1) * BLK, :] = row.T


def pair_mask(segk, segq, key_block, query_block):
    segk = jnp.concatenate([segk] * (BLK // 128), axis=1)
    same = segk == segq
    rel = (lax.broadcasted_iota(jnp.int32, (BLK, BLK), 0)
           - lax.broadcasted_iota(jnp.int32, (BLK, BLK), 1))
    return same & (rel <= (query_block - key_block) * BLK)


def full_blocks(seg_ref, ids_ref, step, hi):
    last = seg_ref[(HALF + step) * BLK + BLK - 1]
    count = jnp.int32(0)
    for p in range(2 * HALF):
        same = seg_ref[store_block(p, ids_ref[0]) * BLK] == last
        count += (same & (p < hi)).astype(jnp.int32)
    return count


def fwd_kernel(seg_ref, ids_ref, q_ref, kv_far0, kv_far1, kv_own, kv_oth, rows_ref, o_ref, lse_ref,
               segk, kv_ref, qt, acc, m_ref, l_ref, pm):
    step = pl.program_id(0)
    core = ids_ref[0]
    scale2 = HD ** -0.5 * math.log2(math.e)
    tok = kv_own.shape[0]

    @pl.when(step == 0)
    def _():
        spread_segments(rows_ref, segk, 0, 2 * HALF)
        for i, part in enumerate((kv_far0, kv_far1, kv_own, kv_oth)):
            kv_ref[i * tok:(i + 1) * tok, :] = part[...]

    flip_heads(q_ref, qt)
    hi = HALF + ((step + 4 * core) & (HALF - 1))
    lo = first_block(seg_ref, ids_ref, step)
    full = jnp.maximum(hi - full_blocks(seg_ref, ids_ref, step, hi), lo)
    segq = rows_ref[HALF + step]

    def start_of(p):
        return pl.multiple_of(store_block(p, core) * BLK, BLK)

    def fold(w):
        return jnp.sum(w.reshape(BLK // 8, 8, BLK), axis=0)

    def keys(start):
        return kv_ref[pl.ds(start, BLK), :HD]

    def values(start):
        return kv_ref[pl.ds(pl.multiple_of(start, BLK), BLK), HD:].T

    def mask_of(start, p):
        return pair_mask(segk[pl.ds(start, BLK), :], segq, p, hi)

    def diagonal():
        start = start_of(hi)
        mask = mask_of(start, hi)
        for h in range(HEADS):
            cols = slice(h * BLK, (h + 1) * BLK)
            s = jnp.where(mask, dot(keys(start), qt[:, cols]) * scale2, -jnp.inf)
            top = jnp.max(s, axis=0, keepdims=True)
            w = jnp.exp2(s - top)
            m_ref[:, cols] = top
            l_ref[:, cols] = fold(w)
            pm[:, cols] = w.astype(jnp.bfloat16)
        acc[...] = jnp.zeros_like(acc)
        return start

    def weigh(p, prev, masked):
        start = start_of(p)
        v_t = values(prev)
        k_blk = keys(start)
        if masked:
            mask = mask_of(start, p)
        for h in range(HEADS):
            cols = slice(h * BLK, (h + 1) * BLK)
            s = dot(k_blk, qt[:, cols]) * scale2 - m_ref[:, cols]
            acc[:, cols] += dot(v_t, pm[:, cols])
            if masked:
                s = jnp.where(mask, s, -jnp.inf)
            w = jnp.exp2(s)
            l_ref[:, cols] += fold(w)
            pm[:, cols] = w.astype(jnp.bfloat16)
        return start

    prev = diagonal()
    prev = lax.fori_loop(0, hi - full, lambda i, c: weigh(hi - 1 - i, c, False), prev)
    prev = lax.fori_loop(0, full - lo, lambda i, c: weigh(full - 1 - i, c, True), prev)
    acc[...] += dot(values(prev), pm[...])

    @pl.when(jnp.logical_not(jnp.max(l_ref[...]) <= 2.0 ** 20))
    def _():
        def safe(i, carry):
            p = hi - 1 - i
            start = start_of(p)
            mask = mask_of(start, p)
            for h in range(HEADS):
                cols = slice(h * BLK, (h + 1) * BLK)
                s = jnp.where(mask, dot(keys(start), qt[:, cols]) * scale2, -jnp.inf)
                top = jnp.maximum(m_ref[:, cols], jnp.max(s, axis=0, keepdims=True))
                fac = jnp.exp2(m_ref[:, cols] - top)
                w = jnp.exp2(s - top)
                m_ref[:, cols] = top
                l_ref[:, cols] = l_ref[:, cols] * fac + fold(w)
                acc[:, cols] = acc[:, cols] * fac + dot(values(start), w.astype(jnp.bfloat16))
            return carry

        first = diagonal()
        acc[...] += dot(values(first), pm[...])
        lax.fori_loop(0, hi - lo, safe, 0)

    total = jnp.sum(l_ref[...], axis=0, keepdims=True)
    lse_ref[0] = m_ref[...] + jnp.log2(total)
    inv = 1.0 / total

    for h in range(HEADS):
        cols = slice(h * BLK, (h + 1) * BLK)
        o_ref[:, h * HD:(h + 1) * HD] = (acc[:, cols] * inv[:, cols]).T.astype(jnp.bfloat16)


def bwd_kernel(remote, *refs):
    if remote:
        (seg_ref, ids_ref, q_ref, do_ref, o_ref, kv_own, kv_oth,
         rows_ref, lse_ref, dq_out, dkv_ref,
         segk, kv_ref, qs, qt, ds_, dt, delta, pm, sm, dqt) = refs
    else:
        (seg_ref, ids_ref, q_ref, do_ref, o_ref, kv_own, kv_oth,
         rows_ref, lse_ref, dq_in, dq_out, dkv_ref,
         segk, kv_ref, qs, qt, ds_, dt, delta, pm, sm, dqt) = refs
    step = pl.program_id(0)
    core = ids_ref[0]
    scale = HD ** -0.5
    scale2 = scale * math.log2(math.e)

    @pl.when(step == 0)
    def _():
        dkv_ref[...] = jnp.zeros_like(dkv_ref)
        spread_segments(rows_ref, segk, 0 if remote else HALF, HALF)
        tok = kv_own.shape[0]
        kv_ref[:tok, :] = kv_own[...]
        kv_ref[tok:, :] = kv_oth[...]

    query = HALF + ((step + 4 * core) & (HALF - 1))
    first = first_block(seg_ref, ids_ref, step)
    if remote:
        lo, hi = first, jnp.int32(HALF - 1)
    else:
        lo, hi = jnp.maximum(first, HALF), query
    count = hi - lo + 1
    segq = rows_ref[HALF + step]

    @pl.when(count > 0)
    def _():
        stack_heads(q_ref, qs)
        flip_heads(q_ref, qt)
        stack_heads(do_ref, ds_)
        flip_heads(do_ref, dt)
        for h in range(HEADS):
            hc = slice(h * HD, (h + 1) * HD)
            prod = do_ref[:, hc].astype(jnp.float32) * o_ref[:, hc].astype(jnp.float32)
            delta[:, h * BLK:(h + 1) * BLK] = jnp.sum(prod.T, axis=0, keepdims=True)

    if remote:
        dqt[...] = jnp.zeros_like(dqt)
    else:
        dqt[...] = dq_in[0]

    def body(it, carry):
        p = lo + it
        key_start = pl.multiple_of((store_block(p, core) & (HALF - 1)) * BLK, BLK)
        k_blk = kv_ref[pl.ds(key_start, BLK), :HD]
        v_blk = kv_ref[pl.ds(key_start, BLK), HD:]
        mask = pair_mask(segk[pl.ds(key_start, BLK), :], segq, p, query)
        for h in range(HEADS):
            cols = slice(h * BLK, (h + 1) * BLK)
            s = dot(k_blk, qt[:, cols])
            w = jnp.where(mask, jnp.exp2(s * scale2 - lse_ref[0, :, cols]), 0.0)
            dp = dot(v_blk, dt[:, cols])
            dsv = w * (dp - delta[:, cols])
            pm[:, cols] = w.astype(jnp.bfloat16)
            sm[:, cols] = dsv.astype(jnp.bfloat16)
        dkv_ref[pl.ds(key_start, BLK), HD:] += dot(pm[...], ds_[...])
        dkv_ref[pl.ds(key_start, BLK), :HD] += dot(sm[...], qs[...])
        dqt[...] += dot(k_blk.T, sm[...])
        return carry

    lax.fori_loop(0, count, body, 0)
    if remote:
        dq_out[0] = dqt[...]
    else:
        for h in range(HEADS):
            cols = slice(h * BLK, (h + 1) * BLK)
            dq_out[:, h * HD:(h + 1) * HD] = (dqt[:, cols] * scale).T.astype(jnp.bfloat16)


def lanes(ref, first, count):
    return jnp.concatenate([ref[first + h] for h in range(count)], axis=1)


def project_kernel(ids_ref, a_own, a_oth, w_ref, out_ref):
    weight = lanes(w_ref, 0, 2)
    half = out_ref.shape[0] // 2

    def put(src):
        for t in (0, half):
            out_ref[t:t + half, :] = dot(src[t:t + half, :], weight).astype(jnp.bfloat16)

    @pl.when(pl.program_id(0) == 0)
    def _():
        put(a_own)

    @pl.when(pl.program_id(0) == 1)
    def _():
        put(a_oth)


def project_kv_kernel(ids_ref, a_ref, wk_ref, wv_ref, out_ref, pass_ref, mine_ref, other_ref, wide):
    @pl.when(pl.program_id(0) == 0)
    def _():
        dim = mine_ref.shape[0]
        for i, ref in enumerate((wk_ref, wv_ref)):
            wide[...] = ref[...].astype(jnp.float32)
            cols = slice(i * HD, (i + 1) * HD)
            mine_ref[:, cols] = wide[pl.ds(ids_ref[0], dim, stride=2), :].astype(jnp.bfloat16)
            other_ref[:, cols] = wide[pl.ds(1 - ids_ref[0], dim, stride=2), :].astype(jnp.bfloat16)

    out_ref[...] = dot(a_ref[...], mine_ref[...]).astype(jnp.bfloat16)
    pass_ref[...] = dot(a_ref[...], other_ref[...]).astype(jnp.bfloat16)


def expand_kernel(ids_ref, a_ref, b_ref, wa_ref, wb_ref, out_ref):
    out_ref[...] = (dot_nt(a_ref[...], lanes(wa_ref, 0, HEADS))
                    + dot_nt(b_ref[...], lanes(wb_ref, 0, HEADS))).astype(jnp.bfloat16)


def expand_kv_kernel(ids_ref, a_ref, b_ref, wa_ref, wb_ref, c_ref, d_ref, wc_ref, wd_ref, out_ref):
    out_ref[...] = (dot_nt(a_ref[...], lanes(wa_ref, 0, HEADS))
                    + dot_nt(b_ref[...], lanes(wb_ref, 0, HEADS))
                    + dot_nt(c_ref[...], wc_ref[...]) + dot_nt(d_ref[...], wd_ref[...])).astype(jnp.bfloat16)


def turn_kernel(ids_ref, a_ref, b_ref, out_ref):
    half = pl.num_programs(0) // 2

    @pl.when(pl.program_id(0) < half)
    def _():
        out_ref[...] = a_ref[...].T

    @pl.when(pl.program_id(0) >= half)
    def _():
        out_ref[...] = b_ref[...].T


def wgrad_kernel(ids_ref, a_ref, b_ref, c_ref, out_ref):
    step = pl.program_id(0)
    half = pl.num_programs(0) // 2
    tok = a_ref.shape[1] // 2

    def put(own, oth):
        val = dot(a_ref[:, :tok], own) + dot(a_ref[:, tok:], oth)
        for h in range(out_ref.shape[0]):
            out_ref[h] = val[:, h * HD:(h + 1) * HD]

    @pl.when(step < half)
    def _():
        put(b_ref[:tok, :], b_ref[tok:, :])

    @pl.when(step >= half)
    def _():
        put(c_ref[tok:, :], c_ref[:tok, :])


def whole(i, *_):
    return (0, 0)


def whole3(i, *_):
    return (0, 0, 0)


def lead(i, *_):
    return (i, 0, 0)


def params(mib, axes=1):
    return pltpu.CompilerParams(dimension_semantics=('arbitrary',) * axes, vmem_limit_bytes=mib * 1024 * 1024)


def attend(seg, ids, q, kv_far, kv_near, rows):
    tok = q.shape[0]
    keys = 2 * tok
    grid = tok // BLK
    block = pl.BlockSpec((BLK, HEADS * HD), lambda i, *_: (i, 0))
    return pl.pallas_call(
        fwd_kernel,
        grid_spec=pltpu.PrefetchScalarGridSpec(
            num_scalar_prefetch=2, grid=(grid,),
            in_specs=[block] + [pl.BlockSpec((tok // 2, 2 * HD), whole)] * 4
            + [pl.BlockSpec((keys // BLK, 1, BLK), whole3)],
            out_specs=[block, pl.BlockSpec((1, 1, WIDE), lead)],
            scratch_shapes=[pltpu.VMEM((keys, 128), jnp.int32), pltpu.VMEM((keys, 2 * HD), jnp.bfloat16),
                            pltpu.VMEM((HD, WIDE), jnp.bfloat16), pltpu.VMEM((HD, WIDE), jnp.float32),
                            pltpu.VMEM((1, WIDE), jnp.float32), pltpu.VMEM((8, WIDE), jnp.float32),
                            pltpu.VMEM((BLK, WIDE), jnp.bfloat16)]),
        out_shape=[jax.ShapeDtypeStruct((tok, HEADS * HD), jnp.bfloat16),
                   jax.ShapeDtypeStruct((grid, 1, WIDE), jnp.float32)],
        compiler_params=params(24), name='attend',
        cost_estimate=pl.CostEstimate(flops=40 * 4 * WIDE * BLK * HD, bytes_accessed=12 << 20, transcendentals=0),
    )(seg, ids, q, *kv_far, *kv_near, rows)


def attend_grad(remote, seg, ids, q, do, o, kv, rows, lse, dq_in=None):
    tok = q.shape[0]
    grid = tok // BLK
    block = pl.BlockSpec((BLK, HEADS * HD), lambda i, *_: (i, 0))
    in_specs = [block] * 3 + [pl.BlockSpec((tok // 2, 2 * HD), whole)] * 2 + [
        pl.BlockSpec(rows.shape, whole3), pl.BlockSpec((1, 1, WIDE), lead)]
    args = [seg, ids, q, do, o, *kv, rows, lse]
    dqt_spec = pl.BlockSpec((1, HD, WIDE), lead)
    kv_grad = jax.ShapeDtypeStruct((tok, 2 * HD), jnp.float32)
    kv_spec = pl.BlockSpec((tok, 2 * HD), whole)
    if remote:
        out_shape = [jax.ShapeDtypeStruct((grid, HD, WIDE), jnp.float32), kv_grad]
        out_specs = [dqt_spec, kv_spec]
    else:
        in_specs.append(dqt_spec)
        args.append(dq_in)
        out_shape = [jax.ShapeDtypeStruct((tok, HEADS * HD), jnp.bfloat16), kv_grad]
        out_specs = [block, kv_spec]
    stack = pltpu.VMEM((WIDE, HD), jnp.bfloat16)
    flip = pltpu.VMEM((HD, WIDE), jnp.bfloat16)
    tile = pltpu.VMEM((BLK, WIDE), jnp.bfloat16)
    return pl.pallas_call(
        functools.partial(bwd_kernel, remote),
        grid_spec=pltpu.PrefetchScalarGridSpec(
            num_scalar_prefetch=2, grid=(grid,), in_specs=in_specs, out_specs=out_specs,
            scratch_shapes=[pltpu.VMEM((tok, 128), jnp.int32), pltpu.VMEM((tok, 2 * HD), jnp.bfloat16),
                            stack, flip, stack, flip, pltpu.VMEM((1, WIDE), jnp.float32),
                            tile, tile, pltpu.VMEM((HD, WIDE), jnp.float32)]),
        out_shape=out_shape, compiler_params=params(28),
        name='attend_grad_remote' if remote else 'attend_grad_local',
        cost_estimate=pl.CostEstimate(flops=20 * 10 * WIDE * BLK * HD, bytes_accessed=20 << 20, transcendentals=0),
    )(*args)


def project(ids, a, b, w):
    tok, dim = a.shape
    steps = HEADS // 2
    return pl.pallas_call(
        project_kernel,
        grid_spec=pltpu.PrefetchScalarGridSpec(
            num_scalar_prefetch=1, grid=(2, steps),
            in_specs=[pl.BlockSpec((tok, dim), whole)] * 2
            + [pl.BlockSpec((2, dim, HD), lambda t, i, ids: (steps * ids[0] + i, 0, 0))],
            out_specs=pl.BlockSpec((tok, 2 * HD), lambda t, i, ids: (t, i))),
        out_shape=jax.ShapeDtypeStruct((2 * tok, HEADS * HD), jnp.bfloat16),
        compiler_params=params(20, 2),
        cost_estimate=pl.CostEstimate(flops=4 * tok * dim * HEADS * HD, bytes_accessed=12 << 20, transcendentals=0),
    )(ids, a, b, w)


def project_kv(ids, a, w_k, w_v):
    tok, dim = a.shape
    mine = jax.ShapeDtypeStruct((dim, 2 * HD), jnp.bfloat16)
    pack = pl.BlockSpec((2 * dim, HD), whole)
    return pl.pallas_call(
        project_kv_kernel,
        grid_spec=pltpu.PrefetchScalarGridSpec(
            num_scalar_prefetch=1, grid=(2,),
            in_specs=[pl.BlockSpec((tok // 2, dim), lambda i, ids: (i, 0)), pack, pack],
            out_specs=[pl.BlockSpec((tok // 2, 2 * HD), lambda i, ids: (i, 0))] * 2
            + [pl.BlockSpec((dim, 2 * HD), whole)] * 2,
            scratch_shapes=[pltpu.VMEM((2 * dim, HD), jnp.float32)]),
        out_shape=[jax.ShapeDtypeStruct((tok, 2 * HD), jnp.bfloat16)] * 2 + [mine, mine],
        compiler_params=params(60), name='project_kv',
        cost_estimate=pl.CostEstimate(flops=4 * tok * dim * HD, bytes_accessed=6 << 20, transcendentals=0),
    )(ids, a, w_k.reshape(2 * dim, HD), w_v.reshape(2 * dim, HD))


def expand(ids, a, b, w, extra=()):
    tok, width = a.shape[0] // 2, a.shape[1]
    dim = w.shape[1]
    cols = 512

    def first(i, ids):
        return (0, 0)

    def second(i, ids):
        return (1, 0)

    specs = [pl.BlockSpec((tok, width), first), pl.BlockSpec((tok, width), second),
             pl.BlockSpec((HEADS, cols, HD), lambda i, ids: (ids[0], i, 0)),
             pl.BlockSpec((HEADS, cols, HD), lambda i, ids: (1 - ids[0], i, 0))]
    args = [a, b, w, w]
    if extra:
        specs += [pl.BlockSpec((tok, 2 * HD), first), pl.BlockSpec((tok, 2 * HD), second)]
        specs += [pl.BlockSpec((cols, 2 * HD), lambda i, ids: (i, 0))] * 2
        args += extra
    return pl.pallas_call(
        expand_kv_kernel if extra else expand_kernel,
        grid_spec=pltpu.PrefetchScalarGridSpec(
            num_scalar_prefetch=1, grid=(dim // cols,), in_specs=specs,
            out_specs=pl.BlockSpec((tok, cols), lambda i, ids: (0, i))),
        out_shape=jax.ShapeDtypeStruct((tok, dim), jnp.bfloat16),
        compiler_params=params(20), name='grad_x' if extra else 'out_y',
        cost_estimate=pl.CostEstimate(flops=4 * tok * dim * width, bytes_accessed=14 << 20, transcendentals=0),
    )(ids, *args)


def turn(where, a, b):
    tok, dim = a.shape
    rows = dim // 4
    part = tok // 2
    return pl.pallas_call(
        turn_kernel,
        grid_spec=pltpu.PrefetchScalarGridSpec(
            num_scalar_prefetch=1, grid=(4,),
            in_specs=[pl.BlockSpec((part, rows), lambda i, ids: (jnp.minimum(i, 1), ids[0])),
                      pl.BlockSpec((part, rows), lambda i, ids: (jnp.maximum(i - 2, 0), ids[0]))],
            out_specs=pl.BlockSpec((rows, part), lambda i, ids: (0, i))),
        out_shape=jax.ShapeDtypeStruct((rows, 2 * tok), jnp.bfloat16),
        compiler_params=params(12),
        cost_estimate=pl.CostEstimate(flops=2 << 30, bytes_accessed=4 * rows * tok * 2, transcendentals=0),
    )(where.reshape(1).astype(jnp.int32), a, b)


def wgrad(core, a, b, c):
    rows, tok = a.shape
    width = b.shape[1]
    step = 256
    half = width // step
    heads = step // HD
    return pl.pallas_call(
        wgrad_kernel,
        grid_spec=pltpu.PrefetchScalarGridSpec(
            num_scalar_prefetch=1, grid=(2 * half,),
            in_specs=[pl.BlockSpec((rows, tok), whole),
                      pl.BlockSpec((tok, step), lambda i, ids: (0, jnp.minimum(i, half - 1))),
                      pl.BlockSpec((tok, step), lambda i, ids: (0, jnp.maximum(i - half, 0)))],
            out_specs=pl.BlockSpec((heads, rows, HD), lambda i, ids: (lax.rem(i + half * ids[0], 2 * half), 0, 0))),
        out_shape=jax.ShapeDtypeStruct((2 * width // HD, rows, HD), jnp.float32),
        compiler_params=params(16),
        cost_estimate=pl.CostEstimate(flops=4 * tok * rows * width, bytes_accessed=10 << 20, transcendentals=0),
    )(core.reshape(1).astype(jnp.int32), a, b, c)


def after(value, *others):
    return lax.optimization_barrier((value, *others))[0]


def solution(mesh):
    row_spec = P(('dp', 'cp'), None)
    tok_spec = P(('dp', 'cp'))
    weight_spec = P(None, None, None)
    grad_spec = P(('dp', 'cp'), None, None)
    core_pairs = [(0, 1), (1, 0), (2, 3), (3, 2)]
    chip_pairs = [(0, 2), (2, 0), (1, 3), (3, 1)]
    up_pairs = [(0, 2), (1, 3)]
    up_cross = [(0, 3), (1, 2)]
    down_pairs = [(2, 0), (3, 1)]

    def send(a, pairs):
        return lax.ppermute(a, 'cp', pairs)

    def layer(x, seg, w_q, w_k, w_v, w_o, dy):
        _, dim = x.shape
        rows = dim // 4
        index = lax.axis_index('cp')
        core = index % 2
        chip = index // 2
        near_rows = index
        far_rows = 2 * (1 - chip) + core
        ids = jnp.stack([core, chip]).astype(jnp.int32)
        w_q = jnp.transpose(w_q, (1, 0, 2))
        w_o = jnp.transpose(w_o, (1, 0, 2))

        x_o = send(x, core_pairs)
        kv_own, kv_pass, wkv_c, wkv_p = project_kv(ids, x, w_k, w_v)
        kv_far0 = send(kv_own, up_pairs)
        kv_far1 = send(kv_pass, up_cross)
        kv_oth = send(kv_pass, core_pairs)
        seg_o = send(after(seg, kv_own), core_pairs)
        dy_o = send(after(dy, kv_own), core_pairs)
        seg_far0 = send(after(seg, kv_own), up_pairs)
        seg_far1 = send(after(seg, kv_own), up_cross)
        seg_all = jnp.concatenate([seg_far0, seg_far1, seg, seg_o])
        seg_rows = seg_all.reshape(-1, 1, BLK)
        kv_far, kv_near = (kv_far0, kv_far1), (kv_own, kv_oth)
        q = project(ids, after(x, kv_own), x_o, w_q)
        do = project(ids, after(dy, kv_own), dy_o, w_o)
        dy_far = turn(far_rows, dy, dy_o)
        x_far = turn(far_rows, x, x_o)

        o, lse = attend(seg_all, ids, q, kv_far, kv_near, seg_rows)
        o_p = send(o, core_pairs)
        dwo_far = wgrad(core, dy_far, o, o_p)
        dwo_in = send(dwo_far, chip_pairs)

        lse = after(lse, dwo_far)
        dq_part, dkv_far = attend_grad(True, seg_all, ids, q, do, o, kv_far, seg_rows, lse)
        dkv_in = send(dkv_far, down_pairs)
        dq, dkv_near = attend_grad(False, seg_all, ids, q, do, o, kv_near, seg_rows, lse, dq_part)
        dq_p = send(dq, core_pairs)
        dwq_far = wgrad(core, x_far, dq, dq_p)
        dwq_in = send(dwq_far, chip_pairs)

        y = expand(ids, after(o, dwq_far), o_p, w_o)
        x_near = turn(near_rows, after(x, dwq_far), x_o)
        dy_near = turn(near_rows, after(dy, dwq_far), dy_o)
        dwo_near = wgrad(core, dy_near, o, o_p)
        dwq_near = wgrad(core, x_near, dq, dq_p)

        dkv = dkv_near + dkv_in
        dkv = jnp.concatenate([dkv[:, :HD] * HD ** -0.5, dkv[:, HD:]], axis=1).astype(jnp.bfloat16)
        dkv_p = send(dkv, core_pairs)
        dwkv_far = wgrad(core, x_far, dkv, dkv_p)
        dwkv_in = send(dwkv_far, chip_pairs)
        dwkv_near = wgrad(core, x_near, after(dkv, dwkv_far), dkv_p)
        dx = expand(ids, after(dq, dwkv_far), dq_p, w_q, (dkv, dkv_p, wkv_c, wkv_p))

        dw_q = jnp.transpose(dwq_near + dwq_in, (1, 0, 2))
        dw_o = jnp.transpose(dwo_near + dwo_in, (1, 0, 2))
        dw_kv = jnp.transpose(dwkv_near + dwkv_in, (1, 0, 2)).reshape(rows, 2, 2, HD)
        return y, dx, dw_q, dw_kv[:, :, 0], dw_kv[:, :, 1], dw_o

    return jax.shard_map(layer, mesh=mesh,
                         in_specs=(row_spec, tok_spec, weight_spec, weight_spec, weight_spec, weight_spec, row_spec),
                         out_specs=(row_spec, row_spec, grad_spec, grad_spec, grad_spec, grad_spec),
                         check_vma=False)
```

```python
import functools
import math

import jax
import jax.numpy as jnp
from jax import lax
from jax.experimental import pallas as pl
from jax.experimental.pallas import tpu as pltpu
from jax.sharding import PartitionSpec as P

BLK = 256
HEADS = 6
HD = 128
WIDE = HEADS * BLK
HALF = 8


def dot(a, b):
    return jnp.dot(a, b, preferred_element_type=jnp.float32)


def dot_nt(a, b):
    return lax.dot_general(a, b, (((1,), (1,)), ((), ())), preferred_element_type=jnp.float32)


def stack_heads(src, dst):
    for h in range(HEADS):
        dst[h * BLK:(h + 1) * BLK, :] = src[:, h * HD:(h + 1) * HD]


def flip_heads(src, dst):
    for h in range(HEADS):
        dst[:, h * BLK:(h + 1) * BLK] = src[:, h * HD:(h + 1) * HD].T


def store_block(p, core):
    return (p & HALF) + ((p + 4 * core) & (HALF - 1))


def first_block(seg_ref, ids_ref, step):
    chip = ids_ref[1]
    first = seg_ref[(HALF + step) * BLK]
    near = jnp.int32(0)
    far = jnp.int32(0)
    for b in range(HALF):
        far += (seg_ref[b * BLK + BLK - 1] < first).astype(jnp.int32)
        near += (seg_ref[(HALF + b) * BLK + BLK - 1] < first).astype(jnp.int32)
    far = jnp.where(chip == 0, HALF, far)
    return far + near


def spread_segments(rows_ref, dst, first, count):
    for b in range(count):
        row = jnp.broadcast_to(rows_ref[first + b], (128, BLK))
        dst[b * BLK:(b + 1) * BLK, :] = row.T


def pair_mask(segk, segq, key_block, query_block):
    segk = jnp.concatenate([segk] * (BLK // 128), axis=1)
    same = segk == segq
    rel = (lax.broadcasted_iota(jnp.int32, (BLK, BLK), 0)
           - lax.broadcasted_iota(jnp.int32, (BLK, BLK), 1))
    return same & (rel <= (query_block - key_block) * BLK)


def full_blocks(seg_ref, ids_ref, step, hi):
    last = seg_ref[(HALF + step) * BLK + BLK - 1]
    count = jnp.int32(0)
    for p in range(2 * HALF):
        same = seg_ref[store_block(p, ids_ref[0]) * BLK] == last
        count += (same & (p < hi)).astype(jnp.int32)
    return count


def fwd_kernel(seg_ref, ids_ref, q_ref, kv_far0, kv_far1, kv_own, kv_oth, rows_ref, o_ref, lse_ref,
               segk, kv_ref, qt, acc, m_ref, l_ref, pm):
    step = pl.program_id(0)
    core = ids_ref[0]
    scale2 = HD ** -0.5 * math.log2(math.e)
    tok = kv_own.shape[0]

    @pl.when(step == 0)
    def _():
        spread_segments(rows_ref, segk, 0, 2 * HALF)
        for i, part in enumerate((kv_far0, kv_far1, kv_own, kv_oth)):
            kv_ref[i * tok:(i + 1) * tok, :] = part[...]

    flip_heads(q_ref, qt)
    hi = HALF + ((step + 4 * core) & (HALF - 1))
    lo = first_block(seg_ref, ids_ref, step)
    full = jnp.maximum(hi - full_blocks(seg_ref, ids_ref, step, hi), lo)
    segq = rows_ref[HALF + step]

    def start_of(p):
        return pl.multiple_of(store_block(p, core) * BLK, BLK)

    def fold(w):
        return jnp.sum(w.reshape(BLK // 8, 8, BLK), axis=0)

    def keys(start):
        return kv_ref[pl.ds(start, BLK), :HD]

    def values(start):
        return kv_ref[pl.ds(pl.multiple_of(start, BLK), BLK), HD:].T

    def mask_of(start, p):
        return pair_mask(segk[pl.ds(start, BLK), :], segq, p, hi)

    def diagonal():
        start = start_of(hi)
        mask = mask_of(start, hi)
        for h in range(HEADS):
            cols = slice(h * BLK, (h + 1) * BLK)
            s = jnp.where(mask, dot(keys(start), qt[:, cols]) * scale2, -jnp.inf)
            top = jnp.max(s, axis=0, keepdims=True)
            w = jnp.exp2(s - top)
            m_ref[:, cols] = top
            l_ref[:, cols] = fold(w)
            pm[:, cols] = w.astype(jnp.bfloat16)
        acc[...] = jnp.zeros_like(acc)
        return start

    def weigh(p, prev, masked):
        start = start_of(p)
        v_t = values(prev)
        k_blk = keys(start)
        if masked:
            mask = mask_of(start, p)
        for h in range(HEADS):
            cols = slice(h * BLK, (h + 1) * BLK)
            s = dot(k_blk, qt[:, cols]) * scale2 - m_ref[:, cols]
            acc[:, cols] += dot(v_t, pm[:, cols])
            if masked:
                s = jnp.where(mask, s, -jnp.inf)
            w = jnp.exp2(s)
            l_ref[:, cols] += fold(w)
            pm[:, cols] = w.astype(jnp.bfloat16)
        return start

    prev = diagonal()
    prev = lax.fori_loop(0, hi - full, lambda i, c: weigh(hi - 1 - i, c, False), prev)
    prev = lax.fori_loop(0, full - lo, lambda i, c: weigh(full - 1 - i, c, True), prev)
    acc[...] += dot(values(prev), pm[...])

    @pl.when(jnp.logical_not(jnp.max(l_ref[...]) <= 2.0 ** 20))
    def _():
        def safe(i, carry):
            p = hi - 1 - i
            start = start_of(p)
            mask = mask_of(start, p)
            for h in range(HEADS):
                cols = slice(h * BLK, (h + 1) * BLK)
                s = jnp.where(mask, dot(keys(start), qt[:, cols]) * scale2, -jnp.inf)
                top = jnp.maximum(m_ref[:, cols], jnp.max(s, axis=0, keepdims=True))
                fac = jnp.exp2(m_ref[:, cols] - top)
                w = jnp.exp2(s - top)
                m_ref[:, cols] = top
                l_ref[:, cols] = l_ref[:, cols] * fac + fold(w)
                acc[:, cols] = acc[:, cols] * fac + dot(values(start), w.astype(jnp.bfloat16))
            return carry

        first = diagonal()
        acc[...] += dot(values(first), pm[...])
        lax.fori_loop(0, hi - lo, safe, 0)

    total = jnp.sum(l_ref[...], axis=0, keepdims=True)
    lse_ref[0] = m_ref[...] + jnp.log2(total)
    inv = 1.0 / total

    for h in range(HEADS):
        cols = slice(h * BLK, (h + 1) * BLK)
        o_ref[:, h * HD:(h + 1) * HD] = (acc[:, cols] * inv[:, cols]).T.astype(jnp.bfloat16)


def bwd_kernel(remote, *refs):
    if remote:
        (seg_ref, ids_ref, q_ref, do_ref, o_ref, kv_own, kv_oth,
         rows_ref, lse_ref, dq_out, dkv_ref,
         segk, kv_ref, qs, qt, ds_, dt, delta, pm, sm, dqt) = refs
    else:
        (seg_ref, ids_ref, q_ref, do_ref, o_ref, kv_own, kv_oth,
         rows_ref, lse_ref, dq_in, dq_out, dkv_ref,
         segk, kv_ref, qs, qt, ds_, dt, delta, pm, sm, dqt) = refs
    step = pl.program_id(0)
    core = ids_ref[0]
    scale = HD ** -0.5
    scale2 = scale * math.log2(math.e)

    @pl.when(step == 0)
    def _():
        dkv_ref[...] = jnp.zeros_like(dkv_ref)
        spread_segments(rows_ref, segk, 0 if remote else HALF, HALF)
        tok = kv_own.shape[0]
        kv_ref[:tok, :] = kv_own[...]
        kv_ref[tok:, :] = kv_oth[...]

    query = HALF + ((step + 4 * core) & (HALF - 1))
    first = first_block(seg_ref, ids_ref, step)
    if remote:
        lo, hi = first, jnp.int32(HALF - 1)
    else:
        lo, hi = jnp.maximum(first, HALF), query
    count = hi - lo + 1
    segq = rows_ref[HALF + step]

    @pl.when(count > 0)
    def _():
        stack_heads(q_ref, qs)
        flip_heads(q_ref, qt)
        stack_heads(do_ref, ds_)
        flip_heads(do_ref, dt)
        for h in range(HEADS):
            hc = slice(h * HD, (h + 1) * HD)
            prod = do_ref[:, hc].astype(jnp.float32) * o_ref[:, hc].astype(jnp.float32)
            delta[:, h * BLK:(h + 1) * BLK] = jnp.sum(prod.T, axis=0, keepdims=True)

    if remote:
        dqt[...] = jnp.zeros_like(dqt)
    else:
        dqt[...] = dq_in[0]

    def body(it, carry):
        p = lo + it
        key_start = pl.multiple_of((store_block(p, core) & (HALF - 1)) * BLK, BLK)
        k_blk = kv_ref[pl.ds(key_start, BLK), :HD]
        v_blk = kv_ref[pl.ds(key_start, BLK), HD:]
        mask = pair_mask(segk[pl.ds(key_start, BLK), :], segq, p, query)
        for h in range(HEADS):
            cols = slice(h * BLK, (h + 1) * BLK)
            s = dot(k_blk, qt[:, cols])
            w = jnp.where(mask, jnp.exp2(s * scale2 - lse_ref[0, :, cols]), 0.0)
            dp = dot(v_blk, dt[:, cols])
            dsv = w * (dp - delta[:, cols])
            pm[:, cols] = w.astype(jnp.bfloat16)
            sm[:, cols] = dsv.astype(jnp.bfloat16)
        dkv_ref[pl.ds(key_start, BLK), HD:] += dot(pm[...], ds_[...])
        dkv_ref[pl.ds(key_start, BLK), :HD] += dot(sm[...], qs[...])
        dqt[...] += dot(k_blk.T, sm[...])
        return carry

    lax.fori_loop(0, count, body, 0)
    if remote:
        dq_out[0] = dqt[...]
    else:
        for h in range(HEADS):
            cols = slice(h * BLK, (h + 1) * BLK)
            dq_out[:, h * HD:(h + 1) * HD] = (dqt[:, cols] * scale).T.astype(jnp.bfloat16)


def lanes(ref, first, count):
    return jnp.concatenate([ref[first + h] for h in range(count)], axis=1)


def project_kernel(ids_ref, a_own, a_oth, w_ref, out_ref):
    half = out_ref.shape[0] // 2

    def put(src):
        for n in range(0, HEADS, 2):
            weight = jnp.concatenate([w_ref[n], w_ref[n + 1]], axis=1)
            for t in (0, half):
                out_ref[t:t + half, n * HD:(n + 2) * HD] = dot(src[t:t + half, :], weight).astype(jnp.bfloat16)

    @pl.when(pl.program_id(0) == 0)
    def _():
        put(a_own)

    @pl.when(pl.program_id(0) == 1)
    def _():
        put(a_oth)


def project_kv_kernel(ids_ref, a_ref, wk_ref, wv_ref, out_ref, pass_ref, mine_ref, other_ref, wide):
    @pl.when(pl.program_id(0) == 0)
    def _():
        dim = mine_ref.shape[0]
        for i, ref in enumerate((wk_ref, wv_ref)):
            wide[...] = ref[...].astype(jnp.float32)
            cols = slice(i * HD, (i + 1) * HD)
            mine_ref[:, cols] = wide[pl.ds(ids_ref[0], dim, stride=2), :].astype(jnp.bfloat16)
            other_ref[:, cols] = wide[pl.ds(1 - ids_ref[0], dim, stride=2), :].astype(jnp.bfloat16)

    out_ref[...] = dot(a_ref[...], mine_ref[...]).astype(jnp.bfloat16)
    pass_ref[...] = dot(a_ref[...], other_ref[...]).astype(jnp.bfloat16)


def expand_kernel(ids_ref, a_ref, b_ref, wa_ref, wb_ref, out_ref):
    out_ref[...] = (dot_nt(a_ref[...], lanes(wa_ref, 0, HEADS))
                    + dot_nt(b_ref[...], lanes(wb_ref, 0, HEADS))).astype(jnp.bfloat16)


def expand_kv_kernel(ids_ref, a_ref, b_ref, wa_ref, wb_ref, c_ref, d_ref, wc_ref, wd_ref, out_ref):
    out_ref[...] = (dot_nt(a_ref[...], lanes(wa_ref, 0, HEADS))
                    + dot_nt(b_ref[...], lanes(wb_ref, 0, HEADS))
                    + dot_nt(c_ref[...], wc_ref[...]) + dot_nt(d_ref[...], wd_ref[...])).astype(jnp.bfloat16)


def turn_kernel(ids_ref, a_ref, b_ref, out_ref):
    half = pl.num_programs(0) // 2

    @pl.when(pl.program_id(0) < half)
    def _():
        out_ref[...] = a_ref[...].T

    @pl.when(pl.program_id(0) >= half)
    def _():
        out_ref[...] = b_ref[...].T


def wgrad_one_kernel(partner, a_ref, b_ref, out_ref):
    tok = a_ref.shape[1] // 2
    first, second = (b_ref[tok:, :], b_ref[:tok, :]) if partner else (b_ref[:tok, :], b_ref[tok:, :])
    val = dot(a_ref[:, :tok], first) + dot(a_ref[:, tok:], second)
    for h in range(out_ref.shape[0]):
        out_ref[h] = val[:, h * HD:(h + 1) * HD]


def wgrad_kernel(ids_ref, a_ref, b_ref, c_ref, out_ref):
    step = pl.program_id(0)
    half = pl.num_programs(0) // 2
    tok = a_ref.shape[1] // 2

    def put(own, oth):
        val = dot(a_ref[:, :tok], own) + dot(a_ref[:, tok:], oth)
        for h in range(out_ref.shape[0]):
            out_ref[h] = val[:, h * HD:(h + 1) * HD]

    @pl.when(step < half)
    def _():
        put(b_ref[:tok, :], b_ref[tok:, :])

    @pl.when(step >= half)
    def _():
        put(c_ref[tok:, :], c_ref[:tok, :])


def whole(i, *_):
    return (0, 0)


def whole3(i, *_):
    return (0, 0, 0)


def lead(i, *_):
    return (i, 0, 0)


def params(mib):
    return pltpu.CompilerParams(dimension_semantics=('arbitrary',), vmem_limit_bytes=mib * 1024 * 1024)


def attend(seg, ids, q, kv_far, kv_near, rows):
    tok = q.shape[0]
    keys = 2 * tok
    grid = tok // BLK
    block = pl.BlockSpec((BLK, HEADS * HD), lambda i, *_: (i, 0))
    return pl.pallas_call(
        fwd_kernel,
        grid_spec=pltpu.PrefetchScalarGridSpec(
            num_scalar_prefetch=2, grid=(grid,),
            in_specs=[block] + [pl.BlockSpec((tok // 2, 2 * HD), whole)] * 4
            + [pl.BlockSpec((keys // BLK, 1, BLK), whole3)],
            out_specs=[block, pl.BlockSpec((1, 1, WIDE), lead)],
            scratch_shapes=[pltpu.VMEM((keys, 128), jnp.int32), pltpu.VMEM((keys, 2 * HD), jnp.bfloat16),
                            pltpu.VMEM((HD, WIDE), jnp.bfloat16), pltpu.VMEM((HD, WIDE), jnp.float32),
                            pltpu.VMEM((1, WIDE), jnp.float32), pltpu.VMEM((8, WIDE), jnp.float32),
                            pltpu.VMEM((BLK, WIDE), jnp.bfloat16)]),
        out_shape=[jax.ShapeDtypeStruct((tok, HEADS * HD), jnp.bfloat16),
                   jax.ShapeDtypeStruct((grid, 1, WIDE), jnp.float32)],
        compiler_params=params(24), name='attend',
        cost_estimate=pl.CostEstimate(flops=40 * 4 * WIDE * BLK * HD, bytes_accessed=12 << 20, transcendentals=0),
    )(seg, ids, q, *kv_far, *kv_near, rows)


def attend_grad(remote, seg, ids, q, do, o, kv, rows, lse, dq_in=None):
    tok = q.shape[0]
    grid = tok // BLK
    block = pl.BlockSpec((BLK, HEADS * HD), lambda i, *_: (i, 0))
    in_specs = [block] * 3 + [pl.BlockSpec((tok // 2, 2 * HD), whole)] * 2 + [
        pl.BlockSpec(rows.shape, whole3), pl.BlockSpec((1, 1, WIDE), lead)]
    args = [seg, ids, q, do, o, *kv, rows, lse]
    dqt_spec = pl.BlockSpec((1, HD, WIDE), lead)
    kv_grad = jax.ShapeDtypeStruct((tok, 2 * HD), jnp.float32)
    kv_spec = pl.BlockSpec((tok, 2 * HD), whole)
    if remote:
        out_shape = [jax.ShapeDtypeStruct((grid, HD, WIDE), jnp.float32), kv_grad]
        out_specs = [dqt_spec, kv_spec]
    else:
        in_specs.append(dqt_spec)
        args.append(dq_in)
        out_shape = [jax.ShapeDtypeStruct((tok, HEADS * HD), jnp.bfloat16), kv_grad]
        out_specs = [block, kv_spec]
    stack = pltpu.VMEM((WIDE, HD), jnp.bfloat16)
    flip = pltpu.VMEM((HD, WIDE), jnp.bfloat16)
    tile = pltpu.VMEM((BLK, WIDE), jnp.bfloat16)
    return pl.pallas_call(
        functools.partial(bwd_kernel, remote),
        grid_spec=pltpu.PrefetchScalarGridSpec(
            num_scalar_prefetch=2, grid=(grid,), in_specs=in_specs, out_specs=out_specs,
            scratch_shapes=[pltpu.VMEM((tok, 128), jnp.int32), pltpu.VMEM((tok, 2 * HD), jnp.bfloat16),
                            stack, flip, stack, flip, pltpu.VMEM((1, WIDE), jnp.float32),
                            tile, tile, pltpu.VMEM((HD, WIDE), jnp.float32)]),
        out_shape=out_shape, compiler_params=params(28),
        name='attend_grad_remote' if remote else 'attend_grad_local',
        cost_estimate=pl.CostEstimate(flops=20 * 10 * WIDE * BLK * HD, bytes_accessed=20 << 20, transcendentals=0),
    )(*args)


def project(ids, a, b, w):
    tok, dim = a.shape
    return pl.pallas_call(
        project_kernel,
        grid_spec=pltpu.PrefetchScalarGridSpec(
            num_scalar_prefetch=1, grid=(2,),
            in_specs=[pl.BlockSpec((tok, dim), whole)] * 2
            + [pl.BlockSpec((HEADS, dim, HD), lambda t, ids: (ids[0], 0, 0))],
            out_specs=pl.BlockSpec((tok, HEADS * HD), lambda t, ids: (t, 0))),
        out_shape=jax.ShapeDtypeStruct((2 * tok, HEADS * HD), jnp.bfloat16),
        compiler_params=params(24),
        cost_estimate=pl.CostEstimate(flops=4 * tok * dim * HEADS * HD, bytes_accessed=12 << 20, transcendentals=0),
    )(ids, a, b, w)


def project_kv(ids, a, w_k, w_v):
    tok, dim = a.shape
    mine = jax.ShapeDtypeStruct((dim, 2 * HD), jnp.bfloat16)
    pack = pl.BlockSpec((2 * dim, HD), whole)
    return pl.pallas_call(
        project_kv_kernel,
        grid_spec=pltpu.PrefetchScalarGridSpec(
            num_scalar_prefetch=1, grid=(2,),
            in_specs=[pl.BlockSpec((tok // 2, dim), lambda i, ids: (i, 0)), pack, pack],
            out_specs=[pl.BlockSpec((tok // 2, 2 * HD), lambda i, ids: (i, 0))] * 2
            + [pl.BlockSpec((dim, 2 * HD), whole)] * 2,
            scratch_shapes=[pltpu.VMEM((2 * dim, HD), jnp.float32)]),
        out_shape=[jax.ShapeDtypeStruct((tok, 2 * HD), jnp.bfloat16)] * 2 + [mine, mine],
        compiler_params=params(60), name='project_kv',
        cost_estimate=pl.CostEstimate(flops=4 * tok * dim * HD, bytes_accessed=6 << 20, transcendentals=0),
    )(ids, a, w_k.reshape(2 * dim, HD), w_v.reshape(2 * dim, HD))


def expand(ids, a, b, w, extra=()):
    tok, width = a.shape[0] // 2, a.shape[1]
    dim = w.shape[1]
    cols = 512

    def first(i, ids):
        return (0, 0)

    def second(i, ids):
        return (1, 0)

    specs = [pl.BlockSpec((tok, width), first), pl.BlockSpec((tok, width), second),
             pl.BlockSpec((HEADS, cols, HD), lambda i, ids: (ids[0], i, 0)),
             pl.BlockSpec((HEADS, cols, HD), lambda i, ids: (1 - ids[0], i, 0))]
    args = [a, b, w, w]
    if extra:
        specs += [pl.BlockSpec((tok, 2 * HD), first), pl.BlockSpec((tok, 2 * HD), second)]
        specs += [pl.BlockSpec((cols, 2 * HD), lambda i, ids: (i, 0))] * 2
        args += extra
    return pl.pallas_call(
        expand_kv_kernel if extra else expand_kernel,
        grid_spec=pltpu.PrefetchScalarGridSpec(
            num_scalar_prefetch=1, grid=(dim // cols,), in_specs=specs,
            out_specs=pl.BlockSpec((tok, cols), lambda i, ids: (0, i))),
        out_shape=jax.ShapeDtypeStruct((tok, dim), jnp.bfloat16),
        compiler_params=params(20), name='grad_x' if extra else 'out_y',
        cost_estimate=pl.CostEstimate(flops=4 * tok * dim * width, bytes_accessed=14 << 20, transcendentals=0),
    )(ids, *args)


def turn(where, a, b):
    tok, dim = a.shape
    rows = dim // 4
    part = tok // 2
    return pl.pallas_call(
        turn_kernel,
        grid_spec=pltpu.PrefetchScalarGridSpec(
            num_scalar_prefetch=1, grid=(4,),
            in_specs=[pl.BlockSpec((part, rows), lambda i, ids: (jnp.minimum(i, 1), ids[0])),
                      pl.BlockSpec((part, rows), lambda i, ids: (jnp.maximum(i - 2, 0), ids[0]))],
            out_specs=pl.BlockSpec((rows, part), lambda i, ids: (0, i))),
        out_shape=jax.ShapeDtypeStruct((rows, 2 * tok), jnp.bfloat16),
        compiler_params=params(12),
        cost_estimate=pl.CostEstimate(flops=2 << 30, bytes_accessed=4 * rows * tok * 2, transcendentals=0),
    )(where.reshape(1).astype(jnp.int32), a, b)


def wgrad(core, a, b, c):
    rows, tok = a.shape
    width = b.shape[1]
    step = 256
    half = width // step
    heads = step // HD
    return pl.pallas_call(
        wgrad_kernel,
        grid_spec=pltpu.PrefetchScalarGridSpec(
            num_scalar_prefetch=1, grid=(2 * half,),
            in_specs=[pl.BlockSpec((rows, tok), whole),
                      pl.BlockSpec((tok, step), lambda i, ids: (0, jnp.minimum(i, half - 1))),
                      pl.BlockSpec((tok, step), lambda i, ids: (0, jnp.maximum(i - half, 0)))],
            out_specs=pl.BlockSpec((heads, rows, HD), lambda i, ids: (lax.rem(i + half * ids[0], 2 * half), 0, 0))),
        out_shape=jax.ShapeDtypeStruct((2 * width // HD, rows, HD), jnp.float32),
        compiler_params=params(16),
        cost_estimate=pl.CostEstimate(flops=4 * tok * rows * width, bytes_accessed=10 << 20, transcendentals=0),
    )(core.reshape(1).astype(jnp.int32), a, b, c)


def wgrad_one(a, b, partner):
    rows, tok = a.shape
    width = b.shape[1]
    step = 256
    heads = step // HD
    return pl.pallas_call(
        functools.partial(wgrad_one_kernel, partner),
        grid=(width // step,),
        in_specs=[pl.BlockSpec((rows, tok), whole), pl.BlockSpec((tok, step), lambda i: (0, i))],
        out_specs=pl.BlockSpec((heads, rows, HD), lambda i: (i, 0, 0)),
        out_shape=jax.ShapeDtypeStruct((width // HD, rows, HD), jnp.float32),
        compiler_params=params(16),
        cost_estimate=pl.CostEstimate(flops=2 * tok * rows * width, bytes_accessed=6 << 20, transcendentals=0),
    )(a, b)


def after(value, *others):
    return lax.optimization_barrier((value, *others))[0]


def solution(mesh):
    row_spec = P(('dp', 'cp'), None)
    tok_spec = P(('dp', 'cp'))
    weight_spec = P(None, None, None)
    grad_spec = P(('dp', 'cp'), None, None)
    core_pairs = [(0, 1), (1, 0), (2, 3), (3, 2)]
    chip_pairs = [(0, 2), (2, 0), (1, 3), (3, 1)]
    up_pairs = [(0, 2), (1, 3)]
    up_cross = [(0, 3), (1, 2)]
    down_pairs = [(2, 0), (3, 1)]

    def send(a, pairs):
        return lax.ppermute(a, 'cp', pairs)

    def layer(x, seg, w_q, w_k, w_v, w_o, dy):
        _, dim = x.shape
        rows = dim // 4
        index = lax.axis_index('cp')
        core = index % 2
        chip = index // 2
        near_rows = index
        far_rows = 2 * (1 - chip) + core
        ids = jnp.stack([core, chip]).astype(jnp.int32)
        w_q = jnp.transpose(w_q, (1, 0, 2))
        w_o = jnp.transpose(w_o, (1, 0, 2))

        x_o = send(x, core_pairs)
        kv_own, kv_pass, wkv_c, wkv_p = project_kv(ids, x, w_k, w_v)
        kv_far0 = send(kv_own, up_pairs)
        kv_far1 = send(kv_pass, up_cross)
        kv_oth = send(kv_pass, core_pairs)
        seg_o = send(after(seg, kv_own), core_pairs)
        dy_o = send(after(dy, kv_own), core_pairs)
        seg_far0 = send(after(seg, kv_own), up_pairs)
        seg_far1 = send(after(seg, kv_own), up_cross)
        seg_all = jnp.concatenate([seg_far0, seg_far1, seg, seg_o])
        seg_rows = seg_all.reshape(-1, 1, BLK)
        kv_far, kv_near = (kv_far0, kv_far1), (kv_own, kv_oth)
        q = project(ids, after(x, kv_own), x_o, w_q)
        do = project(ids, after(dy, kv_own), dy_o, w_o)
        dy_far = turn(far_rows, dy, dy_o)
        x_far = turn(far_rows, x, x_o)

        o, lse = attend(seg_all, ids, q, kv_far, kv_near, seg_rows)
        o_p = send(o, core_pairs)
        dwo_far = wgrad_one(dy_far, o, False)
        dwo_in = send(dwo_far, chip_pairs)
        dwo_far2 = wgrad_one(dy_far, o_p, True)
        dwo_in2 = send(dwo_far2, chip_pairs)

        lse = after(lse, dwo_far2)
        dq_part, dkv_far = attend_grad(True, seg_all, ids, q, do, o, kv_far, seg_rows, lse)
        dkv_in = send(dkv_far, down_pairs)
        dq, dkv_near = attend_grad(False, seg_all, ids, q, do, o, kv_near, seg_rows, lse, dq_part)
        dq_p = send(dq, core_pairs)
        dwq_far1 = wgrad_one(x_far, dq, False)
        dwq_in = send(dwq_far1, chip_pairs)
        dwq_far = wgrad_one(x_far, dq_p, True)
        dwq_in2 = send(dwq_far, chip_pairs)

        y = expand(ids, after(o, dwq_far), o_p, w_o)
        x_near = turn(near_rows, after(x, dwq_far), x_o)
        dy_near = turn(near_rows, after(dy, dwq_far), dy_o)
        dwo_near = wgrad(core, dy_near, o, o_p)
        dwq_near = wgrad(core, x_near, dq, dq_p)

        dkv = dkv_near + dkv_in
        dkv = jnp.concatenate([dkv[:, :HD] * HD ** -0.5, dkv[:, HD:]], axis=1).astype(jnp.bfloat16)
        dkv_p = send(dkv, core_pairs)
        dwkv_far = wgrad(core, x_far, dkv, dkv_p)
        dwkv_in = send(dwkv_far, chip_pairs)
        dwkv_near = wgrad(core, x_near, after(dkv, dwkv_far), dkv_p)
        dx = expand(ids, after(dq, dwkv_far), dq_p, w_q, (dkv, dkv_p, wkv_c, wkv_p))

        def total(near, mine, other):
            far = jnp.where(core == 0, jnp.concatenate([mine, other]), jnp.concatenate([other, mine]))
            return jnp.transpose(near + far, (1, 0, 2))

        dw_o = total(dwo_near, dwo_in, dwo_in2)
        dw_q = total(dwq_near, dwq_in, dwq_in2)
        dw_kv = jnp.transpose(dwkv_near + dwkv_in, (1, 0, 2)).reshape(rows, 2, 2, HD)
        return y, dx, dw_q, dw_kv[:, :, 0], dw_kv[:, :, 1], dw_o

    return jax.shard_map(layer, mesh=mesh,
                         in_specs=(row_spec, tok_spec, weight_spec, weight_spec, weight_spec, weight_spec, row_spec),
                         out_specs=(row_spec, row_spec, grad_spec, grad_spec, grad_spec, grad_spec),
                         check_vma=False)
```

```python
import functools
import math

import jax
import jax.numpy as jnp
from jax import lax
from jax.experimental import pallas as pl
from jax.experimental.pallas import tpu as pltpu
from jax.sharding import PartitionSpec as P

BLK = 256
HEADS = 6
HD = 128
WIDE = HEADS * BLK
HALF = 8


def dot(a, b):
    return jnp.dot(a, b, preferred_element_type=jnp.float32)


def dot_nt(a, b):
    return lax.dot_general(a, b, (((1,), (1,)), ((), ())), preferred_element_type=jnp.float32)


def stack_heads(src, dst):
    for h in range(HEADS):
        dst[h * BLK:(h + 1) * BLK, :] = src[:, h * HD:(h + 1) * HD]


def flip_heads(src, dst):
    for h in range(HEADS):
        dst[:, h * BLK:(h + 1) * BLK] = src[:, h * HD:(h + 1) * HD].T


def store_block(p, core):
    return (p & HALF) + ((p + 4 * core) & (HALF - 1))


def first_block(seg_ref, ids_ref, step):
    chip = ids_ref[1]
    first = seg_ref[(HALF + step) * BLK]
    near = jnp.int32(0)
    far = jnp.int32(0)
    for b in range(HALF):
        far += (seg_ref[b * BLK + BLK - 1] < first).astype(jnp.int32)
        near += (seg_ref[(HALF + b) * BLK + BLK - 1] < first).astype(jnp.int32)
    far = jnp.where(chip == 0, HALF, far)
    return far + near


def spread_segments(rows_ref, dst, first, count):
    for b in range(count):
        row = jnp.broadcast_to(rows_ref[first + b], (128, BLK))
        dst[b * BLK:(b + 1) * BLK, :] = row.T


def pair_mask(segk, segq, key_block, query_block):
    segk = jnp.concatenate([segk] * (BLK // 128), axis=1)
    same = segk == segq
    rel = (lax.broadcasted_iota(jnp.int32, (BLK, BLK), 0)
           - lax.broadcasted_iota(jnp.int32, (BLK, BLK), 1))
    return same & (rel <= (query_block - key_block) * BLK)


def full_blocks(seg_ref, ids_ref, step, hi):
    last = seg_ref[(HALF + step) * BLK + BLK - 1]
    count = jnp.int32(0)
    for p in range(2 * HALF):
        same = seg_ref[store_block(p, ids_ref[0]) * BLK] == last
        count += (same & (p < hi)).astype(jnp.int32)
    return count


def fwd_kernel(seg_ref, ids_ref, q_ref, kv_far0, kv_far1, kv_own, kv_oth, rows_ref, o_ref, lse_ref, reach_ref,
               segk, kv_ref, qt, acc, m_ref, l_ref, pm):
    step = pl.program_id(0)
    core = ids_ref[0]
    scale2 = HD ** -0.5 * math.log2(math.e)
    tok = kv_own.shape[0]

    @pl.when(step == 0)
    def _():
        spread_segments(rows_ref, segk, 0, 2 * HALF)
        first = jnp.where(ids_ref[1] == 0, HALF, 0)
        ends = [seg_ref[store_block(first + p, core) * BLK + BLK - 1] for p in (HALF // 2 - 1, HALF - 1)]
        reach_ref[0] = (ends[0] == ends[1]).astype(jnp.int32)

        for i, part in enumerate((kv_far0, kv_far1, kv_own, kv_oth)):
            kv_ref[i * tok:(i + 1) * tok, :] = part[...]

    flip_heads(q_ref, qt)
    hi = HALF + ((step + 4 * core) & (HALF - 1))
    lo = first_block(seg_ref, ids_ref, step)
    full = jnp.maximum(hi - full_blocks(seg_ref, ids_ref, step, hi), lo)
    segq = rows_ref[HALF + step]

    def start_of(p):
        return pl.multiple_of(store_block(p, core) * BLK, BLK)

    def fold(w):
        return jnp.sum(w.reshape(BLK // 8, 8, BLK), axis=0)

    def keys(start):
        return kv_ref[pl.ds(start, BLK), :HD]

    def values(start):
        return kv_ref[pl.ds(pl.multiple_of(start, BLK), BLK), HD:].T

    def mask_of(start, p):
        return pair_mask(segk[pl.ds(start, BLK), :], segq, p, hi)

    def diagonal():
        start = start_of(hi)
        mask = mask_of(start, hi)
        for h in range(HEADS):
            cols = slice(h * BLK, (h + 1) * BLK)
            s = jnp.where(mask, dot(keys(start), qt[:, cols]) * scale2, -jnp.inf)
            top = jnp.max(s, axis=0, keepdims=True)
            w = jnp.exp2(s - top)
            m_ref[:, cols] = top
            l_ref[:, cols] = fold(w)
            pm[:, cols] = w.astype(jnp.bfloat16)
        acc[...] = jnp.zeros_like(acc)
        return start

    def weigh(p, prev, masked):
        start = start_of(p)
        v_t = values(prev)
        k_blk = keys(start)
        if masked:
            mask = mask_of(start, p)
        for h in range(HEADS):
            cols = slice(h * BLK, (h + 1) * BLK)
            s = dot(k_blk, qt[:, cols]) * scale2 - m_ref[:, cols]
            acc[:, cols] += dot(v_t, pm[:, cols])
            if masked:
                s = jnp.where(mask, s, -jnp.inf)
            w = jnp.exp2(s)
            l_ref[:, cols] += fold(w)
            pm[:, cols] = w.astype(jnp.bfloat16)
        return start

    prev = diagonal()
    prev = lax.fori_loop(0, hi - full, lambda i, c: weigh(hi - 1 - i, c, False), prev)
    prev = lax.fori_loop(0, full - lo, lambda i, c: weigh(full - 1 - i, c, True), prev)
    acc[...] += dot(values(prev), pm[...])

    @pl.when(jnp.logical_not(jnp.max(l_ref[...]) <= 2.0 ** 20))
    def _():
        def safe(i, carry):
            p = hi - 1 - i
            start = start_of(p)
            mask = mask_of(start, p)
            for h in range(HEADS):
                cols = slice(h * BLK, (h + 1) * BLK)
                s = jnp.where(mask, dot(keys(start), qt[:, cols]) * scale2, -jnp.inf)
                top = jnp.maximum(m_ref[:, cols], jnp.max(s, axis=0, keepdims=True))
                fac = jnp.exp2(m_ref[:, cols] - top)
                w = jnp.exp2(s - top)
                m_ref[:, cols] = top
                l_ref[:, cols] = l_ref[:, cols] * fac + fold(w)
                acc[:, cols] = acc[:, cols] * fac + dot(values(start), w.astype(jnp.bfloat16))
            return carry

        first = diagonal()
        acc[...] += dot(values(first), pm[...])
        lax.fori_loop(0, hi - lo, safe, 0)

    total = jnp.sum(l_ref[...], axis=0, keepdims=True)
    lse_ref[0] = m_ref[...] + jnp.log2(total)
    inv = 1.0 / total

    for h in range(HEADS):
        cols = slice(h * BLK, (h + 1) * BLK)
        o_ref[:, h * HD:(h + 1) * HD] = (acc[:, cols] * inv[:, cols]).T.astype(jnp.bfloat16)


def bwd_kernel(remote, *refs):
    if remote:
        (seg_ref, ids_ref, q_ref, do_ref, o_ref, kv_own, kv_oth,
         rows_ref, lse_ref, dq_out, dkv_first, dkv_second,
         segk, kv_ref, qs, qt, ds_, dt, delta, pm, sm, dqt, dkv_ref) = refs
    else:
        (seg_ref, ids_ref, q_ref, do_ref, o_ref, kv_own, kv_oth,
         rows_ref, lse_ref, dq_in, dq_out, dkv_ref,
         segk, kv_ref, qs, qt, ds_, dt, delta, pm, sm, dqt) = refs
    step = pl.program_id(0)
    core = ids_ref[0]
    scale = HD ** -0.5
    scale2 = scale * math.log2(math.e)

    @pl.when(step == 0)
    def _():
        dkv_ref[...] = jnp.zeros_like(dkv_ref)
        spread_segments(rows_ref, segk, 0 if remote else HALF, HALF)
        tok = kv_own.shape[0]
        kv_ref[:tok, :] = kv_own[...]
        kv_ref[tok:, :] = kv_oth[...]

    query = HALF + ((step + 4 * core) & (HALF - 1))
    first = first_block(seg_ref, ids_ref, step)
    if remote:
        lo, hi = first, jnp.int32(HALF - 1)
    else:
        lo, hi = jnp.maximum(first, HALF), query
    count = hi - lo + 1
    segq = rows_ref[HALF + step]

    @pl.when(count > 0)
    def _():
        stack_heads(q_ref, qs)
        flip_heads(q_ref, qt)
        stack_heads(do_ref, ds_)
        flip_heads(do_ref, dt)
        for h in range(HEADS):
            hc = slice(h * HD, (h + 1) * HD)
            prod = do_ref[:, hc].astype(jnp.float32) * o_ref[:, hc].astype(jnp.float32)
            delta[:, h * BLK:(h + 1) * BLK] = jnp.sum(prod.T, axis=0, keepdims=True)

    if remote:
        dqt[...] = jnp.zeros_like(dqt)
    else:
        dqt[...] = dq_in[0]

    def body(it, carry):
        p = lo + it
        key_start = pl.multiple_of((store_block(p, core) & (HALF - 1)) * BLK, BLK)
        k_blk = kv_ref[pl.ds(key_start, BLK), :HD]
        v_blk = kv_ref[pl.ds(key_start, BLK), HD:]
        mask = pair_mask(segk[pl.ds(key_start, BLK), :], segq, p, query)
        for h in range(HEADS):
            cols = slice(h * BLK, (h + 1) * BLK)
            s = dot(k_blk, qt[:, cols])
            w = jnp.where(mask, jnp.exp2(s * scale2 - lse_ref[0, :, cols]), 0.0)
            dp = dot(v_blk, dt[:, cols])
            dsv = w * (dp - delta[:, cols])
            pm[:, cols] = w.astype(jnp.bfloat16)
            sm[:, cols] = dsv.astype(jnp.bfloat16)
        put = pl.multiple_of(p * BLK, BLK) if remote else key_start
        dkv_ref[pl.ds(put, BLK), HD:] += dot(pm[...], ds_[...])
        dkv_ref[pl.ds(put, BLK), :HD] += dot(sm[...], qs[...])
        dqt[...] += dot(k_blk.T, sm[...])
        return carry

    lax.fori_loop(0, count, body, 0)
    if remote:
        dq_out[0] = dqt[...]

        @pl.when(step == pl.num_programs(0) - 1)
        def _():
            tok = dkv_first.shape[0]
            dkv_first[...] = dkv_ref[:tok, :]
            dkv_second[...] = dkv_ref[tok:, :]
    else:
        for h in range(HEADS):
            cols = slice(h * BLK, (h + 1) * BLK)
            dq_out[:, h * HD:(h + 1) * HD] = (dqt[:, cols] * scale).T.astype(jnp.bfloat16)


def lanes(ref, first, count):
    return jnp.concatenate([ref[first + h] for h in range(count)], axis=1)


def project_kernel(ids_ref, a_own, a_oth, w_ref, out_ref):
    half = out_ref.shape[0] // 2

    def put(src):
        for n in range(0, HEADS, 2):
            weight = jnp.concatenate([w_ref[n], w_ref[n + 1]], axis=1)
            for t in (0, half):
                out_ref[t:t + half, n * HD:(n + 2) * HD] = dot(src[t:t + half, :], weight).astype(jnp.bfloat16)

    @pl.when(pl.program_id(0) == 0)
    def _():
        put(a_own)

    @pl.when(pl.program_id(0) == 1)
    def _():
        put(a_oth)


def project_kv_kernel(ids_ref, a_ref, wk_ref, wv_ref, out_ref, pass_ref, mine_ref, other_ref, wide):
    @pl.when(pl.program_id(0) == 0)
    def _():
        dim = mine_ref.shape[0]
        for i, ref in enumerate((wk_ref, wv_ref)):
            wide[...] = ref[...].astype(jnp.float32)
            cols = slice(i * HD, (i + 1) * HD)
            mine_ref[:, cols] = wide[pl.ds(ids_ref[0], dim, stride=2), :].astype(jnp.bfloat16)
            other_ref[:, cols] = wide[pl.ds(1 - ids_ref[0], dim, stride=2), :].astype(jnp.bfloat16)

    out_ref[...] = dot(a_ref[...], mine_ref[...]).astype(jnp.bfloat16)
    pass_ref[...] = dot(a_ref[...], other_ref[...]).astype(jnp.bfloat16)


def expand_kernel(ids_ref, a_ref, b_ref, wa_ref, wb_ref, out_ref):
    out_ref[...] = (dot_nt(a_ref[...], lanes(wa_ref, 0, HEADS))
                    + dot_nt(b_ref[...], lanes(wb_ref, 0, HEADS))).astype(jnp.bfloat16)


def expand_kv_kernel(ids_ref, a_ref, b_ref, wa_ref, wb_ref, c_ref, d_ref, wc_ref, wd_ref, out_ref):
    out_ref[...] = (dot_nt(a_ref[...], lanes(wa_ref, 0, HEADS))
                    + dot_nt(b_ref[...], lanes(wb_ref, 0, HEADS))
                    + dot_nt(c_ref[...], wc_ref[...]) + dot_nt(d_ref[...], wd_ref[...])).astype(jnp.bfloat16)


def turn_kernel(ids_ref, a_ref, b_ref, out_ref):
    half = pl.num_programs(0) // 2

    @pl.when(pl.program_id(0) < half)
    def _():
        out_ref[...] = a_ref[...].T

    @pl.when(pl.program_id(0) >= half)
    def _():
        out_ref[...] = b_ref[...].T


def wgrad_one_kernel(partner, a_ref, b_ref, out_ref):
    tok = a_ref.shape[1] // 2
    first, second = (b_ref[tok:, :], b_ref[:tok, :]) if partner else (b_ref[:tok, :], b_ref[tok:, :])
    val = dot(a_ref[:, :tok], first) + dot(a_ref[:, tok:], second)
    for h in range(out_ref.shape[0]):
        out_ref[h] = val[:, h * HD:(h + 1) * HD]


def wgrad_kernel(ids_ref, a_ref, b_ref, c_ref, out_ref):
    step = pl.program_id(0)
    half = pl.num_programs(0) // 2
    tok = a_ref.shape[1] // 2

    def put(own, oth):
        val = dot(a_ref[:, :tok], own) + dot(a_ref[:, tok:], oth)
        for h in range(out_ref.shape[0]):
            out_ref[h] = val[:, h * HD:(h + 1) * HD]

    @pl.when(step < half)
    def _():
        put(b_ref[:tok, :], b_ref[tok:, :])

    @pl.when(step >= half)
    def _():
        put(c_ref[tok:, :], c_ref[:tok, :])


def whole(i, *_):
    return (0, 0)


def whole3(i, *_):
    return (0, 0, 0)


def lead(i, *_):
    return (i, 0, 0)


def params(mib):
    return pltpu.CompilerParams(dimension_semantics=('arbitrary',), vmem_limit_bytes=mib * 1024 * 1024)


def attend(seg, ids, q, kv_far, kv_near, rows):
    tok = q.shape[0]
    keys = 2 * tok
    grid = tok // BLK
    block = pl.BlockSpec((BLK, HEADS * HD), lambda i, *_: (i, 0))
    return pl.pallas_call(
        fwd_kernel,
        grid_spec=pltpu.PrefetchScalarGridSpec(
            num_scalar_prefetch=2, grid=(grid,),
            in_specs=[block] + [pl.BlockSpec((tok // 2, 2 * HD), whole)] * 4
            + [pl.BlockSpec((keys // BLK, 1, BLK), whole3)],
            out_specs=[block, pl.BlockSpec((1, 1, WIDE), lead), pl.BlockSpec(memory_space=pltpu.SMEM)],
            scratch_shapes=[pltpu.VMEM((keys, 128), jnp.int32), pltpu.VMEM((keys, 2 * HD), jnp.bfloat16),
                            pltpu.VMEM((HD, WIDE), jnp.bfloat16), pltpu.VMEM((HD, WIDE), jnp.float32),
                            pltpu.VMEM((1, WIDE), jnp.float32), pltpu.VMEM((8, WIDE), jnp.float32),
                            pltpu.VMEM((BLK, WIDE), jnp.bfloat16)]),
        out_shape=[jax.ShapeDtypeStruct((tok, HEADS * HD), jnp.bfloat16),
                   jax.ShapeDtypeStruct((grid, 1, WIDE), jnp.float32), jax.ShapeDtypeStruct((1,), jnp.int32)],
        compiler_params=params(24), name='attend',
        cost_estimate=pl.CostEstimate(flops=40 * 4 * WIDE * BLK * HD, bytes_accessed=12 << 20, transcendentals=0),
    )(seg, ids, q, *kv_far, *kv_near, rows)


def attend_grad(remote, seg, ids, q, do, o, kv, rows, lse, dq_in=None):
    tok = q.shape[0]
    grid = tok // BLK
    block = pl.BlockSpec((BLK, HEADS * HD), lambda i, *_: (i, 0))
    in_specs = [block] * 3 + [pl.BlockSpec((tok // 2, 2 * HD), whole)] * 2 + [
        pl.BlockSpec(rows.shape, whole3), pl.BlockSpec((1, 1, WIDE), lead)]
    args = [seg, ids, q, do, o, *kv, rows, lse]
    dqt_spec = pl.BlockSpec((1, HD, WIDE), lead)
    kv_grad = jax.ShapeDtypeStruct((tok, 2 * HD), jnp.float32)
    kv_spec = pl.BlockSpec((tok, 2 * HD), whole)
    extra = []
    if remote:
        shard = jax.ShapeDtypeStruct((tok // 2, 2 * HD), jnp.float32)
        out_shape = [jax.ShapeDtypeStruct((grid, HD, WIDE), jnp.float32), shard, shard]
        out_specs = [dqt_spec] + [pl.BlockSpec((tok // 2, 2 * HD), whole)] * 2
        extra = [pltpu.VMEM((tok, 2 * HD), jnp.float32)]
    else:
        in_specs.append(dqt_spec)
        args.append(dq_in)
        out_shape = [jax.ShapeDtypeStruct((tok, HEADS * HD), jnp.bfloat16), kv_grad]
        out_specs = [block, kv_spec]
    stack = pltpu.VMEM((WIDE, HD), jnp.bfloat16)
    flip = pltpu.VMEM((HD, WIDE), jnp.bfloat16)
    tile = pltpu.VMEM((BLK, WIDE), jnp.bfloat16)
    return pl.pallas_call(
        functools.partial(bwd_kernel, remote),
        grid_spec=pltpu.PrefetchScalarGridSpec(
            num_scalar_prefetch=2, grid=(grid,), in_specs=in_specs, out_specs=out_specs,
            scratch_shapes=[pltpu.VMEM((tok, 128), jnp.int32), pltpu.VMEM((tok, 2 * HD), jnp.bfloat16),
                            stack, flip, stack, flip, pltpu.VMEM((1, WIDE), jnp.float32),
                            tile, tile, pltpu.VMEM((HD, WIDE), jnp.float32)] + extra),
        out_shape=out_shape, compiler_params=params(28),
        name='attend_grad_remote' if remote else 'attend_grad_local',
        cost_estimate=pl.CostEstimate(flops=20 * 10 * WIDE * BLK * HD, bytes_accessed=20 << 20, transcendentals=0),
    )(*args)


def project(ids, a, b, w):
    tok, dim = a.shape
    return pl.pallas_call(
        project_kernel,
        grid_spec=pltpu.PrefetchScalarGridSpec(
            num_scalar_prefetch=1, grid=(2,),
            in_specs=[pl.BlockSpec((tok, dim), whole)] * 2
            + [pl.BlockSpec((HEADS, dim, HD), lambda t, ids: (ids[0], 0, 0))],
            out_specs=pl.BlockSpec((tok, HEADS * HD), lambda t, ids: (t, 0))),
        out_shape=jax.ShapeDtypeStruct((2 * tok, HEADS * HD), jnp.bfloat16),
        compiler_params=params(24),
        cost_estimate=pl.CostEstimate(flops=4 * tok * dim * HEADS * HD, bytes_accessed=12 << 20, transcendentals=0),
    )(ids, a, b, w)


def project_kv(ids, a, w_k, w_v):
    tok, dim = a.shape
    mine = jax.ShapeDtypeStruct((dim, 2 * HD), jnp.bfloat16)
    pack = pl.BlockSpec((2 * dim, HD), whole)
    return pl.pallas_call(
        project_kv_kernel,
        grid_spec=pltpu.PrefetchScalarGridSpec(
            num_scalar_prefetch=1, grid=(2,),
            in_specs=[pl.BlockSpec((tok // 2, dim), lambda i, ids: (i, 0)), pack, pack],
            out_specs=[pl.BlockSpec((tok // 2, 2 * HD), lambda i, ids: (i, 0))] * 2
            + [pl.BlockSpec((dim, 2 * HD), whole)] * 2,
            scratch_shapes=[pltpu.VMEM((2 * dim, HD), jnp.float32)]),
        out_shape=[jax.ShapeDtypeStruct((tok, 2 * HD), jnp.bfloat16)] * 2 + [mine, mine],
        compiler_params=params(60), name='project_kv',
        cost_estimate=pl.CostEstimate(flops=4 * tok * dim * HD, bytes_accessed=6 << 20, transcendentals=0),
    )(ids, a, w_k.reshape(2 * dim, HD), w_v.reshape(2 * dim, HD))


def expand(ids, a, b, w, extra=()):
    tok, width = a.shape[0] // 2, a.shape[1]
    dim = w.shape[1]
    cols = 512

    def first(i, ids):
        return (0, 0)

    def second(i, ids):
        return (1, 0)

    specs = [pl.BlockSpec((tok, width), first), pl.BlockSpec((tok, width), second),
             pl.BlockSpec((HEADS, cols, HD), lambda i, ids: (ids[0], i, 0)),
             pl.BlockSpec((HEADS, cols, HD), lambda i, ids: (1 - ids[0], i, 0))]
    args = [a, b, w, w]
    if extra:
        specs += [pl.BlockSpec((tok, 2 * HD), first), pl.BlockSpec((tok, 2 * HD), second)]
        specs += [pl.BlockSpec((cols, 2 * HD), lambda i, ids: (i, 0))] * 2
        args += extra
    return pl.pallas_call(
        expand_kv_kernel if extra else expand_kernel,
        grid_spec=pltpu.PrefetchScalarGridSpec(
            num_scalar_prefetch=1, grid=(dim // cols,), in_specs=specs,
            out_specs=pl.BlockSpec((tok, cols), lambda i, ids: (0, i))),
        out_shape=jax.ShapeDtypeStruct((tok, dim), jnp.bfloat16),
        compiler_params=params(20), name='grad_x' if extra else 'out_y',
        cost_estimate=pl.CostEstimate(flops=4 * tok * dim * width, bytes_accessed=14 << 20, transcendentals=0),
    )(ids, *args)


def turn(where, a, b):
    tok, dim = a.shape
    rows = dim // 4
    part = tok // 2
    return pl.pallas_call(
        turn_kernel,
        grid_spec=pltpu.PrefetchScalarGridSpec(
            num_scalar_prefetch=1, grid=(4,),
            in_specs=[pl.BlockSpec((part, rows), lambda i, ids: (jnp.minimum(i, 1), ids[0])),
                      pl.BlockSpec((part, rows), lambda i, ids: (jnp.maximum(i - 2, 0), ids[0]))],
            out_specs=pl.BlockSpec((rows, part), lambda i, ids: (0, i))),
        out_shape=jax.ShapeDtypeStruct((rows, 2 * tok), jnp.bfloat16),
        compiler_params=params(12),
        cost_estimate=pl.CostEstimate(flops=2 << 30, bytes_accessed=4 * rows * tok * 2, transcendentals=0),
    )(where.reshape(1).astype(jnp.int32), a, b)


def wgrad(core, a, b, c):
    rows, tok = a.shape
    width = b.shape[1]
    step = 256
    half = width // step
    heads = step // HD
    return pl.pallas_call(
        wgrad_kernel,
        grid_spec=pltpu.PrefetchScalarGridSpec(
            num_scalar_prefetch=1, grid=(2 * half,),
            in_specs=[pl.BlockSpec((rows, tok), whole),
                      pl.BlockSpec((tok, step), lambda i, ids: (0, jnp.minimum(i, half - 1))),
                      pl.BlockSpec((tok, step), lambda i, ids: (0, jnp.maximum(i - half, 0)))],
            out_specs=pl.BlockSpec((heads, rows, HD), lambda i, ids: (lax.rem(i + half * ids[0], 2 * half), 0, 0))),
        out_shape=jax.ShapeDtypeStruct((2 * width // HD, rows, HD), jnp.float32),
        compiler_params=params(16),
        cost_estimate=pl.CostEstimate(flops=4 * tok * rows * width, bytes_accessed=10 << 20, transcendentals=0),
    )(core.reshape(1).astype(jnp.int32), a, b, c)


def wgrad_one(a, b, partner):
    rows, tok = a.shape
    width = b.shape[1]
    step = 256
    heads = step // HD
    return pl.pallas_call(
        functools.partial(wgrad_one_kernel, partner),
        grid=(width // step,),
        in_specs=[pl.BlockSpec((rows, tok), whole), pl.BlockSpec((tok, step), lambda i: (0, i))],
        out_specs=pl.BlockSpec((heads, rows, HD), lambda i: (i, 0, 0)),
        out_shape=jax.ShapeDtypeStruct((width // HD, rows, HD), jnp.float32),
        compiler_params=params(16),
        cost_estimate=pl.CostEstimate(flops=2 * tok * rows * width, bytes_accessed=6 << 20, transcendentals=0),
    )(a, b)


def after(value, *others):
    return lax.optimization_barrier((value, *others))[0]


def solution(mesh):
    row_spec = P(('dp', 'cp'), None)
    tok_spec = P(('dp', 'cp'))
    weight_spec = P(None, None, None)
    grad_spec = P(('dp', 'cp'), None, None)
    core_pairs = [(0, 1), (1, 0), (2, 3), (3, 2)]
    chip_pairs = [(0, 2), (2, 0), (1, 3), (3, 1)]
    up_pairs = [(0, 2), (1, 3)]
    up_cross = [(0, 3), (1, 2)]
    down_pairs = [(2, 0), (3, 1)]

    def send(a, pairs):
        return lax.ppermute(a, 'cp', pairs)

    def layer(x, seg, w_q, w_k, w_v, w_o, dy):
        _, dim = x.shape
        rows = dim // 4
        index = lax.axis_index('cp')
        core = index % 2
        chip = index // 2
        near_rows = index
        far_rows = 2 * (1 - chip) + core
        ids = jnp.stack([core, chip]).astype(jnp.int32)
        w_q = jnp.transpose(w_q, (1, 0, 2))
        w_o = jnp.transpose(w_o, (1, 0, 2))

        x_o = send(x, core_pairs)
        kv_own, kv_pass, wkv_c, wkv_p = project_kv(ids, x, w_k, w_v)
        kv_far0 = send(kv_own, up_pairs)
        kv_far1 = send(kv_pass, up_cross)
        kv_oth = send(kv_pass, core_pairs)
        seg_o = send(after(seg, kv_own), core_pairs)
        dy_o = send(after(dy, kv_own), core_pairs)
        seg_far0 = send(after(seg, kv_own), up_pairs)
        seg_far1 = send(after(seg, kv_own), up_cross)
        seg_all = jnp.concatenate([seg_far0, seg_far1, seg, seg_o])
        seg_rows = seg_all.reshape(-1, 1, BLK)
        kv_far, kv_near = (kv_far0, kv_far1), (kv_own, kv_oth)
        q = project(ids, after(x, kv_own), x_o, w_q)
        dy_far = turn(far_rows, dy, dy_o)
        x_far = turn(far_rows, x, x_o)

        o, lse, reach = attend(seg_all, ids, q, kv_far, kv_near, seg_rows)
        o_p = send(o, core_pairs)
        dwo_far = wgrad_one(dy_far, o, False)
        dwo_in = send(dwo_far, chip_pairs)
        dwo_far2 = wgrad_one(dy_far, o_p, True)
        dwo_in2 = send(dwo_far2, chip_pairs)

        do = project(ids, after(dy, dwo_far), dy_o, w_o)
        dq_part, dkv_far0, dkv_far1 = attend_grad(True, seg_all, ids, q, do, o, kv_far, seg_rows, lse)
        dkv_in1 = send(dkv_far1, down_pairs)

        local = (seg_all, ids, q, do, o, kv_near, seg_rows, lse, dq_part)

        def sent(first, args):
            got = send(first, down_pairs)
            return *attend_grad(False, *args), got

        def kept(first, args):
            return *attend_grad(False, *args), jnp.zeros_like(first)

        dq, dkv_near, dkv_in0 = lax.cond(reach[0] != 0, sent, kept, dkv_far0, local)
        dq_p = send(dq, core_pairs)
        dwq_far1 = wgrad_one(x_far, dq, False)
        dwq_in = send(dwq_far1, chip_pairs)
        dwq_far = wgrad_one(x_far, dq_p, True)
        dwq_in2 = send(dwq_far, chip_pairs)

        y = expand(ids, after(o, dwq_far), o_p, w_o)
        x_near = turn(near_rows, after(x, dwq_far), x_o)
        dy_near = turn(near_rows, after(dy, dwq_far), dy_o)
        dwo_near = wgrad(core, dy_near, o, o_p)
        dwq_near = wgrad(core, x_near, dq, dq_p)

        dkv = dkv_near + jnp.where(core == 0, jnp.concatenate([dkv_in0, dkv_in1]),
                                   jnp.concatenate([dkv_in1, dkv_in0]))
        dkv = jnp.concatenate([dkv[:, :HD] * HD ** -0.5, dkv[:, HD:]], axis=1).astype(jnp.bfloat16)
        dkv_p = send(dkv, core_pairs)
        dwkv_far = wgrad(core, x_far, dkv, dkv_p)
        dwkv_in = send(dwkv_far, chip_pairs)
        dwkv_near = wgrad(core, x_near, after(dkv, dwkv_far), dkv_p)
        dx = expand(ids, after(dq, dwkv_far), dq_p, w_q, (dkv, dkv_p, wkv_c, wkv_p))

        def total(near, mine, other):
            far = jnp.where(core == 0, jnp.concatenate([mine, other]), jnp.concatenate([other, mine]))
            return jnp.transpose(near + far, (1, 0, 2))

        dw_o = total(dwo_near, dwo_in, dwo_in2)
        dw_q = total(dwq_near, dwq_in, dwq_in2)
        dw_kv = jnp.transpose(dwkv_near + dwkv_in, (1, 0, 2)).reshape(rows, 2, 2, HD)
        return y, dx, dw_q, dw_kv[:, :, 0], dw_kv[:, :, 1], dw_o

    return jax.shard_map(layer, mesh=mesh,
                         in_specs=(row_spec, tok_spec, weight_spec, weight_spec, weight_spec, weight_spec, row_spec),
                         out_specs=(row_spec, row_spec, grad_spec, grad_spec, grad_spec, grad_spec),
                         check_vma=False)
```

```python
import functools
import math

import jax
import jax.numpy as jnp
from jax import lax
from jax.experimental import pallas as pl
from jax.experimental.pallas import tpu as pltpu
from jax.sharding import PartitionSpec as P

BLK = 256
HEADS = 6
HD = 128
WIDE = HEADS * BLK
HALF = 8


def dot(a, b):
    return jnp.dot(a, b, preferred_element_type=jnp.float32)


def dot_nt(a, b):
    return lax.dot_general(a, b, (((1,), (1,)), ((), ())), preferred_element_type=jnp.float32)


def stack_heads(src, dst):
    for h in range(HEADS):
        dst[h * BLK:(h + 1) * BLK, :] = src[:, h * HD:(h + 1) * HD]


def flip_heads(src, dst):
    for h in range(HEADS):
        dst[:, h * BLK:(h + 1) * BLK] = src[:, h * HD:(h + 1) * HD].T


def store_block(p, core):
    return (p & HALF) + ((p + 4 * core) & (HALF - 1))


def first_block(seg_ref, ids_ref, step):
    chip = ids_ref[1]
    first = seg_ref[(HALF + step) * BLK]
    near = jnp.int32(0)
    far = jnp.int32(0)
    for b in range(HALF):
        far += (seg_ref[b * BLK + BLK - 1] < first).astype(jnp.int32)
        near += (seg_ref[(HALF + b) * BLK + BLK - 1] < first).astype(jnp.int32)
    far = jnp.where(chip == 0, HALF, far)
    return far + near


def spread_segments(rows_ref, dst, first, count):
    for b in range(count):
        row = jnp.broadcast_to(rows_ref[first + b], (128, BLK))
        dst[b * BLK:(b + 1) * BLK, :] = row.T


def pair_mask(segk, segq, key_block, query_block):
    segk = jnp.concatenate([segk] * (BLK // 128), axis=1)
    same = segk == segq
    rel = (lax.broadcasted_iota(jnp.int32, (BLK, BLK), 0)
           - lax.broadcasted_iota(jnp.int32, (BLK, BLK), 1))
    return same & (rel <= (query_block - key_block) * BLK)


def full_blocks(seg_ref, ids_ref, step, hi):
    last = seg_ref[(HALF + step) * BLK + BLK - 1]
    count = jnp.int32(0)
    for p in range(2 * HALF):
        same = seg_ref[store_block(p, ids_ref[0]) * BLK] == last
        count += (same & (p < hi)).astype(jnp.int32)
    return count


def fwd_kernel(seg_ref, ids_ref, q_ref, kv_far0, kv_far1, kv_own, kv_oth, rows_ref, o_ref, lse_ref, reach_ref,
               segk, kv_ref, qt, acc, m_ref, l_ref, pm):
    step = pl.program_id(0)
    core = ids_ref[0]
    scale2 = HD ** -0.5 * math.log2(math.e)
    tok = kv_own.shape[0]

    @pl.when(step == 0)
    def _():
        spread_segments(rows_ref, segk, 0, 2 * HALF)
        first = jnp.where(ids_ref[1] == 0, HALF, 0)
        ends = [seg_ref[store_block(first + p, core) * BLK + BLK - 1] for p in (3, 5, 7)]
        reach_ref[0] = (ends[0] == ends[2]).astype(jnp.int32) + (ends[1] == ends[2]).astype(jnp.int32)

        for i, part in enumerate((kv_far0, kv_far1, kv_own, kv_oth)):
            kv_ref[i * tok:(i + 1) * tok, :] = part[...]

    flip_heads(q_ref, qt)
    hi = HALF + ((step + 4 * core) & (HALF - 1))
    lo = first_block(seg_ref, ids_ref, step)
    full = jnp.maximum(hi - full_blocks(seg_ref, ids_ref, step, hi), lo)
    segq = rows_ref[HALF + step]

    def start_of(p):
        return pl.multiple_of(store_block(p, core) * BLK, BLK)

    def fold(w):
        return jnp.sum(w.reshape(BLK // 8, 8, BLK), axis=0)

    def keys(start):
        return kv_ref[pl.ds(start, BLK), :HD]

    def values(start):
        return kv_ref[pl.ds(pl.multiple_of(start, BLK), BLK), HD:].T

    def mask_of(start, p):
        return pair_mask(segk[pl.ds(start, BLK), :], segq, p, hi)

    def diagonal():
        start = start_of(hi)
        mask = mask_of(start, hi)
        for h in range(HEADS):
            cols = slice(h * BLK, (h + 1) * BLK)
            s = jnp.where(mask, dot(keys(start), qt[:, cols]) * scale2, -jnp.inf)
            top = jnp.max(s, axis=0, keepdims=True)
            w = jnp.exp2(s - top)
            m_ref[:, cols] = top
            l_ref[:, cols] = fold(w)
            pm[:, cols] = w.astype(jnp.bfloat16)
        acc[...] = jnp.zeros_like(acc)
        return start

    def weigh(p, prev, masked):
        start = start_of(p)
        v_t = values(prev)
        k_blk = keys(start)
        if masked:
            mask = mask_of(start, p)
        for h in range(HEADS):
            cols = slice(h * BLK, (h + 1) * BLK)
            s = dot(k_blk, qt[:, cols]) * scale2 - m_ref[:, cols]
            acc[:, cols] += dot(v_t, pm[:, cols])
            if masked:
                s = jnp.where(mask, s, -jnp.inf)
            w = jnp.exp2(s)
            l_ref[:, cols] += fold(w)
            pm[:, cols] = w.astype(jnp.bfloat16)
        return start

    prev = diagonal()
    prev = lax.fori_loop(0, hi - full, lambda i, c: weigh(hi - 1 - i, c, False), prev)
    prev = lax.fori_loop(0, full - lo, lambda i, c: weigh(full - 1 - i, c, True), prev)
    acc[...] += dot(values(prev), pm[...])

    @pl.when(jnp.logical_not(jnp.max(l_ref[...]) <= 2.0 ** 20))
    def _():
        def safe(i, carry):
            p = hi - 1 - i
            start = start_of(p)
            mask = mask_of(start, p)
            for h in range(HEADS):
                cols = slice(h * BLK, (h + 1) * BLK)
                s = jnp.where(mask, dot(keys(start), qt[:, cols]) * scale2, -jnp.inf)
                top = jnp.maximum(m_ref[:, cols], jnp.max(s, axis=0, keepdims=True))
                fac = jnp.exp2(m_ref[:, cols] - top)
                w = jnp.exp2(s - top)
                m_ref[:, cols] = top
                l_ref[:, cols] = l_ref[:, cols] * fac + fold(w)
                acc[:, cols] = acc[:, cols] * fac + dot(values(start), w.astype(jnp.bfloat16))
            return carry

        first = diagonal()
        acc[...] += dot(values(first), pm[...])
        lax.fori_loop(0, hi - lo, safe, 0)

    total = jnp.sum(l_ref[...], axis=0, keepdims=True)
    lse_ref[0] = m_ref[...] + jnp.log2(total)
    inv = 1.0 / total

    for h in range(HEADS):
        cols = slice(h * BLK, (h + 1) * BLK)
        o_ref[:, h * HD:(h + 1) * HD] = (acc[:, cols] * inv[:, cols]).T.astype(jnp.bfloat16)


def bwd_kernel(remote, *refs):
    if remote:
        (seg_ref, ids_ref, q_ref, do_ref, o_ref, kv_own, kv_oth,
         rows_ref, lse_ref, dq_out, dkv_first, dkv_second, dkv_third,
         segk, kv_ref, qs, qt, ds_, dt, delta, pm, sm, dqt, dkv_ref) = refs
    else:
        (seg_ref, ids_ref, q_ref, do_ref, o_ref, kv_own, kv_oth,
         rows_ref, lse_ref, dq_in, dq_out, dkv_ref,
         segk, kv_ref, qs, qt, ds_, dt, delta, pm, sm, dqt) = refs
    step = pl.program_id(0)
    core = ids_ref[0]
    scale = HD ** -0.5
    scale2 = scale * math.log2(math.e)

    @pl.when(step == 0)
    def _():
        dkv_ref[...] = jnp.zeros_like(dkv_ref)
        spread_segments(rows_ref, segk, 0 if remote else HALF, HALF)
        tok = kv_own.shape[0]
        kv_ref[:tok, :] = kv_own[...]
        kv_ref[tok:, :] = kv_oth[...]

    query = HALF + ((step + 4 * core) & (HALF - 1))
    first = first_block(seg_ref, ids_ref, step)
    if remote:
        lo, hi = first, jnp.int32(HALF - 1)
    else:
        lo, hi = jnp.maximum(first, HALF), query
    count = hi - lo + 1
    segq = rows_ref[HALF + step]

    @pl.when(count > 0)
    def _():
        stack_heads(q_ref, qs)
        flip_heads(q_ref, qt)
        stack_heads(do_ref, ds_)
        flip_heads(do_ref, dt)
        for h in range(HEADS):
            hc = slice(h * HD, (h + 1) * HD)
            prod = do_ref[:, hc].astype(jnp.float32) * o_ref[:, hc].astype(jnp.float32)
            delta[:, h * BLK:(h + 1) * BLK] = jnp.sum(prod.T, axis=0, keepdims=True)

    if remote:
        dqt[...] = jnp.zeros_like(dqt)
    else:
        dqt[...] = dq_in[0]

    def body(it, carry):
        p = lo + it
        key_start = pl.multiple_of((store_block(p, core) & (HALF - 1)) * BLK, BLK)
        k_blk = kv_ref[pl.ds(key_start, BLK), :HD]
        v_blk = kv_ref[pl.ds(key_start, BLK), HD:]
        mask = pair_mask(segk[pl.ds(key_start, BLK), :], segq, p, query)
        for h in range(HEADS):
            cols = slice(h * BLK, (h + 1) * BLK)
            s = dot(k_blk, qt[:, cols])
            w = jnp.where(mask, jnp.exp2(s * scale2 - lse_ref[0, :, cols]), 0.0)
            dp = dot(v_blk, dt[:, cols])
            dsv = w * (dp - delta[:, cols])
            pm[:, cols] = w.astype(jnp.bfloat16)
            sm[:, cols] = dsv.astype(jnp.bfloat16)
        put = pl.multiple_of(p * BLK, BLK) if remote else key_start
        dkv_ref[pl.ds(put, BLK), HD:] += dot(pm[...], ds_[...])
        dkv_ref[pl.ds(put, BLK), :HD] += dot(sm[...], qs[...])
        dqt[...] += dot(k_blk.T, sm[...])
        return carry

    lax.fori_loop(0, count, body, 0)
    if remote:
        dq_out[0] = dqt[...]

        @pl.when(step == pl.num_programs(0) - 1)
        def _():
            at = 0
            for part in (dkv_first, dkv_second, dkv_third):
                part[...] = dkv_ref[at:at + part.shape[0], :]
                at += part.shape[0]
    else:
        for h in range(HEADS):
            cols = slice(h * BLK, (h + 1) * BLK)
            dq_out[:, h * HD:(h + 1) * HD] = (dqt[:, cols] * scale).T.astype(jnp.bfloat16)


def lanes(ref, first, count):
    return jnp.concatenate([ref[first + h] for h in range(count)], axis=1)


def project_kernel(ids_ref, a_own, a_oth, w_ref, out_ref):
    half = out_ref.shape[0] // 2

    def put(src):
        for n in range(0, HEADS, 2):
            weight = jnp.concatenate([w_ref[n], w_ref[n + 1]], axis=1)
            for t in (0, half):
                out_ref[t:t + half, n * HD:(n + 2) * HD] = dot(src[t:t + half, :], weight).astype(jnp.bfloat16)

    @pl.when(pl.program_id(0) == 0)
    def _():
        put(a_own)

    @pl.when(pl.program_id(0) == 1)
    def _():
        put(a_oth)


def project_kv_kernel(ids_ref, a_ref, wk_ref, wv_ref, out_ref, pass_ref, mine_ref, other_ref, wide):
    @pl.when(pl.program_id(0) == 0)
    def _():
        dim = mine_ref.shape[0]
        for i, ref in enumerate((wk_ref, wv_ref)):
            wide[...] = ref[...].astype(jnp.float32)
            cols = slice(i * HD, (i + 1) * HD)
            mine_ref[:, cols] = wide[pl.ds(ids_ref[0], dim, stride=2), :].astype(jnp.bfloat16)
            other_ref[:, cols] = wide[pl.ds(1 - ids_ref[0], dim, stride=2), :].astype(jnp.bfloat16)

    out_ref[...] = dot(a_ref[...], mine_ref[...]).astype(jnp.bfloat16)
    pass_ref[...] = dot(a_ref[...], other_ref[...]).astype(jnp.bfloat16)


def expand_kernel(ids_ref, a_ref, b_ref, wa_ref, wb_ref, out_ref):
    out_ref[...] = (dot_nt(a_ref[...], lanes(wa_ref, 0, HEADS))
                    + dot_nt(b_ref[...], lanes(wb_ref, 0, HEADS))).astype(jnp.bfloat16)


def expand_kv_kernel(ids_ref, a_ref, b_ref, wa_ref, wb_ref, c_ref, d_ref, wc_ref, wd_ref, out_ref):
    out_ref[...] = (dot_nt(a_ref[...], lanes(wa_ref, 0, HEADS))
                    + dot_nt(b_ref[...], lanes(wb_ref, 0, HEADS))
                    + dot_nt(c_ref[...], wc_ref[...]) + dot_nt(d_ref[...], wd_ref[...])).astype(jnp.bfloat16)


def turn_kernel(ids_ref, a_ref, b_ref, out_ref):
    half = pl.num_programs(0) // 2

    @pl.when(pl.program_id(0) < half)
    def _():
        out_ref[...] = a_ref[...].T

    @pl.when(pl.program_id(0) >= half)
    def _():
        out_ref[...] = b_ref[...].T


def wgrad_one_kernel(partner, a_ref, b_ref, out_ref):
    tok = a_ref.shape[1] // 2
    first, second = (b_ref[tok:, :], b_ref[:tok, :]) if partner else (b_ref[:tok, :], b_ref[tok:, :])
    val = dot(a_ref[:, :tok], first) + dot(a_ref[:, tok:], second)
    for h in range(out_ref.shape[0]):
        out_ref[h] = val[:, h * HD:(h + 1) * HD]


def wgrad_kernel(ids_ref, a_ref, b_ref, c_ref, out_ref):
    step = pl.program_id(0)
    half = pl.num_programs(0) // 2
    tok = a_ref.shape[1] // 2

    def put(own, oth):
        val = dot(a_ref[:, :tok], own) + dot(a_ref[:, tok:], oth)
        for h in range(out_ref.shape[0]):
            out_ref[h] = val[:, h * HD:(h + 1) * HD]

    @pl.when(step < half)
    def _():
        put(b_ref[:tok, :], b_ref[tok:, :])

    @pl.when(step >= half)
    def _():
        put(c_ref[tok:, :], c_ref[:tok, :])


def whole(i, *_):
    return (0, 0)


def whole3(i, *_):
    return (0, 0, 0)


def lead(i, *_):
    return (i, 0, 0)


def params(mib):
    return pltpu.CompilerParams(dimension_semantics=('arbitrary',), vmem_limit_bytes=mib * 1024 * 1024)


def attend(seg, ids, q, kv_far, kv_near, rows):
    tok = q.shape[0]
    keys = 2 * tok
    grid = tok // BLK
    block = pl.BlockSpec((BLK, HEADS * HD), lambda i, *_: (i, 0))
    return pl.pallas_call(
        fwd_kernel,
        grid_spec=pltpu.PrefetchScalarGridSpec(
            num_scalar_prefetch=2, grid=(grid,),
            in_specs=[block] + [pl.BlockSpec((tok // 2, 2 * HD), whole)] * 4
            + [pl.BlockSpec((keys // BLK, 1, BLK), whole3)],
            out_specs=[block, pl.BlockSpec((1, 1, WIDE), lead), pl.BlockSpec(memory_space=pltpu.SMEM)],
            scratch_shapes=[pltpu.VMEM((keys, 128), jnp.int32), pltpu.VMEM((keys, 2 * HD), jnp.bfloat16),
                            pltpu.VMEM((HD, WIDE), jnp.bfloat16), pltpu.VMEM((HD, WIDE), jnp.float32),
                            pltpu.VMEM((1, WIDE), jnp.float32), pltpu.VMEM((8, WIDE), jnp.float32),
                            pltpu.VMEM((BLK, WIDE), jnp.bfloat16)]),
        out_shape=[jax.ShapeDtypeStruct((tok, HEADS * HD), jnp.bfloat16),
                   jax.ShapeDtypeStruct((grid, 1, WIDE), jnp.float32), jax.ShapeDtypeStruct((1,), jnp.int32)],
        compiler_params=params(24), name='attend',
        cost_estimate=pl.CostEstimate(flops=40 * 4 * WIDE * BLK * HD, bytes_accessed=12 << 20, transcendentals=0),
    )(seg, ids, q, *kv_far, *kv_near, rows)


def attend_grad(remote, seg, ids, q, do, o, kv, rows, lse, dq_in=None):
    tok = q.shape[0]
    grid = tok // BLK
    block = pl.BlockSpec((BLK, HEADS * HD), lambda i, *_: (i, 0))
    in_specs = [block] * 3 + [pl.BlockSpec((tok // 2, 2 * HD), whole)] * 2 + [
        pl.BlockSpec(rows.shape, whole3), pl.BlockSpec((1, 1, WIDE), lead)]
    args = [seg, ids, q, do, o, *kv, rows, lse]
    dqt_spec = pl.BlockSpec((1, HD, WIDE), lead)
    kv_grad = jax.ShapeDtypeStruct((tok, 2 * HD), jnp.float32)
    kv_spec = pl.BlockSpec((tok, 2 * HD), whole)
    extra = []
    if remote:
        parts = [(n, 2 * HD) for n in (tok // 2, tok // 4, tok // 4)]
        out_shape = [jax.ShapeDtypeStruct((grid, HD, WIDE), jnp.float32)]
        out_shape += [jax.ShapeDtypeStruct(part, jnp.float32) for part in parts]
        out_specs = [dqt_spec] + [pl.BlockSpec(part, whole) for part in parts]
        extra = [pltpu.VMEM((tok, 2 * HD), jnp.float32)]
    else:
        in_specs.append(dqt_spec)
        args.append(dq_in)
        out_shape = [jax.ShapeDtypeStruct((tok, HEADS * HD), jnp.bfloat16), kv_grad]
        out_specs = [block, kv_spec]
    stack = pltpu.VMEM((WIDE, HD), jnp.bfloat16)
    flip = pltpu.VMEM((HD, WIDE), jnp.bfloat16)
    tile = pltpu.VMEM((BLK, WIDE), jnp.bfloat16)
    return pl.pallas_call(
        functools.partial(bwd_kernel, remote),
        grid_spec=pltpu.PrefetchScalarGridSpec(
            num_scalar_prefetch=2, grid=(grid,), in_specs=in_specs, out_specs=out_specs,
            scratch_shapes=[pltpu.VMEM((tok, 128), jnp.int32), pltpu.VMEM((tok, 2 * HD), jnp.bfloat16),
                            stack, flip, stack, flip, pltpu.VMEM((1, WIDE), jnp.float32),
                            tile, tile, pltpu.VMEM((HD, WIDE), jnp.float32)] + extra),
        out_shape=out_shape, compiler_params=params(28),
        name='attend_grad_remote' if remote else 'attend_grad_local',
        cost_estimate=pl.CostEstimate(flops=20 * 10 * WIDE * BLK * HD, bytes_accessed=20 << 20, transcendentals=0),
    )(*args)


def project(ids, a, b, w):
    tok, dim = a.shape
    return pl.pallas_call(
        project_kernel,
        grid_spec=pltpu.PrefetchScalarGridSpec(
            num_scalar_prefetch=1, grid=(2,),
            in_specs=[pl.BlockSpec((tok, dim), whole)] * 2
            + [pl.BlockSpec((HEADS, dim, HD), lambda t, ids: (ids[0], 0, 0))],
            out_specs=pl.BlockSpec((tok, HEADS * HD), lambda t, ids: (t, 0))),
        out_shape=jax.ShapeDtypeStruct((2 * tok, HEADS * HD), jnp.bfloat16),
        compiler_params=params(24),
        cost_estimate=pl.CostEstimate(flops=4 * tok * dim * HEADS * HD, bytes_accessed=12 << 20, transcendentals=0),
    )(ids, a, b, w)


def project_kv(ids, a, w_k, w_v):
    tok, dim = a.shape
    mine = jax.ShapeDtypeStruct((dim, 2 * HD), jnp.bfloat16)
    pack = pl.BlockSpec((2 * dim, HD), whole)
    return pl.pallas_call(
        project_kv_kernel,
        grid_spec=pltpu.PrefetchScalarGridSpec(
            num_scalar_prefetch=1, grid=(2,),
            in_specs=[pl.BlockSpec((tok // 2, dim), lambda i, ids: (i, 0)), pack, pack],
            out_specs=[pl.BlockSpec((tok // 2, 2 * HD), lambda i, ids: (i, 0))] * 2
            + [pl.BlockSpec((dim, 2 * HD), whole)] * 2,
            scratch_shapes=[pltpu.VMEM((2 * dim, HD), jnp.float32)]),
        out_shape=[jax.ShapeDtypeStruct((tok, 2 * HD), jnp.bfloat16)] * 2 + [mine, mine],
        compiler_params=params(60), name='project_kv',
        cost_estimate=pl.CostEstimate(flops=4 * tok * dim * HD, bytes_accessed=6 << 20, transcendentals=0),
    )(ids, a, w_k.reshape(2 * dim, HD), w_v.reshape(2 * dim, HD))


def expand(ids, a, b, w, extra=()):
    tok, width = a.shape[0] // 2, a.shape[1]
    dim = w.shape[1]
    cols = 512

    def first(i, ids):
        return (0, 0)

    def second(i, ids):
        return (1, 0)

    specs = [pl.BlockSpec((tok, width), first), pl.BlockSpec((tok, width), second),
             pl.BlockSpec((HEADS, cols, HD), lambda i, ids: (ids[0], i, 0)),
             pl.BlockSpec((HEADS, cols, HD), lambda i, ids: (1 - ids[0], i, 0))]
    args = [a, b, w, w]
    if extra:
        specs += [pl.BlockSpec((tok, 2 * HD), first), pl.BlockSpec((tok, 2 * HD), second)]
        specs += [pl.BlockSpec((cols, 2 * HD), lambda i, ids: (i, 0))] * 2
        args += extra
    return pl.pallas_call(
        expand_kv_kernel if extra else expand_kernel,
        grid_spec=pltpu.PrefetchScalarGridSpec(
            num_scalar_prefetch=1, grid=(dim // cols,), in_specs=specs,
            out_specs=pl.BlockSpec((tok, cols), lambda i, ids: (0, i))),
        out_shape=jax.ShapeDtypeStruct((tok, dim), jnp.bfloat16),
        compiler_params=params(20), name='grad_x' if extra else 'out_y',
        cost_estimate=pl.CostEstimate(flops=4 * tok * dim * width, bytes_accessed=14 << 20, transcendentals=0),
    )(ids, *args)


def turn(where, a, b):
    tok, dim = a.shape
    rows = dim // 4
    part = tok // 2
    return pl.pallas_call(
        turn_kernel,
        grid_spec=pltpu.PrefetchScalarGridSpec(
            num_scalar_prefetch=1, grid=(4,),
            in_specs=[pl.BlockSpec((part, rows), lambda i, ids: (jnp.minimum(i, 1), ids[0])),
                      pl.BlockSpec((part, rows), lambda i, ids: (jnp.maximum(i - 2, 0), ids[0]))],
            out_specs=pl.BlockSpec((rows, part), lambda i, ids: (0, i))),
        out_shape=jax.ShapeDtypeStruct((rows, 2 * tok), jnp.bfloat16),
        compiler_params=params(12),
        cost_estimate=pl.CostEstimate(flops=2 << 30, bytes_accessed=4 * rows * tok * 2, transcendentals=0),
    )(where.reshape(1).astype(jnp.int32), a, b)


def wgrad(core, a, b, c):
    rows, tok = a.shape
    width = b.shape[1]
    step = 256
    half = width // step
    heads = step // HD
    return pl.pallas_call(
        wgrad_kernel,
        grid_spec=pltpu.PrefetchScalarGridSpec(
            num_scalar_prefetch=1, grid=(2 * half,),
            in_specs=[pl.BlockSpec((rows, tok), whole),
                      pl.BlockSpec((tok, step), lambda i, ids: (0, jnp.minimum(i, half - 1))),
                      pl.BlockSpec((tok, step), lambda i, ids: (0, jnp.maximum(i - half, 0)))],
            out_specs=pl.BlockSpec((heads, rows, HD), lambda i, ids: (lax.rem(i + half * ids[0], 2 * half), 0, 0))),
        out_shape=jax.ShapeDtypeStruct((2 * width // HD, rows, HD), jnp.float32),
        compiler_params=params(16),
        cost_estimate=pl.CostEstimate(flops=4 * tok * rows * width, bytes_accessed=10 << 20, transcendentals=0),
    )(core.reshape(1).astype(jnp.int32), a, b, c)


def wgrad_one(a, b, partner):
    rows, tok = a.shape
    width = b.shape[1]
    step = 256
    heads = step // HD
    return pl.pallas_call(
        functools.partial(wgrad_one_kernel, partner),
        grid=(width // step,),
        in_specs=[pl.BlockSpec((rows, tok), whole), pl.BlockSpec((tok, step), lambda i: (0, i))],
        out_specs=pl.BlockSpec((heads, rows, HD), lambda i: (i, 0, 0)),
        out_shape=jax.ShapeDtypeStruct((width // HD, rows, HD), jnp.float32),
        compiler_params=params(16),
        cost_estimate=pl.CostEstimate(flops=2 * tok * rows * width, bytes_accessed=6 << 20, transcendentals=0),
    )(a, b)


def after(value, *others):
    return lax.optimization_barrier((value, *others))[0]


def solution(mesh):
    row_spec = P(('dp', 'cp'), None)
    tok_spec = P(('dp', 'cp'))
    weight_spec = P(None, None, None)
    grad_spec = P(('dp', 'cp'), None, None)
    core_pairs = [(0, 1), (1, 0), (2, 3), (3, 2)]
    chip_pairs = [(0, 2), (2, 0), (1, 3), (3, 1)]
    up_pairs = [(0, 2), (1, 3)]
    up_cross = [(0, 3), (1, 2)]
    down_pairs = [(2, 0), (3, 1)]

    def send(a, pairs):
        return lax.ppermute(a, 'cp', pairs)

    def layer(x, seg, w_q, w_k, w_v, w_o, dy):
        _, dim = x.shape
        rows = dim // 4
        index = lax.axis_index('cp')
        core = index % 2
        chip = index // 2
        near_rows = index
        far_rows = 2 * (1 - chip) + core
        ids = jnp.stack([core, chip]).astype(jnp.int32)
        w_q = jnp.transpose(w_q, (1, 0, 2))
        w_o = jnp.transpose(w_o, (1, 0, 2))

        x_o = send(x, core_pairs)
        kv_own, kv_pass, wkv_c, wkv_p = project_kv(ids, x, w_k, w_v)
        kv_far0 = send(kv_own, up_pairs)
        kv_far1 = send(kv_pass, up_cross)
        kv_oth = send(kv_pass, core_pairs)
        seg_o = send(after(seg, kv_own), core_pairs)
        dy_o = send(after(dy, kv_own), core_pairs)
        seg_far0 = send(after(seg, kv_own), up_pairs)
        seg_far1 = send(after(seg, kv_own), up_cross)
        seg_all = jnp.concatenate([seg_far0, seg_far1, seg, seg_o])
        seg_rows = seg_all.reshape(-1, 1, BLK)
        kv_far, kv_near = (kv_far0, kv_far1), (kv_own, kv_oth)
        q = project(ids, after(x, kv_own), x_o, w_q)
        dy_far = turn(far_rows, dy, dy_o)
        x_far = turn(far_rows, x, x_o)

        o, lse, reach = attend(seg_all, ids, q, kv_far, kv_near, seg_rows)
        o_p = send(o, core_pairs)
        dwo_far = wgrad_one(dy_far, o, False)
        dwo_in = send(dwo_far, chip_pairs)
        dwo_far2 = wgrad_one(dy_far, o_p, True)
        dwo_in2 = send(dwo_far2, chip_pairs)

        do = project(ids, after(dy, dwo_far), dy_o, w_o)
        dq_part, *far = attend_grad(True, seg_all, ids, q, do, o, kv_far, seg_rows, lse)
        last_in = send(far[2], down_pairs)
        local = (seg_all, ids, q, do, o, kv_near, seg_rows, lse, dq_part)

        def near_pass(level):
            def run(first, second, x_far, args):
                second_in = send(second, down_pairs) if level > 0 else jnp.zeros_like(second)
                first_in = send(first, down_pairs) if level > 1 else jnp.zeros_like(first)
                dq, dkv = attend_grad(False, *args)
                return dq, dkv, wgrad_one(x_far, dq, False), first_in, second_in

            return run

        dq, dkv_near, dwq_far1, first_in, second_in = lax.switch(
            reach[0], [near_pass(level) for level in range(3)], far[0], far[1], x_far, local)
        dwq_in = send(dwq_far1, chip_pairs)
        dq_p = send(dq, core_pairs)
        dwq_far = wgrad_one(x_far, dq_p, True)
        dwq_in2 = send(dwq_far, chip_pairs)

        y = expand(ids, after(o, dwq_far), o_p, w_o)
        x_near = turn(near_rows, after(x, dwq_far), x_o)
        dy_near = turn(near_rows, after(dy, dwq_far), dy_o)
        dwo_near = wgrad(core, dy_near, o, o_p)
        dwq_near = wgrad(core, x_near, dq, dq_p)

        dkv = dkv_near + jnp.where(core == 0, jnp.concatenate([first_in, second_in, last_in]),
                                   jnp.concatenate([second_in, last_in, first_in]))
        dkv = jnp.concatenate([dkv[:, :HD] * HD ** -0.5, dkv[:, HD:]], axis=1).astype(jnp.bfloat16)
        dkv_p = send(dkv, core_pairs)
        dwkv_far = wgrad(core, x_far, dkv, dkv_p)
        dwkv_in = send(dwkv_far, chip_pairs)
        dwkv_near = wgrad(core, x_near, after(dkv, dwkv_far), dkv_p)
        dx = expand(ids, after(dq, dwkv_far), dq_p, w_q, (dkv, dkv_p, wkv_c, wkv_p))

        def total(near, mine, other):
            far = jnp.where(core == 0, jnp.concatenate([mine, other]), jnp.concatenate([other, mine]))
            return jnp.transpose(near + far, (1, 0, 2))

        dw_o = total(dwo_near, dwo_in, dwo_in2)
        dw_q = total(dwq_near, dwq_in, dwq_in2)
        dw_kv = jnp.transpose(dwkv_near + dwkv_in, (1, 0, 2)).reshape(rows, 2, 2, HD)
        return y, dx, dw_q, dw_kv[:, :, 0], dw_kv[:, :, 1], dw_o

    return jax.shard_map(layer, mesh=mesh,
                         in_specs=(row_spec, tok_spec, weight_spec, weight_spec, weight_spec, weight_spec, row_spec),
                         out_specs=(row_spec, row_spec, grad_spec, grad_spec, grad_spec, grad_spec),
                         check_vma=False)
```

```python
import functools
import math

import jax
import jax.numpy as jnp
from jax import lax
from jax.experimental import pallas as pl
from jax.experimental.pallas import tpu as pltpu
from jax.sharding import PartitionSpec as P

BLK = 256
HEADS = 6
HD = 128
WIDE = HEADS * BLK
HALF = 8


def dot(a, b):
    return jnp.dot(a, b, preferred_element_type=jnp.float32)


def dot_nt(a, b):
    return lax.dot_general(a, b, (((1,), (1,)), ((), ())), preferred_element_type=jnp.float32)


def flip_heads(src, dst):
    for h in range(HEADS):
        dst[:, h * BLK:(h + 1) * BLK] = src[:, h * HD:(h + 1) * HD].T


def store_block(p, core):
    return (p & HALF) + ((p + 4 * core) & (HALF - 1))


def first_block(seg_ref, ids_ref, step):
    chip = ids_ref[1]
    first = seg_ref[(HALF + step) * BLK]
    near = jnp.int32(0)
    far = jnp.int32(0)
    for b in range(HALF):
        far += (seg_ref[b * BLK + BLK - 1] < first).astype(jnp.int32)
        near += (seg_ref[(HALF + b) * BLK + BLK - 1] < first).astype(jnp.int32)
    far = jnp.where(chip == 0, HALF, far)
    return far + near


def spread_segments(rows_ref, dst, first, count):
    for b in range(count):
        row = jnp.broadcast_to(rows_ref[first + b], (128, BLK))
        dst[b * BLK:(b + 1) * BLK, :] = row.T


def pair_mask(segk, segq, key_block, query_block):
    segk = jnp.concatenate([segk] * (BLK // 128), axis=1)
    same = segk == segq
    rel = (lax.broadcasted_iota(jnp.int32, (BLK, BLK), 0)
           - lax.broadcasted_iota(jnp.int32, (BLK, BLK), 1))
    return same & (rel <= (query_block - key_block) * BLK)


def full_blocks(seg_ref, ids_ref, step, hi):
    last = seg_ref[(HALF + step) * BLK + BLK - 1]
    count = jnp.int32(0)
    for p in range(2 * HALF):
        same = seg_ref[store_block(p, ids_ref[0]) * BLK] == last
        count += (same & (p < hi)).astype(jnp.int32)
    return count


def fwd_kernel(seg_ref, ids_ref, q_ref, kv_far0, kv_far1, kv_own, kv_oth, rows_ref, o_ref, lse_ref, reach_ref,
               segk, kv_ref, qt, acc, m_ref, l_ref, pm):
    step = pl.program_id(0)
    core = ids_ref[0]
    scale2 = HD ** -0.5 * math.log2(math.e)
    tok = kv_own.shape[0]

    @pl.when(step == 0)
    def _():
        spread_segments(rows_ref, segk, 0, 2 * HALF)
        first = jnp.where(ids_ref[1] == 0, HALF, 0)
        ends = [seg_ref[store_block(first + p, core) * BLK + BLK - 1] for p in (3, 5, 7)]
        reach_ref[0] = (ends[0] == ends[2]).astype(jnp.int32) + (ends[1] == ends[2]).astype(jnp.int32)

        for i, part in enumerate((kv_far0, kv_far1, kv_own, kv_oth)):
            kv_ref[i * tok:(i + 1) * tok, :] = part[...]

    flip_heads(q_ref, qt)
    hi = HALF + ((step + 4 * core) & (HALF - 1))
    lo = first_block(seg_ref, ids_ref, step)
    full = jnp.maximum(hi - full_blocks(seg_ref, ids_ref, step, hi), lo)
    segq = rows_ref[HALF + step]

    def start_of(p):
        return pl.multiple_of(store_block(p, core) * BLK, BLK)

    def fold(w):
        return jnp.sum(w.reshape(BLK // 8, 8, BLK), axis=0)

    def keys(start):
        return kv_ref[pl.ds(start, BLK), :HD]

    def values(start):
        return kv_ref[pl.ds(pl.multiple_of(start, BLK), BLK), HD:].T

    def mask_of(start, p):
        return pair_mask(segk[pl.ds(start, BLK), :], segq, p, hi)

    def diagonal():
        start = start_of(hi)
        mask = mask_of(start, hi)
        for h in range(HEADS):
            cols = slice(h * BLK, (h + 1) * BLK)
            s = jnp.where(mask, dot(keys(start), qt[:, cols]) * scale2, -jnp.inf)
            top = jnp.max(s, axis=0, keepdims=True)
            w = jnp.exp2(s - top)
            m_ref[:, cols] = top
            l_ref[:, cols] = fold(w)
            pm[:, cols] = w.astype(jnp.bfloat16)
        acc[...] = jnp.zeros_like(acc)
        return start

    def weigh(p, prev, masked):
        start = start_of(p)
        v_t = values(prev)
        k_blk = keys(start)
        if masked:
            mask = mask_of(start, p)
        for h in range(HEADS):
            cols = slice(h * BLK, (h + 1) * BLK)
            s = dot(k_blk, qt[:, cols]) * scale2 - m_ref[:, cols]
            acc[:, cols] += dot(v_t, pm[:, cols])
            if masked:
                s = jnp.where(mask, s, -jnp.inf)
            w = jnp.exp2(s)
            l_ref[:, cols] += fold(w)
            pm[:, cols] = w.astype(jnp.bfloat16)
        return start

    prev = diagonal()
    prev = lax.fori_loop(0, hi - full, lambda i, c: weigh(hi - 1 - i, c, False), prev)
    prev = lax.fori_loop(0, full - lo, lambda i, c: weigh(full - 1 - i, c, True), prev)
    acc[...] += dot(values(prev), pm[...])

    @pl.when(jnp.logical_not(jnp.max(l_ref[...]) <= 2.0 ** 20))
    def _():
        def safe(i, carry):
            p = hi - 1 - i
            start = start_of(p)
            mask = mask_of(start, p)
            for h in range(HEADS):
                cols = slice(h * BLK, (h + 1) * BLK)
                s = jnp.where(mask, dot(keys(start), qt[:, cols]) * scale2, -jnp.inf)
                top = jnp.maximum(m_ref[:, cols], jnp.max(s, axis=0, keepdims=True))
                fac = jnp.exp2(m_ref[:, cols] - top)
                w = jnp.exp2(s - top)
                m_ref[:, cols] = top
                l_ref[:, cols] = l_ref[:, cols] * fac + fold(w)
                acc[:, cols] = acc[:, cols] * fac + dot(values(start), w.astype(jnp.bfloat16))
            return carry

        first = diagonal()
        acc[...] += dot(values(first), pm[...])
        lax.fori_loop(0, hi - lo, safe, 0)

    total = jnp.sum(l_ref[...], axis=0, keepdims=True)
    lse_ref[0] = m_ref[...] + jnp.log2(total)
    inv = 1.0 / total

    for h in range(HEADS):
        cols = slice(h * BLK, (h + 1) * BLK)
        o_ref[:, h * HD:(h + 1) * HD] = (acc[:, cols] * inv[:, cols]).T.astype(jnp.bfloat16)


def bwd_kernel(remote, *refs):
    if remote:
        (seg_ref, ids_ref, q_ref, do_ref, o_ref, kv_own, kv_oth,
         rows_ref, lse_ref, dq_out, dkv_first, dkv_second, dkv_third,
         segk, kv_ref, qt, dt, delta, pmt, smt, sm, dqt, dkvt) = refs
    else:
        (seg_ref, ids_ref, q_ref, do_ref, o_ref, kv_own, kv_oth,
         rows_ref, lse_ref, dq_in, dq_out, dkv_ref,
         segk, kv_ref, qt, dt, delta, pmt, smt, sm, dqt, dkvt) = refs
    step = pl.program_id(0)
    core = ids_ref[0]
    scale = HD ** -0.5
    scale2 = scale * math.log2(math.e)

    @pl.when(step == 0)
    def _():
        dkvt[...] = jnp.zeros_like(dkvt)
        spread_segments(rows_ref, segk, 0 if remote else HALF, HALF)
        tok = kv_own.shape[0]
        kv_ref[:tok, :] = kv_own[...]
        kv_ref[tok:, :] = kv_oth[...]

    query = HALF + ((step + 4 * core) & (HALF - 1))
    first = first_block(seg_ref, ids_ref, step)
    if remote:
        lo, hi = first, jnp.int32(HALF - 1)
    else:
        lo, hi = jnp.maximum(first, HALF), query
    count = hi - lo + 1
    segq = rows_ref[HALF + step]

    @pl.when(count > 0)
    def _():
        flip_heads(q_ref, qt)
        flip_heads(do_ref, dt)
        for h in range(HEADS):
            hc = slice(h * HD, (h + 1) * HD)
            prod = do_ref[:, hc].astype(jnp.float32) * o_ref[:, hc].astype(jnp.float32)
            delta[:, h * BLK:(h + 1) * BLK] = jnp.sum(prod.T, axis=0, keepdims=True)

    if remote:
        dqt[...] = jnp.zeros_like(dqt)
    else:
        dqt[...] = dq_in[0]

    def body(it, carry):
        p = lo + it
        key_start = pl.multiple_of((store_block(p, core) & (HALF - 1)) * BLK, BLK)
        k_blk = kv_ref[pl.ds(key_start, BLK), :HD]
        v_blk = kv_ref[pl.ds(key_start, BLK), HD:]
        mask = pair_mask(segk[pl.ds(key_start, BLK), :], segq, p, query)
        for h in range(HEADS):
            cols = slice(h * BLK, (h + 1) * BLK)
            s = dot(k_blk, qt[:, cols])
            w = jnp.where(mask, jnp.exp2(s * scale2 - lse_ref[0, :, cols]), 0.0)
            dp = dot(v_blk, dt[:, cols])
            dsv = w * (dp - delta[:, cols])
            pmt[cols, :] = w.astype(jnp.bfloat16).T
            ds_half = dsv.astype(jnp.bfloat16)
            sm[:, cols] = ds_half
            smt[cols, :] = ds_half.T
        put = pl.multiple_of(p * BLK, BLK) if remote else key_start
        dkvt[HD:, pl.ds(put, BLK)] += dot(dt[...], pmt[...])
        dkvt[:HD, pl.ds(put, BLK)] += dot(qt[...], smt[...])
        dqt[...] += dot(k_blk.T, sm[...])
        return carry

    lax.fori_loop(0, count, body, 0)

    @pl.when(step == pl.num_programs(0) - 1)
    def _():
        at = 0
        for part in (dkv_first, dkv_second, dkv_third) if remote else (dkv_ref,):
            for t in range(0, part.shape[0], BLK):
                part[t:t + BLK, :] = dkvt[:, at + t:at + t + BLK].T
            at += part.shape[0]

    if remote:
        dq_out[0] = dqt[...]
    else:
        for h in range(HEADS):
            cols = slice(h * BLK, (h + 1) * BLK)
            dq_out[:, h * HD:(h + 1) * HD] = (dqt[:, cols] * scale).T.astype(jnp.bfloat16)


def lanes(ref, first, count):
    return jnp.concatenate([ref[first + h] for h in range(count)], axis=1)


def project_kernel(ids_ref, a_own, a_oth, w_ref, out_ref):
    half = out_ref.shape[0] // 2

    def put(src):
        for n in range(0, HEADS, 2):
            weight = jnp.concatenate([w_ref[n], w_ref[n + 1]], axis=1)
            for t in (0, half):
                out_ref[t:t + half, n * HD:(n + 2) * HD] = dot(src[t:t + half, :], weight).astype(jnp.bfloat16)

    @pl.when(pl.program_id(0) == 0)
    def _():
        put(a_own)

    @pl.when(pl.program_id(0) == 1)
    def _():
        put(a_oth)


def project_kv_kernel(ids_ref, a_ref, wk_ref, wv_ref, out_ref, pass_ref, mine_ref, other_ref, wide):
    @pl.when(pl.program_id(0) == 0)
    def _():
        dim = mine_ref.shape[0]
        for i, ref in enumerate((wk_ref, wv_ref)):
            wide[...] = ref[...].astype(jnp.float32)
            cols = slice(i * HD, (i + 1) * HD)
            mine_ref[:, cols] = wide[pl.ds(ids_ref[0], dim, stride=2), :].astype(jnp.bfloat16)
            other_ref[:, cols] = wide[pl.ds(1 - ids_ref[0], dim, stride=2), :].astype(jnp.bfloat16)

    out_ref[...] = dot(a_ref[...], mine_ref[...]).astype(jnp.bfloat16)
    pass_ref[...] = dot(a_ref[...], other_ref[...]).astype(jnp.bfloat16)


def expand_kernel(ids_ref, a_ref, b_ref, wa_ref, wb_ref, out_ref):
    out_ref[...] = (dot_nt(a_ref[...], lanes(wa_ref, 0, HEADS))
                    + dot_nt(b_ref[...], lanes(wb_ref, 0, HEADS))).astype(jnp.bfloat16)


def expand_kv_kernel(ids_ref, a_ref, b_ref, wa_ref, wb_ref, c_ref, d_ref, wc_ref, wd_ref, out_ref):
    out_ref[...] = (dot_nt(a_ref[...], lanes(wa_ref, 0, HEADS))
                    + dot_nt(b_ref[...], lanes(wb_ref, 0, HEADS))
                    + dot_nt(c_ref[...], wc_ref[...]) + dot_nt(d_ref[...], wd_ref[...])).astype(jnp.bfloat16)


def turn_kernel(ids_ref, a_ref, b_ref, out_ref):
    half = pl.num_programs(0) // 2

    @pl.when(pl.program_id(0) < half)
    def _():
        out_ref[...] = a_ref[...].T

    @pl.when(pl.program_id(0) >= half)
    def _():
        out_ref[...] = b_ref[...].T


def wgrad_one_kernel(partner, a_ref, b_ref, out_ref):
    tok = a_ref.shape[1] // 2
    first, second = (b_ref[tok:, :], b_ref[:tok, :]) if partner else (b_ref[:tok, :], b_ref[tok:, :])
    val = dot(a_ref[:, :tok], first) + dot(a_ref[:, tok:], second)
    for h in range(out_ref.shape[0]):
        out_ref[h] = val[:, h * HD:(h + 1) * HD]


def wgrad_kernel(ids_ref, a_ref, b_ref, c_ref, out_ref):
    step = pl.program_id(0)
    half = pl.num_programs(0) // 2
    tok = a_ref.shape[1] // 2

    def put(own, oth):
        val = dot(a_ref[:, :tok], own) + dot(a_ref[:, tok:], oth)
        for h in range(out_ref.shape[0]):
            out_ref[h] = val[:, h * HD:(h + 1) * HD]

    @pl.when(step < half)
    def _():
        put(b_ref[:tok, :], b_ref[tok:, :])

    @pl.when(step >= half)
    def _():
        put(c_ref[tok:, :], c_ref[:tok, :])


def whole(i, *_):
    return (0, 0)


def whole3(i, *_):
    return (0, 0, 0)


def lead(i, *_):
    return (i, 0, 0)


def params(mib):
    return pltpu.CompilerParams(dimension_semantics=('arbitrary',), vmem_limit_bytes=mib * 1024 * 1024)


def attend(seg, ids, q, kv_far, kv_near, rows):
    tok = q.shape[0]
    keys = 2 * tok
    grid = tok // BLK
    block = pl.BlockSpec((BLK, HEADS * HD), lambda i, *_: (i, 0))
    return pl.pallas_call(
        fwd_kernel,
        grid_spec=pltpu.PrefetchScalarGridSpec(
            num_scalar_prefetch=2, grid=(grid,),
            in_specs=[block] + [pl.BlockSpec((tok // 2, 2 * HD), whole)] * 4
            + [pl.BlockSpec((keys // BLK, 1, BLK), whole3)],
            out_specs=[block, pl.BlockSpec((1, 1, WIDE), lead), pl.BlockSpec(memory_space=pltpu.SMEM)],
            scratch_shapes=[pltpu.VMEM((keys, 128), jnp.int32), pltpu.VMEM((keys, 2 * HD), jnp.bfloat16),
                            pltpu.VMEM((HD, WIDE), jnp.bfloat16), pltpu.VMEM((HD, WIDE), jnp.float32),
                            pltpu.VMEM((1, WIDE), jnp.float32), pltpu.VMEM((8, WIDE), jnp.float32),
                            pltpu.VMEM((BLK, WIDE), jnp.bfloat16)]),
        out_shape=[jax.ShapeDtypeStruct((tok, HEADS * HD), jnp.bfloat16),
                   jax.ShapeDtypeStruct((grid, 1, WIDE), jnp.float32), jax.ShapeDtypeStruct((1,), jnp.int32)],
        compiler_params=params(24), name='attend',
        cost_estimate=pl.CostEstimate(flops=40 * 4 * WIDE * BLK * HD, bytes_accessed=12 << 20, transcendentals=0),
    )(seg, ids, q, *kv_far, *kv_near, rows)


def attend_grad(remote, seg, ids, q, do, o, kv, rows, lse, dq_in=None):
    tok = q.shape[0]
    grid = tok // BLK
    block = pl.BlockSpec((BLK, HEADS * HD), lambda i, *_: (i, 0))
    in_specs = [block] * 3 + [pl.BlockSpec((tok // 2, 2 * HD), whole)] * 2 + [
        pl.BlockSpec(rows.shape, whole3), pl.BlockSpec((1, 1, WIDE), lead)]
    args = [seg, ids, q, do, o, *kv, rows, lse]
    dqt_spec = pl.BlockSpec((1, HD, WIDE), lead)
    kv_grad = jax.ShapeDtypeStruct((tok, 2 * HD), jnp.float32)
    kv_spec = pl.BlockSpec((tok, 2 * HD), whole)
    if remote:
        parts = [(n, 2 * HD) for n in (tok // 2, tok // 4, tok // 4)]
        out_shape = [jax.ShapeDtypeStruct((grid, HD, WIDE), jnp.float32)]
        out_shape += [jax.ShapeDtypeStruct(part, jnp.float32) for part in parts]
        out_specs = [dqt_spec] + [pl.BlockSpec(part, whole) for part in parts]
    else:
        in_specs.append(dqt_spec)
        args.append(dq_in)
        out_shape = [jax.ShapeDtypeStruct((tok, HEADS * HD), jnp.bfloat16), kv_grad]
        out_specs = [block, kv_spec]
    flip = pltpu.VMEM((HD, WIDE), jnp.bfloat16)
    turned = pltpu.VMEM((WIDE, BLK), jnp.bfloat16)
    return pl.pallas_call(
        functools.partial(bwd_kernel, remote),
        grid_spec=pltpu.PrefetchScalarGridSpec(
            num_scalar_prefetch=2, grid=(grid,), in_specs=in_specs, out_specs=out_specs,
            scratch_shapes=[pltpu.VMEM((tok, 128), jnp.int32), pltpu.VMEM((tok, 2 * HD), jnp.bfloat16),
                            flip, flip, pltpu.VMEM((1, WIDE), jnp.float32), turned, turned,
                            pltpu.VMEM((BLK, WIDE), jnp.bfloat16), pltpu.VMEM((HD, WIDE), jnp.float32),
                            pltpu.VMEM((2 * HD, tok), jnp.float32)]),
        out_shape=out_shape, compiler_params=params(28),
        name='attend_grad_remote' if remote else 'attend_grad_local',
        cost_estimate=pl.CostEstimate(flops=20 * 10 * WIDE * BLK * HD, bytes_accessed=20 << 20, transcendentals=0),
    )(*args)


def project(ids, a, b, w):
    tok, dim = a.shape
    return pl.pallas_call(
        project_kernel,
        grid_spec=pltpu.PrefetchScalarGridSpec(
            num_scalar_prefetch=1, grid=(2,),
            in_specs=[pl.BlockSpec((tok, dim), whole)] * 2
            + [pl.BlockSpec((HEADS, dim, HD), lambda t, ids: (ids[0], 0, 0))],
            out_specs=pl.BlockSpec((tok, HEADS * HD), lambda t, ids: (t, 0))),
        out_shape=jax.ShapeDtypeStruct((2 * tok, HEADS * HD), jnp.bfloat16),
        compiler_params=params(24),
        cost_estimate=pl.CostEstimate(flops=4 * tok * dim * HEADS * HD, bytes_accessed=12 << 20, transcendentals=0),
    )(ids, a, b, w)


def project_kv(ids, a, w_k, w_v):
    tok, dim = a.shape
    mine = jax.ShapeDtypeStruct((dim, 2 * HD), jnp.bfloat16)
    pack = pl.BlockSpec((2 * dim, HD), whole)
    return pl.pallas_call(
        project_kv_kernel,
        grid_spec=pltpu.PrefetchScalarGridSpec(
            num_scalar_prefetch=1, grid=(2,),
            in_specs=[pl.BlockSpec((tok // 2, dim), lambda i, ids: (i, 0)), pack, pack],
            out_specs=[pl.BlockSpec((tok // 2, 2 * HD), lambda i, ids: (i, 0))] * 2
            + [pl.BlockSpec((dim, 2 * HD), whole)] * 2,
            scratch_shapes=[pltpu.VMEM((2 * dim, HD), jnp.float32)]),
        out_shape=[jax.ShapeDtypeStruct((tok, 2 * HD), jnp.bfloat16)] * 2 + [mine, mine],
        compiler_params=params(60), name='project_kv',
        cost_estimate=pl.CostEstimate(flops=4 * tok * dim * HD, bytes_accessed=6 << 20, transcendentals=0),
    )(ids, a, w_k.reshape(2 * dim, HD), w_v.reshape(2 * dim, HD))


def expand(ids, a, b, w, extra=()):
    tok, width = a.shape[0] // 2, a.shape[1]
    dim = w.shape[1]
    cols = 512

    def first(i, ids):
        return (0, 0)

    def second(i, ids):
        return (1, 0)

    specs = [pl.BlockSpec((tok, width), first), pl.BlockSpec((tok, width), second),
             pl.BlockSpec((HEADS, cols, HD), lambda i, ids: (ids[0], i, 0)),
             pl.BlockSpec((HEADS, cols, HD), lambda i, ids: (1 - ids[0], i, 0))]
    args = [a, b, w, w]
    if extra:
        specs += [pl.BlockSpec((tok, 2 * HD), first), pl.BlockSpec((tok, 2 * HD), second)]
        specs += [pl.BlockSpec((cols, 2 * HD), lambda i, ids: (i, 0))] * 2
        args += extra
    return pl.pallas_call(
        expand_kv_kernel if extra else expand_kernel,
        grid_spec=pltpu.PrefetchScalarGridSpec(
            num_scalar_prefetch=1, grid=(dim // cols,), in_specs=specs,
            out_specs=pl.BlockSpec((tok, cols), lambda i, ids: (0, i))),
        out_shape=jax.ShapeDtypeStruct((tok, dim), jnp.bfloat16),
        compiler_params=params(20), name='grad_x' if extra else 'out_y',
        cost_estimate=pl.CostEstimate(flops=4 * tok * dim * width, bytes_accessed=14 << 20, transcendentals=0),
    )(ids, *args)


def turn(where, a, b):
    tok, dim = a.shape
    rows = dim // 4
    part = tok // 2
    return pl.pallas_call(
        turn_kernel,
        grid_spec=pltpu.PrefetchScalarGridSpec(
            num_scalar_prefetch=1, grid=(4,),
            in_specs=[pl.BlockSpec((part, rows), lambda i, ids: (jnp.minimum(i, 1), ids[0])),
                      pl.BlockSpec((part, rows), lambda i, ids: (jnp.maximum(i - 2, 0), ids[0]))],
            out_specs=pl.BlockSpec((rows, part), lambda i, ids: (0, i))),
        out_shape=jax.ShapeDtypeStruct((rows, 2 * tok), jnp.bfloat16),
        compiler_params=params(12),
        cost_estimate=pl.CostEstimate(flops=2 << 30, bytes_accessed=4 * rows * tok * 2, transcendentals=0),
    )(where.reshape(1).astype(jnp.int32), a, b)


def wgrad(core, a, b, c):
    rows, tok = a.shape
    width = b.shape[1]
    step = 256
    half = width // step
    heads = step // HD
    return pl.pallas_call(
        wgrad_kernel,
        grid_spec=pltpu.PrefetchScalarGridSpec(
            num_scalar_prefetch=1, grid=(2 * half,),
            in_specs=[pl.BlockSpec((rows, tok), whole),
                      pl.BlockSpec((tok, step), lambda i, ids: (0, jnp.minimum(i, half - 1))),
                      pl.BlockSpec((tok, step), lambda i, ids: (0, jnp.maximum(i - half, 0)))],
            out_specs=pl.BlockSpec((heads, rows, HD), lambda i, ids: (lax.rem(i + half * ids[0], 2 * half), 0, 0))),
        out_shape=jax.ShapeDtypeStruct((2 * width // HD, rows, HD), jnp.float32),
        compiler_params=params(16),
        cost_estimate=pl.CostEstimate(flops=4 * tok * rows * width, bytes_accessed=10 << 20, transcendentals=0),
    )(core.reshape(1).astype(jnp.int32), a, b, c)


def wgrad_one(a, b, partner):
    rows, tok = a.shape
    width = b.shape[1]
    step = 256
    heads = step // HD
    return pl.pallas_call(
        functools.partial(wgrad_one_kernel, partner),
        grid=(width // step,),
        in_specs=[pl.BlockSpec((rows, tok), whole), pl.BlockSpec((tok, step), lambda i: (0, i))],
        out_specs=pl.BlockSpec((heads, rows, HD), lambda i: (i, 0, 0)),
        out_shape=jax.ShapeDtypeStruct((width // HD, rows, HD), jnp.float32),
        compiler_params=params(16),
        cost_estimate=pl.CostEstimate(flops=2 * tok * rows * width, bytes_accessed=6 << 20, transcendentals=0),
    )(a, b)


def after(value, *others):
    return lax.optimization_barrier((value, *others))[0]


def solution(mesh):
    row_spec = P(('dp', 'cp'), None)
    tok_spec = P(('dp', 'cp'))
    weight_spec = P(None, None, None)
    grad_spec = P(('dp', 'cp'), None, None)
    core_pairs = [(0, 1), (1, 0), (2, 3), (3, 2)]
    chip_pairs = [(0, 2), (2, 0), (1, 3), (3, 1)]
    up_pairs = [(0, 2), (1, 3)]
    up_cross = [(0, 3), (1, 2)]
    down_pairs = [(2, 0), (3, 1)]

    def send(a, pairs):
        return lax.ppermute(a, 'cp', pairs)

    def layer(x, seg, w_q, w_k, w_v, w_o, dy):
        _, dim = x.shape
        rows = dim // 4
        index = lax.axis_index('cp')
        core = index % 2
        chip = index // 2
        near_rows = index
        far_rows = 2 * (1 - chip) + core
        ids = jnp.stack([core, chip]).astype(jnp.int32)
        w_q = jnp.transpose(w_q, (1, 0, 2))
        w_o = jnp.transpose(w_o, (1, 0, 2))

        x_o = send(x, core_pairs)
        kv_own, kv_pass, wkv_c, wkv_p = project_kv(ids, x, w_k, w_v)
        kv_far0 = send(kv_own, up_pairs)
        kv_far1 = send(kv_pass, up_cross)
        kv_oth = send(kv_pass, core_pairs)
        seg_o = send(after(seg, kv_own), core_pairs)
        dy_o = send(after(dy, kv_own), core_pairs)
        seg_far0 = send(after(seg, kv_own), up_pairs)
        seg_far1 = send(after(seg, kv_own), up_cross)
        seg_all = jnp.concatenate([seg_far0, seg_far1, seg, seg_o])
        seg_rows = seg_all.reshape(-1, 1, BLK)
        kv_far, kv_near = (kv_far0, kv_far1), (kv_own, kv_oth)
        q = project(ids, after(x, kv_own), x_o, w_q)
        dy_far = turn(far_rows, dy, dy_o)
        x_far = turn(far_rows, x, x_o)

        o, lse, reach = attend(seg_all, ids, q, kv_far, kv_near, seg_rows)
        o_p = send(o, core_pairs)
        dwo_far = wgrad_one(dy_far, o, False)
        dwo_in = send(dwo_far, chip_pairs)
        dwo_far2 = wgrad_one(dy_far, o_p, True)
        dwo_in2 = send(dwo_far2, chip_pairs)

        do = project(ids, after(dy, dwo_far), dy_o, w_o)
        dq_part, *far = attend_grad(True, seg_all, ids, q, do, o, kv_far, seg_rows, lse)
        last_in = send(far[2], down_pairs)
        local = (seg_all, ids, q, do, o, kv_near, seg_rows, lse, dq_part)

        def near_pass(level):
            def run(first, second, x_far, args):
                second_in = send(second, down_pairs) if level > 0 else jnp.zeros_like(second)
                first_in = send(first, down_pairs) if level > 1 else jnp.zeros_like(first)
                dq, dkv = attend_grad(False, *args)
                return dq, dkv, wgrad_one(x_far, dq, False), first_in, second_in

            return run

        dq, dkv_near, dwq_far1, first_in, second_in = lax.switch(
            reach[0], [near_pass(level) for level in range(3)], far[0], far[1], x_far, local)
        dwq_in = send(dwq_far1, chip_pairs)
        dq_p = send(dq, core_pairs)
        dwq_far = wgrad_one(x_far, dq_p, True)
        dwq_in2 = send(dwq_far, chip_pairs)

        y = expand(ids, after(o, dwq_far), o_p, w_o)
        x_near = turn(near_rows, after(x, dwq_far), x_o)
        dy_near = turn(near_rows, after(dy, dwq_far), dy_o)
        dwo_near = wgrad(core, dy_near, o, o_p)
        dwq_near = wgrad(core, x_near, dq, dq_p)

        dkv = dkv_near + jnp.where(core == 0, jnp.concatenate([first_in, second_in, last_in]),
                                   jnp.concatenate([second_in, last_in, first_in]))
        dkv = jnp.concatenate([dkv[:, :HD] * HD ** -0.5, dkv[:, HD:]], axis=1).astype(jnp.bfloat16)
        dkv_p = send(dkv, core_pairs)
        dwkv_far = wgrad(core, x_far, dkv, dkv_p)
        dwkv_in = send(dwkv_far, chip_pairs)
        dwkv_near = wgrad(core, x_near, after(dkv, dwkv_far), dkv_p)
        dx = expand(ids, after(dq, dwkv_far), dq_p, w_q, (dkv, dkv_p, wkv_c, wkv_p))

        def total(near, mine, other):
            far = jnp.where(core == 0, jnp.concatenate([mine, other]), jnp.concatenate([other, mine]))
            return jnp.transpose(near + far, (1, 0, 2))

        dw_o = total(dwo_near, dwo_in, dwo_in2)
        dw_q = total(dwq_near, dwq_in, dwq_in2)
        dw_kv = jnp.transpose(dwkv_near + dwkv_in, (1, 0, 2)).reshape(rows, 2, 2, HD)
        return y, dx, dw_q, dw_kv[:, :, 0], dw_kv[:, :, 1], dw_o

    return jax.shard_map(layer, mesh=mesh,
                         in_specs=(row_spec, tok_spec, weight_spec, weight_spec, weight_spec, weight_spec, row_spec),
                         out_specs=(row_spec, row_spec, grad_spec, grad_spec, grad_spec, grad_spec),
                         check_vma=False)
```
